32 devices in a mesh: dp: 8 (over y, x, core), seq: 4 (over z).
Axes of the slice: x: 2, y: 2, z: 4, core: 2. Of those that a mesh axis runs over, the one named last changes fastest.
Arguments:
- tokens: bfloat16 [16, 1024, 1024], P('dp', 'seq'), may hold values from -16 to 16
- condition: bfloat16 [16, 1024], P('dp'), may hold values from -6 to 6
- ada_weight: bfloat16 [1024, 6144], P('dp'), may hold values from -0.1875 to 0.1875
- ada_bias: bfloat16 [6144], P('dp'), may hold values from -3 to 3
- qkv_weight: bfloat16 [1024, 3072], P('dp'), may hold values from -4 to 4
- qv_bias: bfloat16 [2048], P('dp'), may hold values from -3 to 3
- out_weight: bfloat16 [1024, 1024], P('dp'), may hold values from -0.75 to 0.75
- out_bias: bfloat16 [1024], P('dp'), may hold values from -3 to 3
- up_weight: bfloat16 [1024, 4096], P('dp'), may hold values from -0.1875 to 0.1875
- up_bias: bfloat16 [4096], P('dp'), may hold values from -3 to 3
- down_weight: bfloat16 [4096, 1024], P('dp'), may hold values from -0.09375 to 0.09375
- down_bias: bfloat16 [1024], P('dp'), may hold values from -3 to 3
- cotangent: bfloat16 [16, 1024, 1024], P('dp', 'seq'), may hold values from -6 to 6
Outputs:
- output: bfloat16 [16, 1024, 1024], P('dp', 'seq')
- tokens_grad: float32 [16, 1024, 1024], P('dp', 'seq')
- condition_grad: float32 [16, 1024], P('dp')
- ada_weight_grad: float32 [1024, 6144], P('dp')
- ada_bias_grad: float32 [6144], P('dp')
- qkv_weight_grad: float32 [1024, 3072], P('dp')
- qv_bias_grad: float32 [2048], P('dp')
- out_weight_grad: float32 [1024, 1024], P('dp')
- out_bias_grad: float32 [1024], P('dp')
- up_weight_grad: float32 [1024, 4096], P('dp')
- up_bias_grad: float32 [4096], P('dp')
- down_weight_grad: float32 [4096, 1024], P('dp')
- down_bias_grad: float32 [1024], P('dp')
The draws below stay inside these ranges and needn't reach their ends.
All inputs are finite; a program needn't handle non-finite values.
Results may differ from the reference program's by a relative error of at most 0.012.
The reference program's roundings to bfloat16 on the way count: a program that leaves them out, or rounds other values in their place, can miss the bound.
Values may be sent and summed in bfloat16 or wider, within the bound.
A program may use at most 256 MiB of HBM per device.

```python
import jax
import jax.numpy as jnp
from jax import lax

D = 1024
H = 16
HD = 64
FF = 4096
SEQLEN = 1024
LATENTS = 16


def draw_tokens(key, part):
    key_base = jax.random.fold_in(jax.random.fold_in(key, 11), 0)
    shape = (LATENTS, SEQLEN, D)
    drawn = jnp.clip(jax.random.normal(key_base, shape, jnp.float32), -6.0, 6.0)
    return drawn.astype(jnp.bfloat16)


def draw_qkv_weight(key, part):
    key_base = jax.random.fold_in(key, 23)
    shape = (D, 3 * D)
    drawn = jnp.clip(jax.random.normal(key_base, shape, jnp.float32), -6.0, 6.0) * D ** (-0.5)
    return drawn.astype(jnp.bfloat16)


def levels(key, dims, cuts, smallest, top_value):
    def one(position, parts):
        heights = jax.random.uniform(jax.random.fold_in(jax.random.fold_in(key, 6), position), (parts,), jnp.float32, smallest / len(cuts), top_value / len(cuts))
        return jnp.repeat(jnp.exp(heights), dims[position] // parts).reshape((-1,) + (1,) * (len(dims) - position - 1))

    factor_of = one(*cuts[0])
    for cut in cuts[1:]:
        factor_of = factor_of * one(*cut)
    return factor_of


def normal_values(key, extent, deviation, bound, shards=(), held_as=jnp.bfloat16):
    factor_of = levels(key, extent, shards, -0.22, 0.18) if shards else 1.0
    entries = jax.random.normal(key, extent, jnp.float32) * deviation * factor_of
    return jnp.minimum(jnp.maximum(entries, -bound), bound).astype(held_as)


def setup_inputs(seed: int = 0) -> dict:
    seeds = jax.random.split(jax.random.key(seed), 14)
    return {
        "tokens": draw_tokens(jax.random.fold_in(seeds[13], 71), 0),
        "condition": normal_values(seeds[1], (LATENTS, D), 1.0, 6.0, ((0, 8),)),
        "ada_weight": normal_values(seeds[2], (D, 6 * D), D ** -0.5, 0.1875, ((0, 8),)),
        "ada_bias": normal_values(seeds[3], (6 * D,), 0.5, 3.0, ((0, 8),)),
        "qkv_weight": draw_qkv_weight(jax.random.fold_in(seeds[13], 71), 0),
        "qv_bias": normal_values(seeds[5], (2 * D,), 0.5, 3.0, ((0, 8),)),
        "out_weight": normal_values(seeds[6], (D, D), (D // 16) ** -0.5, 0.75, ((0, 8),)),
        "out_bias": normal_values(seeds[7], (D,), 0.5, 3.0, ((0, 8),)),
        "up_weight": normal_values(seeds[8], (D, FF), D ** -0.5, 0.1875, ((0, 8),)),
        "up_bias": normal_values(seeds[9], (FF,), 0.5, 3.0, ((0, 8),)),
        "down_weight": normal_values(seeds[10], (FF, D), FF ** -0.5, 0.09375, ((0, 8),)),
        "down_bias": normal_values(seeds[11], (D,), 0.5, 3.0, ((0, 8),)),
        "cotangent": normal_values(seeds[12], (LATENTS, SEQLEN, D), 1.0, 6.0, ((0, 8), (1, 4))),
    }


EPSILON = 1e-06

def norm_shift(inputs, shift_row, scale_row):
    centred = inputs - lax.optimization_barrier(jnp.mean(inputs, axis=-1, keepdims=True))
    variance = lax.optimization_barrier(jnp.mean(centred * centred, axis=-1, keepdims=True))
    return centred * lax.rsqrt(variance + EPSILON) * (1.0 + scale_row) + shift_row

def gelu_tanh(inputs):
    return jax.nn.gelu(inputs, approximate=True)

def to_half(inputs):
    return lax.optimization_barrier(inputs.astype(jnp.bfloat16)).astype(jnp.float32)

def split_heads(matrix):
    return matrix.astype(jnp.float32).reshape(matrix.shape[0], H, HD)

def attend_forward(query_rows, key_rows, value_rows):
    query_heads = split_heads(query_rows)
    key_heads = split_heads(key_rows)
    value_heads = split_heads(value_rows)
    scores = jnp.einsum('qhd,khd->hqk', query_heads, key_heads) * HD ** (-0.5)
    row_peak = lax.optimization_barrier(jnp.max(scores, axis=-1, keepdims=True))
    logsum = row_peak[..., 0] + jnp.log(lax.optimization_barrier(jnp.sum(jnp.exp(scores - row_peak), axis=-1)))
    attn_probs = to_half(jnp.exp(scores - logsum[..., None]))
    mixed_rows = jnp.einsum('hqk,khd->qhd', attn_probs, value_heads)
    return (mixed_rows.reshape(query_rows.shape[0], D).astype(jnp.bfloat16), logsum)

def attend_backward(query_rows, key_rows, value_rows, logsum, grad_rows):
    query_heads = split_heads(query_rows)
    key_heads = split_heads(key_rows)
    value_heads = split_heads(value_rows)
    grad_heads = split_heads(grad_rows)
    scale_value = HD ** (-0.5)
    scores = jnp.einsum('qhd,khd->hqk', query_heads, key_heads) * scale_value
    attn_probs = jnp.exp(scores - logsum[..., None])
    probs_half = to_half(attn_probs)
    grad_value = jnp.einsum('hqk,qhd->khd', probs_half, grad_heads)
    grad_probs = jnp.einsum('qhd,khd->hqk', grad_heads, value_heads)
    inner_sum = lax.optimization_barrier(jnp.sum(attn_probs * grad_probs, axis=-1, keepdims=True))
    grad_scores = to_half(attn_probs * (grad_probs - inner_sum) * scale_value)
    grad_query = jnp.einsum('hqk,khd->qhd', grad_scores, key_heads)
    grad_key = jnp.einsum('hqk,qhd->khd', grad_scores, query_heads)
    token_count = query_rows.shape[0]
    return jnp.concatenate([grad_query.reshape(token_count, D), grad_key.reshape(token_count, D), grad_value.reshape(token_count, D)], axis=1).astype(jnp.bfloat16)

def latent_pass(weights, tokens_one, mod_row, cot_one):
    qkv_weight, qv_bias, out_weight, out_bias, up_weight, up_bias, down_weight, down_bias = weights
    mod_pieces = mod_row.reshape(6, D)
    shift_a, scale_a, gate_a = (mod_pieces[0], mod_pieces[1], mod_pieces[2])
    shift_b, scale_b, gate_b = (mod_pieces[3], mod_pieces[4], mod_pieces[5])
    tokens_float = tokens_one.astype(jnp.float32)
    normed_a = norm_shift(tokens_float, shift_a, scale_a).astype(jnp.bfloat16)
    bias_all = jnp.concatenate([qv_bias[:D], jnp.zeros((D,), qv_bias.dtype), qv_bias[D:]]).astype(jnp.float32)
    projected = (jnp.dot(normed_a, qkv_weight, preferred_element_type=jnp.float32) + bias_all).astype(jnp.bfloat16)
    attended, logsum = attend_forward(projected[:, :D], projected[:, D:2 * D], projected[:, 2 * D:])
    branch_a = jnp.dot(attended, out_weight, preferred_element_type=jnp.float32) + out_bias.astype(jnp.float32)
    middle = tokens_float + gate_a * branch_a
    normed_b = norm_shift(middle, shift_b, scale_b).astype(jnp.bfloat16)
    hidden_pre = jnp.dot(normed_b, up_weight, preferred_element_type=jnp.float32) + up_bias.astype(jnp.float32)
    hidden = gelu_tanh(hidden_pre).astype(jnp.bfloat16)
    branch_b = jnp.dot(hidden, down_weight, preferred_element_type=jnp.float32) + down_bias.astype(jnp.float32)
    result = (middle + gate_b * branch_b).astype(jnp.bfloat16)
    cot_float = cot_one.astype(jnp.float32)
    grad_gate_b = lax.optimization_barrier(jnp.sum(cot_float * branch_b, axis=0))
    grad_branch_b = cot_float * gate_b
    down_bias_grad = lax.optimization_barrier(jnp.sum(grad_branch_b, axis=0))
    grad_branch_half = grad_branch_b.astype(jnp.bfloat16)
    down_weight_grad = jnp.dot(hidden.T, grad_branch_half, preferred_element_type=jnp.float32)
    grad_hidden = jnp.dot(grad_branch_half, down_weight.T, preferred_element_type=jnp.float32)
    _, gelu_back = jax.vjp(gelu_tanh, hidden_pre)
    grad_pre = gelu_back(grad_hidden)[0]
    up_bias_grad = lax.optimization_barrier(jnp.sum(grad_pre, axis=0))
    grad_pre_half = grad_pre.astype(jnp.bfloat16)
    up_weight_grad = jnp.dot(normed_b.T, grad_pre_half, preferred_element_type=jnp.float32)
    grad_normed_b = jnp.dot(grad_pre_half, up_weight.T, preferred_element_type=jnp.float32)
    _, norm_back_b = jax.vjp(norm_shift, middle, shift_b, scale_b)
    grad_mid_norm, grad_shift_b, grad_scale_b = norm_back_b(grad_normed_b)
    grad_middle = cot_float + grad_mid_norm
    grad_gate_a = lax.optimization_barrier(jnp.sum(grad_middle * branch_a, axis=0))
    grad_branch_a = grad_middle * gate_a
    out_bias_grad = lax.optimization_barrier(jnp.sum(grad_branch_a, axis=0))
    grad_branch_a_half = grad_branch_a.astype(jnp.bfloat16)
    out_weight_grad = jnp.dot(attended.T, grad_branch_a_half, preferred_element_type=jnp.float32)
    grad_attended = jnp.dot(grad_branch_a_half, out_weight.T, preferred_element_type=jnp.float32).astype(jnp.bfloat16)
    grad_projected = attend_backward(projected[:, :D], projected[:, D:2 * D], projected[:, 2 * D:], logsum, grad_attended)
    qkv_weight_grad = jnp.dot(normed_a.T, grad_projected, preferred_element_type=jnp.float32)
    grad_proj_float = grad_projected.astype(jnp.float32)
    qv_bias_grad = jnp.concatenate([lax.optimization_barrier(jnp.sum(grad_proj_float[:, :D], axis=0)), lax.optimization_barrier(jnp.sum(grad_proj_float[:, 2 * D:], axis=0))])
    grad_normed_a = jnp.dot(grad_projected, qkv_weight.T, preferred_element_type=jnp.float32)
    _, norm_back_a = jax.vjp(norm_shift, tokens_float, shift_a, scale_a)
    grad_tok_norm, grad_shift_a, grad_scale_a = norm_back_a(grad_normed_a)
    tokens_grad = grad_middle + grad_tok_norm
    grad_modulation = jnp.concatenate([grad_shift_a, grad_scale_a, grad_gate_a, grad_shift_b, grad_scale_b, grad_gate_b])
    grads = (qkv_weight_grad, qv_bias_grad, out_weight_grad, out_bias_grad, up_weight_grad, up_bias_grad, down_weight_grad, down_bias_grad)
    return (result, tokens_grad, grad_modulation, grads)

def reference(tokens, condition, ada_weight, ada_bias, qkv_weight, qv_bias, out_weight, out_bias, up_weight, up_bias, down_weight, down_bias, cotangent):
    cond_float = condition.astype(jnp.float32)
    silu_cond = jax.nn.silu(cond_float).astype(jnp.bfloat16)
    modulation = jnp.dot(silu_cond, ada_weight, preferred_element_type=jnp.float32) + ada_bias.astype(jnp.float32)
    weights = (qkv_weight, qv_bias, out_weight, out_bias, up_weight, up_bias, down_weight, down_bias)
    zero_totals = tuple((jnp.zeros(item.shape, jnp.float32) for item in weights))

    def scan_step(totals, inputs):
        tokens_one, mod_row, cot_one = inputs
        result, tokens_grad_one, grad_mod_one, grads = latent_pass(weights, tokens_one, mod_row, cot_one)
        new_totals = tuple((total + grad for total, grad in zip(totals, grads)))
        return (new_totals, (result, tokens_grad_one, grad_mod_one))
    totals, (output, tokens_grad, grad_modulation) = lax.scan(scan_step, zero_totals, (tokens, modulation, cotangent))
    grad_mod_half = grad_modulation.astype(jnp.bfloat16)
    ada_weight_grad = jnp.dot(silu_cond.T, grad_mod_half, preferred_element_type=jnp.float32)
    ada_bias_grad = lax.optimization_barrier(jnp.sum(grad_modulation, axis=0))
    sigmoid_cond = jax.nn.sigmoid(cond_float)
    silu_slope = sigmoid_cond * (1.0 + cond_float * (1.0 - sigmoid_cond))
    condition_grad = silu_slope * jnp.dot(grad_mod_half, ada_weight.T, preferred_element_type=jnp.float32)
    return (output, tokens_grad, condition_grad, ada_weight_grad, ada_bias_grad, totals[0], totals[1], totals[2], totals[3], totals[4], totals[5], totals[6], totals[7])
```

```python
import functools

import jax
import jax.numpy as jnp
from jax import lax
from jax.experimental import pallas as pl
from jax.experimental.pallas import tpu as pltpu
from jax.sharding import PartitionSpec as P

HD = 64
LANES = 128
EPSILON = 1e-06
HALF = jnp.bfloat16
F32 = jnp.float32


def nn(a, b):
    return jnp.dot(a, b, preferred_element_type=F32)


def nt(a, b):
    return lax.dot_general(a, b, (((1,), (1,)), ((), ())), preferred_element_type=F32)


def tn(a, b):
    return lax.dot_general(a, b, (((0,), (0,)), ((), ())), preferred_element_type=F32)


def attend_kernel(groups, *refs):
    q_ref = refs[0]
    k_refs = refs[1 : 1 + groups]
    v_refs = refs[1 + groups : 1 + 2 * groups]
    out_ref, lse_ref, lse_acc = refs[1 + 2 * groups :]
    step = pl.program_id(0)
    rows = q_ref.shape[0]
    block = 256
    low = lax.broadcasted_iota(jnp.int32, (block, LANES), 1) < HD
    lane = lax.broadcasted_iota(jnp.int32, (block, LANES), 1)
    for start in range(0, rows, block):
        here = pl.ds(start, block)
        q = q_ref[here, :] * HALF(HD**-0.5)
        pieces = []
        for head in range(2):
            own = low if head == 0 else jnp.logical_not(low)
            qm = jnp.where(own, q, jnp.zeros_like(q))
            scores = [nt(qm, k[...]) for k in k_refs]
            peak = functools.reduce(
                jnp.maximum, [jnp.max(s, axis=-1, keepdims=True) for s in scores]
            )
            raised = [jnp.exp(s - peak) for s in scores]
            total = sum(jnp.sum(e, axis=-1, keepdims=True) for e in raised)
            mixed = sum(nn(e.astype(HALF), v[...]) for e, v in zip(raised, v_refs))
            pieces.append(mixed / total)
            spot = lane == 2 * step + head
            logsum = jnp.broadcast_to(peak + jnp.log(total), (block, LANES))
            lse_acc[here, :] = jnp.where(spot, logsum, lse_acc[here, :])
        out_ref[here, :] = jnp.where(low, pieces[0], pieces[1]).astype(HALF)

    @pl.when(step == pl.num_programs(0) - 1)
    def _():
        lse_ref[...] = lse_acc[...].T


def attend(projected, others, width):
    rows = projected.shape[0]
    groups = 1 + len(others)
    tiles = width // LANES
    col = lambda base: pl.BlockSpec((rows, LANES), lambda i, base=base: (0, base + i))
    return pl.pallas_call(
        functools.partial(attend_kernel, groups),
        grid=(tiles,),
        out_shape=(
            jax.ShapeDtypeStruct((rows, width), HALF),
            jax.ShapeDtypeStruct((LANES, rows), F32),
        ),
        in_specs=[col(0), col(tiles)] + [col(0)] * len(others) + [col(2 * tiles)] + [col(tiles)] * len(others),
        out_specs=(col(0), pl.BlockSpec((LANES, rows), lambda i: (0, 0))),
        scratch_shapes=[pltpu.VMEM((rows, LANES), F32)],
        compiler_params=pltpu.CompilerParams(vmem_limit_bytes=48 << 20),
        name="attend",
    )(projected, projected, *others, projected, *others)


def attend_grad_kernel(groups, *refs):
    q_ref = refs[0]
    k_refs = refs[1 : 1 + groups]
    v_refs = refs[1 + groups : 1 + 2 * groups]
    do_ref, o_ref, lse_ref = refs[1 + 2 * groups : 4 + 2 * groups]
    dq_ref = refs[4 + 2 * groups]
    dk_refs = refs[5 + 2 * groups : 5 + 3 * groups]
    dv_refs = refs[5 + 3 * groups : 5 + 4 * groups]
    step = pl.program_id(0)
    rows = q_ref.shape[0]
    block = 256
    scale = HALF(HD**-0.5)
    q = q_ref[...] * scale
    grad = do_ref[...]
    product = grad.astype(F32) * o_ref[...].astype(F32)
    top = product.astype(HALF)
    rest = (product - top.astype(F32)).astype(HALF)
    pick = lax.broadcasted_iota(jnp.int32, (8, LANES), 0) == (
        lax.broadcasted_iota(jnp.int32, (8, LANES), 1) // HD
    )
    pick = jnp.where(pick, 1.0, 0.0).astype(HALF)
    inner = nt(pick, top) + nt(pick, rest)
    low = lax.broadcasted_iota(jnp.int32, (block, LANES), 1) < HD
    dq_t = [jnp.zeros((LANES, rows), F32) for _ in range(2)]
    for k_ref, v_ref, dk_ref, dv_ref in zip(k_refs, v_refs, dk_refs, dv_refs):
        for start in range(0, rows, block):
            here = pl.ds(start, block)
            k = k_ref[here, :]
            v = v_ref[here, :]
            k_t = k.T
            dks, dvs = [], []
            for head in range(2):
                own = low if head == 0 else jnp.logical_not(low)
                lse = lse_ref[pl.ds(2 * step + head, 1), :]
                scores = nt(jnp.where(own, k, jnp.zeros_like(k)), q)
                probs = jnp.exp(scores - lse)
                dvs.append(nn(probs.astype(HALF), grad))
                gp = nt(jnp.where(own, v, jnp.zeros_like(v)), grad)
                gs = (probs * (gp - inner[head : head + 1, :])).astype(HALF)
                dks.append(nn(gs, q))
                dq_t[head] = dq_t[head] + nn(k_t, gs)
            dk_ref[here, :] = jnp.where(low, dks[0], dks[1]).astype(HALF)
            dv_ref[here, :] = jnp.where(low, dvs[0], dvs[1]).astype(HALF)
    upper = lax.broadcasted_iota(jnp.int32, (LANES, rows), 0) < HD
    dq = jnp.where(upper, dq_t[0], dq_t[1]).T * HD**-0.5
    dq_ref[...] = dq.astype(HALF)


def attend_grad(projected, others, grad, attended, logsum, width):
    rows = projected.shape[0]
    groups = 1 + len(others)
    tiles = width // LANES
    col = lambda base: pl.BlockSpec((rows, LANES), lambda i, base=base: (0, base + i))
    out = jax.ShapeDtypeStruct((rows, width), HALF)
    return pl.pallas_call(
        functools.partial(attend_grad_kernel, groups),
        grid=(tiles,),
        out_shape=(out,) * (1 + 2 * groups),
        in_specs=[col(0), col(tiles)]
        + [col(0)] * len(others)
        + [col(2 * tiles)]
        + [col(tiles)] * len(others)
        + [col(0), col(0), pl.BlockSpec((LANES, rows), lambda i: (0, 0))],
        out_specs=(col(0),) * (1 + 2 * groups),
        compiler_params=pltpu.CompilerParams(vmem_limit_bytes=48 << 20),
        name="attend_grad",
    )(projected, projected, *others, projected, *others, grad, attended, logsum)


def norm_parts(rows):
    centred = rows - jnp.mean(rows, axis=-1, keepdims=True)
    variance = jnp.mean(centred * centred, axis=-1, keepdims=True)
    inverse = lax.rsqrt(variance + EPSILON)
    return centred * inverse, inverse


def norm_grad(grad, hat, inverse, scale):
    g = grad * (1.0 + scale)
    return (
        g
        - jnp.mean(g, axis=-1, keepdims=True)
        - hat * jnp.mean(g * hat, axis=-1, keepdims=True)
    ) * inverse


def gelu_tanh(inputs):
    return jax.nn.gelu(inputs, approximate=True)


def body(
    tokens,
    condition,
    ada_weight,
    ada_bias,
    qkv_weight,
    qv_bias,
    out_weight,
    out_bias,
    up_weight,
    up_bias,
    down_weight,
    down_bias,
    cotangent,
):
    lats, part, width = tokens.shape
    dp = lax.axis_size("dp")
    seq = lax.axis_size("seq")
    me = lax.axis_index("dp")
    z = lax.axis_index("seq")
    core = me % 2
    pair = me // 2
    chip_lats = 2 * lats
    sub = seq // chip_lats
    first = core == 0

    def flip(x):
        return lax.ppermute(x, "dp", [(i, i ^ 1) for i in range(dp)])

    def shift(x, by):
        if by % sub == 0:
            return x
        return lax.ppermute(
            x, "seq", [(i, i // sub * sub + (i - by) % sub) for i in range(seq)]
        )

    def spread(x):
        halves = x.reshape(lats, 2, part // 2, width)
        keep = lax.dynamic_index_in_dim(halves, core, 1, keepdims=False)
        give = lax.dynamic_index_in_dim(halves, 1 - core, 1, keepdims=False)
        got = flip(give)
        both = jnp.concatenate(
            [jnp.where(first, keep, got), jnp.where(first, got, keep)], axis=0
        )
        both = both.reshape(seq, part // (2 * sub), width)
        return lax.all_to_all(both, "seq", 0, 0, tiled=True).reshape(-1, width)

    def collect(x):
        both = x.reshape(seq, part // (2 * sub), width)
        both = lax.all_to_all(both, "seq", 0, 0, tiled=True)
        both = both.reshape(2, lats, part // 2, width)
        mine = lax.dynamic_index_in_dim(both, core, 0, keepdims=False)
        give = lax.dynamic_index_in_dim(both, 1 - core, 0, keepdims=False)
        got = flip(give)
        return jnp.stack(
            [jnp.where(first, mine, got), jnp.where(first, got, mine)], axis=1
        ).reshape(lats, part, width)

    small = jnp.concatenate(
        [ada_bias, qv_bias, out_bias, up_bias, down_bias, condition.reshape(-1)]
    )
    small_all = lax.all_gather(small, "dp", axis=0, tiled=False)
    sizes = [a.shape[0] for a in (ada_bias, qv_bias, out_bias, up_bias, down_bias)]
    cuts = [0]
    for size in sizes:
        cuts.append(cuts[-1] + size)
    ada_bias_full, qv_full, out_bias_full, up_bias_full, down_bias_full = [
        small_all[:, a:b].reshape(-1).astype(F32) for a, b in zip(cuts[:-1], cuts[1:])
    ]
    cond_all = small_all[:, cuts[-1] :].reshape(dp * lats, width).astype(F32)
    depth = ada_weight.shape[0]
    silu_all = jax.nn.silu(cond_all).astype(HALF)
    silu_mine = lax.dynamic_slice_in_dim(silu_all, me * depth, depth, axis=1)
    partial = nn(silu_mine, ada_weight)
    row_here = z // sub
    wanted = partial.reshape(dp // 2, chip_lats, 6 * width)
    wanted = lax.dynamic_index_in_dim(wanted, row_here, 1, keepdims=True)
    wanted = jnp.broadcast_to(wanted, (dp // 2, 2, 6 * width)).reshape(dp, 6 * width)
    modulation = lax.psum_scatter(wanted, "dp", scatter_dimension=0, tiled=True)[0]
    modulation = (modulation + ada_bias_full).reshape(6, 1, width)
    shift_a, scale_a, gate_a, shift_b, scale_b, gate_b = [modulation[i] for i in range(6)]

    qkv_full = lax.all_gather(qkv_weight, "dp", axis=0, tiled=True)
    out_full = lax.all_gather(out_weight, "dp", axis=0, tiled=True)
    up_full = lax.all_gather(up_weight, "dp", axis=0, tiled=True)
    down_full = lax.all_gather(down_weight, "dp", axis=0, tiled=True)

    rows = spread(tokens).astype(F32)
    cot = spread(cotangent).astype(F32)

    hat_a, inverse_a = norm_parts(rows)
    normed_a = (hat_a * (1.0 + scale_a) + shift_a).astype(HALF)
    bias_all = jnp.concatenate([qv_full[:width], jnp.zeros((width,), F32), qv_full[width:]])
    projected = (nn(normed_a, qkv_full) + bias_all).astype(HALF)
    kv = projected[:, width:]
    ways = [(a, s) for s in range(sub) for a in range(2)]
    others = [shift(flip(kv) if a else kv, s) for a, s in ways[1:]]
    attended, logsum = attend(projected, others, width)
    branch_a = nn(attended, out_full) + out_bias_full
    middle = rows + gate_a * branch_a
    hat_b, inverse_b = norm_parts(middle)
    normed_b = (hat_b * (1.0 + scale_b) + shift_b).astype(HALF)
    hidden_pre = nn(normed_b, up_full) + up_bias_full
    hidden = gelu_tanh(hidden_pre).astype(HALF)
    branch_b = nn(hidden, down_full) + down_bias_full
    output = collect((middle + gate_b * branch_b).astype(HALF))

    grad_gate_b = jnp.sum(cot * branch_b, axis=0)
    grad_branch_b = cot * gate_b
    down_bias_grad = jnp.sum(grad_branch_b, axis=0)
    grad_branch_half = grad_branch_b.astype(HALF)
    down_weight_grad = tn(hidden, grad_branch_half).astype(HALF)
    grad_hidden = nt(grad_branch_half, down_full)
    _, gelu_back = jax.vjp(gelu_tanh, hidden_pre)
    grad_pre = gelu_back(grad_hidden)[0]
    up_bias_grad = jnp.sum(grad_pre, axis=0)
    grad_pre_half = grad_pre.astype(HALF)
    up_weight_grad = tn(normed_b, grad_pre_half).astype(HALF)
    grad_normed_b = nt(grad_pre_half, up_full)
    grad_shift_b = jnp.sum(grad_normed_b, axis=0)
    grad_scale_b = jnp.sum(grad_normed_b * hat_b, axis=0)
    grad_middle = cot + norm_grad(grad_normed_b, hat_b, inverse_b, scale_b)
    grad_gate_a = jnp.sum(grad_middle * branch_a, axis=0)
    grad_branch_a = grad_middle * gate_a
    out_bias_grad = jnp.sum(grad_branch_a, axis=0)
    grad_branch_a_half = grad_branch_a.astype(HALF)
    out_weight_grad = tn(attended, grad_branch_a_half).astype(HALF)
    grad_attended = nt(grad_branch_a_half, out_full).astype(HALF)

    results = attend_grad(projected, others, grad_attended, attended, logsum, width)
    count = len(ways)
    grad_query = results[0]
    grad_keys = results[1 : 1 + count]
    grad_values = results[1 + count :]
    grad_kv = [jnp.concatenate([k, v], axis=1) for k, v in zip(grad_keys, grad_values)]
    total_kv = grad_kv[0].astype(F32)
    for (a, s), part_kv in zip(ways[1:], grad_kv[1:]):
        back = shift(part_kv, -s)
        total_kv = total_kv + (flip(back) if a else back).astype(F32)
    grad_projected = jnp.concatenate([grad_query, total_kv.astype(HALF)], axis=1)
    qkv_weight_grad = tn(normed_a, grad_projected).astype(HALF)
    grad_proj_float = grad_projected.astype(F32)
    qv_bias_grad = jnp.concatenate(
        [
            jnp.sum(grad_proj_float[:, :width], axis=0),
            jnp.sum(grad_proj_float[:, 2 * width :], axis=0),
        ]
    )
    grad_normed_a = nt(grad_projected, qkv_full)
    grad_shift_a = jnp.sum(grad_normed_a, axis=0)
    grad_scale_a = jnp.sum(grad_normed_a * hat_a, axis=0)
    grad_tokens = grad_middle + norm_grad(grad_normed_a, hat_a, inverse_a, scale_a)
    tokens_grad = collect(grad_tokens.astype(HALF)).astype(F32)

    grad_mod = jnp.concatenate(
        [grad_shift_a, grad_scale_a, grad_gate_a, grad_shift_b, grad_scale_b, grad_gate_b]
    )
    every = lax.all_gather(grad_mod, "seq", axis=0, tiled=False)
    every = lax.all_gather(every, "dp", axis=0, tiled=False)
    every = every.reshape(dp // 2, 2, chip_lats, sub, 6 * width).sum(axis=(1, 3))
    every = every.reshape(dp * lats, 6 * width)
    every_half = every.astype(HALF)
    ada_weight_grad = tn(silu_mine, every_half)
    bias_len = ada_bias.shape[0]
    ada_bias_grad = jnp.sum(
        lax.dynamic_slice_in_dim(every, me * bias_len, bias_len, axis=1), axis=0
    )
    cond_part = nt(every_half, ada_weight).reshape(dp, lats, depth)
    cond_part = lax.all_to_all(cond_part, "dp", 0, 0, tiled=True)
    cond_part = cond_part.transpose(1, 0, 2).reshape(lats, width)
    cond_float = condition.astype(F32)
    sigmoid_cond = jax.nn.sigmoid(cond_float)
    silu_slope = sigmoid_cond * (1.0 + cond_float * (1.0 - sigmoid_cond))
    condition_grad = silu_slope * cond_part

    def reduce_weight(grad):
        share = lax.psum_scatter(grad, "dp", scatter_dimension=0, tiled=True)
        return lax.psum(share, "seq").astype(F32)

    bias_parts = jnp.concatenate(
        [
            b.reshape(dp, -1)
            for b in (qv_bias_grad, out_bias_grad, up_bias_grad, down_bias_grad)
        ],
        axis=1,
    )
    bias_parts = lax.psum_scatter(bias_parts, "dp", scatter_dimension=0, tiled=True)
    bias_parts = lax.psum(bias_parts, "seq")[0]
    cuts = [c - sizes[0] for c in cuts[1:]]
    qv_g, ob_g, ub_g, db_g = [bias_parts[a:b] for a, b in zip(cuts[:-1], cuts[1:])]
    return (
        output,
        tokens_grad,
        condition_grad,
        ada_weight_grad,
        ada_bias_grad,
        reduce_weight(qkv_weight_grad),
        qv_g,
        reduce_weight(out_weight_grad),
        ob_g,
        reduce_weight(up_weight_grad),
        ub_g,
        reduce_weight(down_weight_grad),
        db_g,
    )


def solution(mesh):
    return jax.shard_map(
        body,
        mesh=mesh,
        in_specs=(
            P("dp", "seq", None),
            P("dp", None),
            P("dp", None),
            P("dp"),
            P("dp", None),
            P("dp"),
            P("dp", None),
            P("dp"),
            P("dp", None),
            P("dp"),
            P("dp", None),
            P("dp"),
            P("dp", "seq", None),
        ),
        out_specs=(
            P("dp", "seq", None),
            P("dp", "seq", None),
            P("dp", None),
            P("dp", None),
            P("dp"),
            P("dp", None),
            P("dp"),
            P("dp", None),
            P("dp"),
            P("dp", None),
            P("dp"),
            P("dp", None),
            P("dp"),
        ),
        check_vma=False,
    )
```

```python
import functools

import jax
import jax.numpy as jnp
from jax import lax
from jax.experimental import pallas as pl
from jax.experimental.pallas import tpu as pltpu
from jax.sharding import PartitionSpec as P

HD = 64
LANES = 128
EPSILON = 1e-06
HALF = jnp.bfloat16
F32 = jnp.float32


def nn(a, b):
    return jnp.dot(a, b, preferred_element_type=F32)


def nt(a, b):
    return lax.dot_general(a, b, (((1,), (1,)), ((), ())), preferred_element_type=F32)


def tn(a, b):
    return lax.dot_general(a, b, (((0,), (0,)), ((), ())), preferred_element_type=F32)


def attend_kernel(groups, *refs):
    q_ref = refs[0]
    k_refs = refs[1 : 1 + groups]
    v_refs = refs[1 + groups : 1 + 2 * groups]
    out_ref, lse_ref, lse_acc = refs[1 + 2 * groups :]
    step = pl.program_id(0)
    rows = q_ref.shape[0]
    block = 256
    low = lax.broadcasted_iota(jnp.int32, (block, LANES), 1) < HD
    lane = lax.broadcasted_iota(jnp.int32, (block, LANES), 1)
    for start in range(0, rows, block):
        here = pl.ds(start, block)
        q = q_ref[here, :] * HALF(HD**-0.5)
        pieces = []
        for head in range(2):
            own = low if head == 0 else jnp.logical_not(low)
            qm = jnp.where(own, q, jnp.zeros_like(q))
            scores = [nt(qm, k[...]) for k in k_refs]
            peak = functools.reduce(
                jnp.maximum, [jnp.max(s, axis=-1, keepdims=True) for s in scores]
            )
            raised = [jnp.exp(s - peak) for s in scores]
            total = sum(jnp.sum(e, axis=-1, keepdims=True) for e in raised)
            mixed = sum(nn(e.astype(HALF), v[...]) for e, v in zip(raised, v_refs))
            pieces.append(mixed / total)
            spot = lane == 2 * step + head
            logsum = jnp.broadcast_to(peak + jnp.log(total), (block, LANES))
            lse_acc[here, :] = jnp.where(spot, logsum, lse_acc[here, :])
        out_ref[here, :] = jnp.where(low, pieces[0], pieces[1]).astype(HALF)

    @pl.when(step == pl.num_programs(0) - 1)
    def _():
        lse_ref[...] = lse_acc[...].T


def attend(projected, others, width):
    rows = projected.shape[0]
    groups = 1 + len(others)
    tiles = width // LANES
    col = lambda base: pl.BlockSpec((rows, LANES), lambda i, base=base: (0, base + i))
    return pl.pallas_call(
        functools.partial(attend_kernel, groups),
        grid=(tiles,),
        out_shape=(
            jax.ShapeDtypeStruct((rows, width), HALF),
            jax.ShapeDtypeStruct((LANES, rows), F32),
        ),
        in_specs=[col(0), col(tiles)] + [col(0)] * len(others) + [col(2 * tiles)] + [col(tiles)] * len(others),
        out_specs=(col(0), pl.BlockSpec((LANES, rows), lambda i: (0, 0))),
        scratch_shapes=[pltpu.VMEM((rows, LANES), F32)],
        compiler_params=pltpu.CompilerParams(vmem_limit_bytes=48 << 20),
        name="attend",
    )(projected, projected, *others, projected, *others)


def attend_grad_kernel(groups, *refs):
    q_ref = refs[0]
    k_refs = refs[1 : 1 + groups]
    v_refs = refs[1 + groups : 1 + 2 * groups]
    do_ref, o_ref, lse_ref = refs[1 + 2 * groups : 4 + 2 * groups]
    dq_ref = refs[4 + 2 * groups]
    dk_refs = refs[5 + 2 * groups : 5 + 3 * groups]
    dv_refs = refs[5 + 3 * groups : 5 + 4 * groups]
    step = pl.program_id(0)
    rows = q_ref.shape[0]
    block = 256
    scale = HALF(HD**-0.5)
    q = q_ref[...] * scale
    grad = do_ref[...]
    product = grad.astype(F32) * o_ref[...].astype(F32)
    top = product.astype(HALF)
    rest = (product - top.astype(F32)).astype(HALF)
    pick = lax.broadcasted_iota(jnp.int32, (8, LANES), 0) == (
        lax.broadcasted_iota(jnp.int32, (8, LANES), 1) // HD
    )
    pick = jnp.where(pick, 1.0, 0.0).astype(HALF)
    inner = nt(pick, top) + nt(pick, rest)
    low = lax.broadcasted_iota(jnp.int32, (block, LANES), 1) < HD
    dq_t = [jnp.zeros((LANES, rows), F32) for _ in range(2)]
    for k_ref, v_ref, dk_ref, dv_ref in zip(k_refs, v_refs, dk_refs, dv_refs):
        for start in range(0, rows, block):
            here = pl.ds(start, block)
            k = k_ref[here, :]
            v = v_ref[here, :]
            k_t = k.T
            dks, dvs = [], []
            for head in range(2):
                own = low if head == 0 else jnp.logical_not(low)
                lse = lse_ref[pl.ds(2 * step + head, 1), :]
                scores = nt(jnp.where(own, k, jnp.zeros_like(k)), q)
                probs = jnp.exp(scores - lse)
                dvs.append(nn(probs.astype(HALF), grad))
                gp = nt(jnp.where(own, v, jnp.zeros_like(v)), grad)
                gs = (probs * (gp - inner[head : head + 1, :])).astype(HALF)
                dks.append(nn(gs, q))
                dq_t[head] = dq_t[head] + nn(k_t, gs)
            dk_ref[here, :] = jnp.where(low, dks[0], dks[1]).astype(HALF)
            dv_ref[here, :] = jnp.where(low, dvs[0], dvs[1]).astype(HALF)
    upper = lax.broadcasted_iota(jnp.int32, (LANES, rows), 0) < HD
    dq = jnp.where(upper, dq_t[0], dq_t[1]).T * HD**-0.5
    dq_ref[...] = dq.astype(HALF)


def attend_grad(projected, others, grad, attended, logsum, width):
    rows = projected.shape[0]
    groups = 1 + len(others)
    tiles = width // LANES
    col = lambda base: pl.BlockSpec((rows, LANES), lambda i, base=base: (0, base + i))
    out = jax.ShapeDtypeStruct((rows, width), HALF)
    return pl.pallas_call(
        functools.partial(attend_grad_kernel, groups),
        grid=(tiles,),
        out_shape=(out,) * (1 + 2 * groups),
        in_specs=[col(0), col(tiles)]
        + [col(0)] * len(others)
        + [col(2 * tiles)]
        + [col(tiles)] * len(others)
        + [col(0), col(0), pl.BlockSpec((LANES, rows), lambda i: (0, 0))],
        out_specs=(col(0),) * (1 + 2 * groups),
        compiler_params=pltpu.CompilerParams(vmem_limit_bytes=48 << 20),
        name="attend_grad",
    )(projected, projected, *others, projected, *others, grad, attended, logsum)


MESH_ID = pl.DeviceIdType.MESH
CHUNKS = 12


class Gather:
    SLOTS = 9

    def __init__(self, local, whole, send, recv):
        self.local, self.whole, self.send, self.recv = local, whole, send, recv
        self.d = lax.axis_index("dp")
        self.z = lax.axis_index("seq")
        self.depth = local.shape[1]
        self.pending = []

    def _peer(self, flip):
        return (jnp.bitwise_xor(self.d, flip), self.z)

    def _copy(self, chunk, slot, flip, block_flip, lo, size, own=False):
        row = jnp.bitwise_xor(self.d, block_flip) * self.depth + lo
        row = pl.multiple_of(row, 64)
        dst = self.whole.at[chunk, pl.ds(row, size), :]
        src = self.local.at[chunk] if own else dst
        return pltpu.make_async_remote_copy(
            src_ref=src,
            dst_ref=dst,
            send_sem=self.send.at[chunk, slot],
            recv_sem=self.recv.at[chunk, slot],
            device_id=self._peer(flip),
            device_id_type=MESH_ID,
        )

    def _start(self, *args, **kw):
        copy = self._copy(*args, **kw)
        copy.start()
        self.pending.append(copy)

    def _arrived(self, chunk, slot, block_flip, lo, size):
        self._copy(chunk, slot, 1, block_flip, lo, size).wait_recv()

    def begin(self, i):
        n = self.depth
        self._start(i, 0, 2, 0, 0, n, own=True)
        self._start(i, 1, 4, 0, 0, n, own=True)
        self._start(i, 2, 1, 0, 0, n, own=True)

    def relay(self, i):
        n, h = self.depth, self.depth // 2
        self._arrived(i, 0, 2, 0, n)
        self._start(i, 5, 4, 2, 0, h)
        self._arrived(i, 1, 4, 0, n)
        self._start(i, 6, 2, 4, h, h)
        self._start(i, 3, 1, 2, 0, n)
        self._start(i, 4, 1, 4, 0, n)

    def share(self, i):
        h = self.depth // 2
        self._arrived(i, 5, 6, 0, h)
        self._start(i, 7, 1, 6, 0, h)
        self._arrived(i, 6, 6, h, h)
        self._start(i, 8, 1, 6, h, h)

    def finish(self, i):
        n, h = self.depth, self.depth // 2
        self._arrived(i, 2, 1, 0, n)
        self._arrived(i, 3, 3, 0, n)
        self._arrived(i, 4, 5, 0, n)
        self._arrived(i, 7, 7, 0, h)
        self._arrived(i, 8, 7, h, h)

    def drain(self):
        for copy in self.pending:
            copy.wait_send()
        self.pending = []


def greet(peers):
    barrier = pltpu.get_barrier_semaphore()
    for peer in peers:
        pl.semaphore_signal(barrier, inc=1, device_id=peer, device_id_type=MESH_ID)
    pl.semaphore_wait(barrier, len(peers))


def gather_kernel(local, whole, send, recv, place):
    d, z = lax.axis_index("dp"), lax.axis_index("seq")
    greet([(jnp.bitwise_xor(d, f), z) for f in (1, 2, 4)])
    gather = Gather(local, whole, send, recv)
    puts = []
    for i in range(CHUNKS):
        row = pl.multiple_of(d * gather.depth, 128)
        put = pltpu.make_async_copy(
            local.at[i], whole.at[i, pl.ds(row, gather.depth), :], place.at[i]
        )
        put.start()
        puts.append(put)
    for t in range(CHUNKS + 4):
        if t < CHUNKS:
            gather.begin(t)
        if 0 <= t - 1 < CHUNKS:
            gather.relay(t - 1)
        if 0 <= t - 3 < CHUNKS:
            gather.share(t - 3)
        if 0 <= t - 4 < CHUNKS:
            gather.finish(t - 4)
    for put in puts:
        put.wait()
    gather.drain()


def gather_all(local):
    depth, cols = local.shape[1:]
    return pl.pallas_call(
        gather_kernel,
        out_shape=jax.ShapeDtypeStruct((CHUNKS, 8 * depth, cols), HALF),
        in_specs=[pl.BlockSpec(memory_space=pltpu.VMEM)],
        out_specs=pl.BlockSpec(memory_space=pl.ANY),
        scratch_shapes=[
            pltpu.SemaphoreType.DMA((CHUNKS, Gather.SLOTS)),
            pltpu.SemaphoreType.DMA((CHUNKS, Gather.SLOTS)),
            pltpu.SemaphoreType.DMA((CHUNKS,)),
        ],
        compiler_params=pltpu.CompilerParams(
            collective_id=1, has_side_effects=True, vmem_limit_bytes=32 << 20
        ),
        name="gather_all",
    )(local)


class Reduce:
    SLOTS = 8

    def __init__(self, bufs, sems):
        (self.own, self.rc, self.s, self.rx, self.ry, self.t, self.ry2, self.rx2, self.r, self.rz1, self.q, self.rz2, self.out) = bufs
        self.send, self.recv, self.load = sems
        self.d = lax.axis_index("dp")
        self.z = lax.axis_index("seq")
        self.c = self.d % 2
        self.x = self.d // 2 % 2
        self.y = self.d // 4
        self.h = self.z % 2
        self.depth = self.out.shape[1]
        self.cols = self.out.shape[2]
        self.pending = {}

    def _remote(self, i, slot, src, dst, peer):
        copy = pltpu.make_async_remote_copy(
            src_ref=src,
            dst_ref=dst,
            send_sem=self.send.at[i, slot],
            recv_sem=self.recv.at[i, slot],
            device_id=peer,
            device_id_type=MESH_ID,
        )
        copy.start()
        self.pending[(i, slot)] = copy

    def _plane(self, flip):
        return (jnp.bitwise_xor(self.d, flip), self.z)

    def _line(self, flip):
        return (self.d, jnp.bitwise_xor(self.z, flip))

    def sent(self, i, slot):
        self.pending.pop((i, slot)).wait_send()

    def arrived(self, i, slot):
        self.pending[(i, slot)].wait_recv()

    def begin(self, i, grads):
        self._remote(i, 0, grads.at[:, 1 - self.c], self.rc.at[i], self._plane(1))
        self.fetch = getattr(self, "fetch", {})
        copy = pltpu.make_async_copy(grads.at[:, self.c], self.own.at[i % 3], self.load.at[i % 3])
        copy.start()
        self.fetch[i] = copy

    def plane(self, i):
        slot, half = i % 3, self.cols // 2
        self.fetch.pop(i).wait()
        self.arrived(i, 0)
        if i >= 3:
            self.sent(i - 3, 1)
            self.sent(i - 3, 2)

        @pl.loop(0, 4)
        def _(k):
            self.s[slot, k] = (
                self.own[slot, k].astype(F32) + self.rc[i, k].astype(F32)
            ).astype(HALF)

        self._remote(
            i, 1, self.s.at[slot].reshape(2, 2, self.depth, self.cols).at[:, 1 - self.x, :, pl.ds(0, half)],
            self.rx.at[i], self._plane(2),
        )
        self._remote(
            i, 2, self.s.at[slot].reshape(2, 2, self.depth, self.cols).at[1 - self.y, :, :, pl.ds(half, half)],
            self.ry.at[i], self._plane(4),
        )

    def cross(self, i):
        slot, half = i % 3, self.cols // 2
        self.arrived(i, 1)
        self.arrived(i, 2)
        if i >= 3:
            self.sent(i - 3, 3)
            self.sent(i - 3, 4)
        for k in range(2):
            self.t[slot, 0, k] = (
                self.s[slot, 2 * k + self.x, :, pl.ds(0, half)].astype(F32)
                + self.rx[i, k].astype(F32)
            ).astype(HALF)
            self.t[slot, 1, k] = (
                self.s[slot, 2 * self.y + k, :, pl.ds(half, half)].astype(F32)
                + self.ry[i, k].astype(F32)
            ).astype(HALF)
        self._remote(i, 3, self.t.at[slot, 0, 1 - self.y], self.ry2.at[i], self._plane(4))
        self._remote(i, 4, self.t.at[slot, 1, 1 - self.x], self.rx2.at[i], self._plane(2))

    def line(self, i):
        slot, half = i % 3, self.cols // 2
        rows = self.depth // 2
        self.arrived(i, 3)
        self.arrived(i, 4)
        if i >= 3:
            self.sent(i - 3, 5)
        self.r[slot, :, pl.ds(0, half)] = (
            self.t[slot, 0, self.y].astype(F32) + self.ry2[i].astype(F32)
        ).astype(HALF)
        self.r[slot, :, pl.ds(half, half)] = (
            self.t[slot, 1, self.x].astype(F32) + self.rx2[i].astype(F32)
        ).astype(HALF)
        away = pl.multiple_of((1 - self.h) * rows, rows)
        self._remote(i, 5, self.r.at[slot, pl.ds(away, rows), :], self.rz1.at[i], self._line(1))

    def far(self, i):
        slot, rows = i % 3, self.depth // 2
        self.arrived(i, 5)
        if i >= 3:
            self.sent(i - 3, 6)
        mine = pl.multiple_of(self.h * rows, rows)
        self.q[slot] = (
            self.r[slot, pl.ds(mine, rows), :].astype(F32) + self.rz1[i].astype(F32)
        ).astype(HALF)
        self._remote(i, 6, self.q.at[slot], self.rz2.at[i], self._line(2))

    def close(self, i):
        slot, rows = i % 3, self.depth // 2
        self.arrived(i, 6)
        mine = pl.multiple_of(self.h * rows, rows)
        self.out[i, pl.ds(mine, rows), :] = (
            self.q[slot].astype(F32) + self.rz2[i].astype(F32)
        ).astype(HALF)
        here = self.out.at[i, pl.ds(mine, rows), :]
        self._remote(i, 7, here, here, self._line(1))

    def finish(self, i):
        self.arrived(i, 7)

    def drain(self):
        for copy in self.pending.values():
            copy.wait_send()
        self.pending = {}


REDUCE_LAG = (0, 1, 2, 4, 6, 8, 10)


def reduce_steps(red, grads_of, t):
    steps = (
        lambda i: red.begin(i, grads_of(i)),
        red.plane,
        red.cross,
        red.line,
        red.far,
        red.close,
        red.finish,
    )
    for lag, step in zip(REDUCE_LAG, steps):
        if 0 <= t - lag < CHUNKS:
            step(t - lag)


def reduce_kernel(grads, out, *scratch):
    d, z = lax.axis_index("dp"), lax.axis_index("seq")
    greet(
        [(jnp.bitwise_xor(d, f), z) for f in (1, 2, 4)]
        + [(d, jnp.bitwise_xor(z, f)) for f in (1, 2)]
    )
    red = Reduce(scratch[:12] + (out,), scratch[12:])
    for t in range(CHUNKS + REDUCE_LAG[-1]):
        reduce_steps(red, lambda i: grads.at[i], t)
    red.drain()


def reduce_scratch(depth, cols):
    half, rows = cols // 2, depth // 2
    ring = 3
    return [
        pltpu.VMEM((ring, 4, depth, cols), HALF),
        pltpu.VMEM((CHUNKS, 4, depth, cols), HALF),
        pltpu.VMEM((ring, 4, depth, cols), HALF),
        pltpu.VMEM((CHUNKS, 2, depth, half), HALF),
        pltpu.VMEM((CHUNKS, 2, depth, half), HALF),
        pltpu.VMEM((ring, 2, 2, depth, half), HALF),
        pltpu.VMEM((CHUNKS, depth, half), HALF),
        pltpu.VMEM((CHUNKS, depth, half), HALF),
        pltpu.VMEM((ring, depth, cols), HALF),
        pltpu.VMEM((CHUNKS, rows, cols), HALF),
        pltpu.VMEM((ring, rows, cols), HALF),
        pltpu.VMEM((CHUNKS, rows, cols), HALF),
        pltpu.SemaphoreType.DMA((CHUNKS, Reduce.SLOTS)),
        pltpu.SemaphoreType.DMA((CHUNKS, Reduce.SLOTS)),
        pltpu.SemaphoreType.DMA((ring,)),
    ]


def reduce_all(grads):
    depth, cols = grads.shape[-2:]
    return pl.pallas_call(
        reduce_kernel,
        out_shape=jax.ShapeDtypeStruct((CHUNKS, depth, cols), HALF),
        in_specs=[pl.BlockSpec(memory_space=pl.ANY)],
        out_specs=pl.BlockSpec(memory_space=pltpu.VMEM),
        scratch_shapes=reduce_scratch(depth, cols),
        compiler_params=pltpu.CompilerParams(
            collective_id=2, has_side_effects=True, vmem_limit_bytes=58 << 20
        ),
        name="reduce_all",
    )(grads)


def norm_parts(rows):
    centred = rows - jnp.mean(rows, axis=-1, keepdims=True)
    variance = jnp.mean(centred * centred, axis=-1, keepdims=True)
    inverse = lax.rsqrt(variance + EPSILON)
    return centred * inverse, inverse


def norm_grad(grad, hat, inverse, scale):
    g = grad * (1.0 + scale)
    return (
        g
        - jnp.mean(g, axis=-1, keepdims=True)
        - hat * jnp.mean(g * hat, axis=-1, keepdims=True)
    ) * inverse


def gelu_tanh(inputs):
    return jax.nn.gelu(inputs, approximate=True)


def body(
    tokens,
    condition,
    ada_weight,
    ada_bias,
    qkv_weight,
    qv_bias,
    out_weight,
    out_bias,
    up_weight,
    up_bias,
    down_weight,
    down_bias,
    cotangent,
):
    lats, part, width = tokens.shape
    dp = lax.axis_size("dp")
    seq = lax.axis_size("seq")
    me = lax.axis_index("dp")
    z = lax.axis_index("seq")
    core = me % 2
    pair = me // 2
    chip_lats = 2 * lats
    sub = seq // chip_lats
    first = core == 0

    def flip(x):
        return lax.ppermute(x, "dp", [(i, i ^ 1) for i in range(dp)])

    def shift(x, by):
        if by % sub == 0:
            return x
        return lax.ppermute(
            x, "seq", [(i, i // sub * sub + (i - by) % sub) for i in range(seq)]
        )

    def spread(x):
        halves = x.reshape(lats, 2, part // 2, width)
        keep = lax.dynamic_index_in_dim(halves, core, 1, keepdims=False)
        give = lax.dynamic_index_in_dim(halves, 1 - core, 1, keepdims=False)
        got = flip(give)
        both = jnp.concatenate(
            [jnp.where(first, keep, got), jnp.where(first, got, keep)], axis=0
        )
        both = both.reshape(seq, part // (2 * sub), width)
        return lax.all_to_all(both, "seq", 0, 0, tiled=True).reshape(-1, width)

    def collect(x):
        both = x.reshape(seq, part // (2 * sub), width)
        both = lax.all_to_all(both, "seq", 0, 0, tiled=True)
        both = both.reshape(2, lats, part // 2, width)
        mine = lax.dynamic_index_in_dim(both, core, 0, keepdims=False)
        give = lax.dynamic_index_in_dim(both, 1 - core, 0, keepdims=False)
        got = flip(give)
        return jnp.stack(
            [jnp.where(first, mine, got), jnp.where(first, got, mine)], axis=1
        ).reshape(lats, part, width)

    small = jnp.concatenate(
        [ada_bias, qv_bias, out_bias, up_bias, down_bias, condition.reshape(-1)]
    )
    small_all = lax.all_gather(small, "dp", axis=0, tiled=False)
    sizes = [a.shape[0] for a in (ada_bias, qv_bias, out_bias, up_bias, down_bias)]
    cuts = [0]
    for size in sizes:
        cuts.append(cuts[-1] + size)
    ada_bias_full, qv_full, out_bias_full, up_bias_full, down_bias_full = [
        small_all[:, a:b].reshape(-1).astype(F32) for a, b in zip(cuts[:-1], cuts[1:])
    ]
    cond_all = small_all[:, cuts[-1] :].reshape(dp * lats, width).astype(F32)
    depth = ada_weight.shape[0]
    silu_all = jax.nn.silu(cond_all).astype(HALF)
    silu_mine = lax.dynamic_slice_in_dim(silu_all, me * depth, depth, axis=1)
    partial = nn(silu_mine, ada_weight)
    row_here = z // sub
    wanted = partial.reshape(dp // 2, chip_lats, 6 * width)
    wanted = lax.dynamic_index_in_dim(wanted, row_here, 1, keepdims=True)
    wanted = jnp.broadcast_to(wanted, (dp // 2, 2, 6 * width)).reshape(dp, 6 * width)
    modulation = lax.psum_scatter(wanted, "dp", scatter_dimension=0, tiled=True)[0]
    modulation = (modulation + ada_bias_full).reshape(6, 1, width)
    shift_a, scale_a, gate_a, shift_b, scale_b, gate_b = [modulation[i] for i in range(6)]

    own = dp == 8 and seq == 4 and lats == 2
    wide = up_bias.shape[0] * dp
    if own:
        cut = wide // (4 * dp)
        local = jnp.concatenate(
            [
                qkv_weight.reshape(depth, 3, width).transpose(1, 0, 2),
                out_weight[None],
                up_weight.reshape(depth, dp, 4, cut).transpose(2, 0, 1, 3).reshape(4, depth, width),
                down_weight.reshape(4, cut, width),
            ],
            axis=0,
        )
        whole = gather_all(local)
        qkv_full = whole[:3].transpose(1, 0, 2).reshape(width, 3 * width)
        out_full = whole[3]
        up_full = whole[4:8].transpose(1, 0, 2).reshape(width, wide)
        down_full = whole[8:].reshape(wide, width)
        up_bias_full = up_bias_full.reshape(dp, 4, cut).transpose(1, 0, 2).reshape(-1)
    else:
        qkv_full = lax.all_gather(qkv_weight, "dp", axis=0, tiled=True)
        out_full = lax.all_gather(out_weight, "dp", axis=0, tiled=True)
        up_full = lax.all_gather(up_weight, "dp", axis=0, tiled=True)
        down_full = lax.all_gather(down_weight, "dp", axis=0, tiled=True)

    rows = spread(tokens).astype(F32)
    cot = spread(cotangent).astype(F32)

    hat_a, inverse_a = norm_parts(rows)
    normed_a = (hat_a * (1.0 + scale_a) + shift_a).astype(HALF)
    bias_all = jnp.concatenate([qv_full[:width], jnp.zeros((width,), F32), qv_full[width:]])
    projected = (nn(normed_a, qkv_full) + bias_all).astype(HALF)
    kv = projected[:, width:]
    ways = [(a, s) for s in range(sub) for a in range(2)]
    others = [shift(flip(kv) if a else kv, s) for a, s in ways[1:]]
    attended, logsum = attend(projected, others, width)
    branch_a = nn(attended, out_full) + out_bias_full
    middle = rows + gate_a * branch_a
    hat_b, inverse_b = norm_parts(middle)
    normed_b = (hat_b * (1.0 + scale_b) + shift_b).astype(HALF)
    hidden_pre = nn(normed_b, up_full) + up_bias_full
    hidden = gelu_tanh(hidden_pre).astype(HALF)
    branch_b = nn(hidden, down_full) + down_bias_full
    output = collect((middle + gate_b * branch_b).astype(HALF))

    grad_gate_b = jnp.sum(cot * branch_b, axis=0)
    grad_branch_b = cot * gate_b
    down_bias_grad = jnp.sum(grad_branch_b, axis=0)
    grad_branch_half = grad_branch_b.astype(HALF)
    down_weight_grad = tn(hidden, grad_branch_half).astype(HALF)
    grad_hidden = nt(grad_branch_half, down_full)
    _, gelu_back = jax.vjp(gelu_tanh, hidden_pre)
    grad_pre = gelu_back(grad_hidden)[0]
    up_bias_grad = jnp.sum(grad_pre, axis=0)
    grad_pre_half = grad_pre.astype(HALF)
    up_weight_grad = tn(normed_b, grad_pre_half).astype(HALF)
    grad_normed_b = nt(grad_pre_half, up_full)
    grad_shift_b = jnp.sum(grad_normed_b, axis=0)
    grad_scale_b = jnp.sum(grad_normed_b * hat_b, axis=0)
    grad_middle = cot + norm_grad(grad_normed_b, hat_b, inverse_b, scale_b)
    grad_gate_a = jnp.sum(grad_middle * branch_a, axis=0)
    grad_branch_a = grad_middle * gate_a
    out_bias_grad = jnp.sum(grad_branch_a, axis=0)
    grad_branch_a_half = grad_branch_a.astype(HALF)
    out_weight_grad = tn(attended, grad_branch_a_half).astype(HALF)
    grad_attended = nt(grad_branch_a_half, out_full).astype(HALF)

    results = attend_grad(projected, others, grad_attended, attended, logsum, width)
    count = len(ways)
    grad_query = results[0]
    grad_keys = results[1 : 1 + count]
    grad_values = results[1 + count :]
    grad_kv = [jnp.concatenate([k, v], axis=1) for k, v in zip(grad_keys, grad_values)]
    total_kv = grad_kv[0].astype(F32)
    for (a, s), part_kv in zip(ways[1:], grad_kv[1:]):
        back = shift(part_kv, -s)
        total_kv = total_kv + (flip(back) if a else back).astype(F32)
    grad_projected = jnp.concatenate([grad_query, total_kv.astype(HALF)], axis=1)
    qkv_weight_grad = tn(normed_a, grad_projected).astype(HALF)
    grad_proj_float = grad_projected.astype(F32)
    qv_bias_grad = jnp.concatenate(
        [
            jnp.sum(grad_proj_float[:, :width], axis=0),
            jnp.sum(grad_proj_float[:, 2 * width :], axis=0),
        ]
    )
    grad_normed_a = nt(grad_projected, qkv_full)
    grad_shift_a = jnp.sum(grad_normed_a, axis=0)
    grad_scale_a = jnp.sum(grad_normed_a * hat_a, axis=0)
    grad_tokens = grad_middle + norm_grad(grad_normed_a, hat_a, inverse_a, scale_a)
    tokens_grad = collect(grad_tokens.astype(HALF)).astype(F32)

    grad_mod = jnp.concatenate(
        [grad_shift_a, grad_scale_a, grad_gate_a, grad_shift_b, grad_scale_b, grad_gate_b]
    )
    every = lax.all_gather(grad_mod, "seq", axis=0, tiled=False)
    every = lax.all_gather(every, "dp", axis=0, tiled=False)
    every = every.reshape(dp // 2, 2, chip_lats, sub, 6 * width).sum(axis=(1, 3))
    every = every.reshape(dp * lats, 6 * width)
    every_half = every.astype(HALF)
    ada_weight_grad = tn(silu_mine, every_half)
    bias_len = ada_bias.shape[0]
    ada_bias_grad = jnp.sum(
        lax.dynamic_slice_in_dim(every, me * bias_len, bias_len, axis=1), axis=0
    )
    cond_part = nt(every_half, ada_weight).reshape(dp, lats, depth)
    cond_part = lax.all_to_all(cond_part, "dp", 0, 0, tiled=True)
    cond_part = cond_part.transpose(1, 0, 2).reshape(lats, width)
    cond_float = condition.astype(F32)
    sigmoid_cond = jax.nn.sigmoid(cond_float)
    silu_slope = sigmoid_cond * (1.0 + cond_float * (1.0 - sigmoid_cond))
    condition_grad = silu_slope * cond_part

    def reduce_weight(grad):
        share = lax.psum_scatter(grad, "dp", scatter_dimension=0, tiled=True)
        return lax.psum(share, "seq").astype(F32)

    if own:
        up_bias_grad = up_bias_grad.reshape(4, dp, cut).transpose(1, 0, 2).reshape(-1)
        grads = jnp.concatenate(
            [
                qkv_weight_grad.reshape(width, 3, width).transpose(1, 0, 2),
                out_weight_grad[None],
                up_weight_grad.reshape(width, 4, width).transpose(1, 0, 2),
                down_weight_grad.reshape(4, width, width),
            ],
            axis=0,
        )
        shares = reduce_all(grads.reshape(CHUNKS, dp // 2, 2, depth, width)).astype(F32)
        qkv_g = shares[:3].transpose(1, 0, 2).reshape(depth, 3 * width)
        out_g = shares[3]
        up_g = shares[4:8].reshape(4, depth, dp, cut).transpose(1, 2, 0, 3).reshape(depth, wide)
        down_g = shares[8:].reshape(4 * cut, width)
    else:
        qkv_g, out_g, up_g, down_g = map(
            reduce_weight, (qkv_weight_grad, out_weight_grad, up_weight_grad, down_weight_grad)
        )

    bias_parts = jnp.concatenate(
        [
            b.reshape(dp, -1)
            for b in (qv_bias_grad, out_bias_grad, up_bias_grad, down_bias_grad)
        ],
        axis=1,
    )
    bias_parts = lax.psum_scatter(bias_parts, "dp", scatter_dimension=0, tiled=True)
    bias_parts = lax.psum(bias_parts, "seq")[0]
    cuts = [c - sizes[0] for c in cuts[1:]]
    qv_g, ob_g, ub_g, db_g = [bias_parts[a:b] for a, b in zip(cuts[:-1], cuts[1:])]
    return (
        output,
        tokens_grad,
        condition_grad,
        ada_weight_grad,
        ada_bias_grad,
        qkv_g,
        qv_g,
        out_g,
        ob_g,
        up_g,
        ub_g,
        down_g,
        db_g,
    )


def solution(mesh):
    return jax.shard_map(
        body,
        mesh=mesh,
        in_specs=(
            P("dp", "seq", None),
            P("dp", None),
            P("dp", None),
            P("dp"),
            P("dp", None),
            P("dp"),
            P("dp", None),
            P("dp"),
            P("dp", None),
            P("dp"),
            P("dp", None),
            P("dp"),
            P("dp", "seq", None),
        ),
        out_specs=(
            P("dp", "seq", None),
            P("dp", "seq", None),
            P("dp", None),
            P("dp", None),
            P("dp"),
            P("dp", None),
            P("dp"),
            P("dp", None),
            P("dp"),
            P("dp", None),
            P("dp"),
            P("dp", None),
            P("dp"),
        ),
        check_vma=False,
    )
```

```python
import functools

import jax
import jax.numpy as jnp
from jax import lax
from jax.experimental import pallas as pl
from jax.experimental.pallas import tpu as pltpu
from jax.sharding import PartitionSpec as P

HD = 64
LANES = 128
EPSILON = 1e-06
HALF = jnp.bfloat16
F32 = jnp.float32


def nn(a, b):
    return jnp.dot(a, b, preferred_element_type=F32)


def nt(a, b):
    return lax.dot_general(a, b, (((1,), (1,)), ((), ())), preferred_element_type=F32)


def tn(a, b):
    return lax.dot_general(a, b, (((0,), (0,)), ((), ())), preferred_element_type=F32)


def attend_kernel(groups, *refs):
    q_ref = refs[0]
    k_refs = refs[1 : 1 + groups]
    v_refs = refs[1 + groups : 1 + 2 * groups]
    out_ref, lse_ref, lse_acc = refs[1 + 2 * groups :]
    step = pl.program_id(0)
    rows = q_ref.shape[0]
    block = 256
    low = lax.broadcasted_iota(jnp.int32, (block, LANES), 1) < HD
    lane = lax.broadcasted_iota(jnp.int32, (block, LANES), 1)
    for start in range(0, rows, block):
        here = pl.ds(start, block)
        q = q_ref[here, :] * HALF(HD**-0.5)
        pieces = []
        for head in range(2):
            own = low if head == 0 else jnp.logical_not(low)
            qm = jnp.where(own, q, jnp.zeros_like(q))
            scores = [nt(qm, k[...]) for k in k_refs]
            peak = functools.reduce(
                jnp.maximum, [jnp.max(s, axis=-1, keepdims=True) for s in scores]
            )
            raised = [jnp.exp(s - peak) for s in scores]
            total = sum(jnp.sum(e, axis=-1, keepdims=True) for e in raised)
            mixed = sum(nn(e.astype(HALF), v[...]) for e, v in zip(raised, v_refs))
            pieces.append(mixed / total)
            spot = lane == 2 * step + head
            logsum = jnp.broadcast_to(peak + jnp.log(total), (block, LANES))
            lse_acc[here, :] = jnp.where(spot, logsum, lse_acc[here, :])
        out_ref[here, :] = jnp.where(low, pieces[0], pieces[1]).astype(HALF)

    @pl.when(step == pl.num_programs(0) - 1)
    def _():
        lse_ref[...] = lse_acc[...].T


def attend(projected, others, width):
    rows = projected.shape[0]
    groups = 1 + len(others)
    tiles = width // LANES
    col = lambda base: pl.BlockSpec((rows, LANES), lambda i, base=base: (0, base + i))
    return pl.pallas_call(
        functools.partial(attend_kernel, groups),
        grid=(tiles,),
        out_shape=(
            jax.ShapeDtypeStruct((rows, width), HALF),
            jax.ShapeDtypeStruct((LANES, rows), F32),
        ),
        in_specs=[col(0), col(tiles)] + [col(0)] * len(others) + [col(2 * tiles)] + [col(tiles)] * len(others),
        out_specs=(col(0), pl.BlockSpec((LANES, rows), lambda i: (0, 0))),
        scratch_shapes=[pltpu.VMEM((rows, LANES), F32)],
        compiler_params=pltpu.CompilerParams(vmem_limit_bytes=48 << 20),
        name="attend",
    )(projected, projected, *others, projected, *others)


def attend_grad_kernel(groups, *refs):
    q_ref = refs[0]
    k_refs = refs[1 : 1 + groups]
    v_refs = refs[1 + groups : 1 + 2 * groups]
    do_ref, o_ref, lse_ref = refs[1 + 2 * groups : 4 + 2 * groups]
    dq_ref = refs[4 + 2 * groups]
    dk_refs = refs[5 + 2 * groups : 5 + 3 * groups]
    dv_refs = refs[5 + 3 * groups : 5 + 4 * groups]
    step = pl.program_id(0)
    rows = q_ref.shape[0]
    block = 256
    scale = HALF(HD**-0.5)
    q = q_ref[...] * scale
    grad = do_ref[...]
    product = grad.astype(F32) * o_ref[...].astype(F32)
    top = product.astype(HALF)
    rest = (product - top.astype(F32)).astype(HALF)
    pick = lax.broadcasted_iota(jnp.int32, (8, LANES), 0) == (
        lax.broadcasted_iota(jnp.int32, (8, LANES), 1) // HD
    )
    pick = jnp.where(pick, 1.0, 0.0).astype(HALF)
    inner = nt(pick, top) + nt(pick, rest)
    low = lax.broadcasted_iota(jnp.int32, (block, LANES), 1) < HD
    dq_t = [jnp.zeros((LANES, rows), F32) for _ in range(2)]
    for k_ref, v_ref, dk_ref, dv_ref in zip(k_refs, v_refs, dk_refs, dv_refs):
        for start in range(0, rows, block):
            here = pl.ds(start, block)
            k = k_ref[here, :]
            v = v_ref[here, :]
            k_t = k.T
            dks, dvs = [], []
            for head in range(2):
                own = low if head == 0 else jnp.logical_not(low)
                lse = lse_ref[pl.ds(2 * step + head, 1), :]
                scores = nt(jnp.where(own, k, jnp.zeros_like(k)), q)
                probs = jnp.exp(scores - lse)
                dvs.append(nn(probs.astype(HALF), grad))
                gp = nt(jnp.where(own, v, jnp.zeros_like(v)), grad)
                gs = (probs * (gp - inner[head : head + 1, :])).astype(HALF)
                dks.append(nn(gs, q))
                dq_t[head] = dq_t[head] + nn(k_t, gs)
            dk_ref[here, :] = jnp.where(low, dks[0], dks[1]).astype(HALF)
            dv_ref[here, :] = jnp.where(low, dvs[0], dvs[1]).astype(HALF)
    upper = lax.broadcasted_iota(jnp.int32, (LANES, rows), 0) < HD
    dq = jnp.where(upper, dq_t[0], dq_t[1]).T * HD**-0.5
    dq_ref[...] = dq.astype(HALF)


def attend_grad(projected, others, grad, attended, logsum, width):
    rows = projected.shape[0]
    groups = 1 + len(others)
    tiles = width // LANES
    col = lambda base: pl.BlockSpec((rows, LANES), lambda i, base=base: (0, base + i))
    out = jax.ShapeDtypeStruct((rows, width), HALF)
    return pl.pallas_call(
        functools.partial(attend_grad_kernel, groups),
        grid=(tiles,),
        out_shape=(out,) * (1 + 2 * groups),
        in_specs=[col(0), col(tiles)]
        + [col(0)] * len(others)
        + [col(2 * tiles)]
        + [col(tiles)] * len(others)
        + [col(0), col(0), pl.BlockSpec((LANES, rows), lambda i: (0, 0))],
        out_specs=(col(0),) * (1 + 2 * groups),
        compiler_params=pltpu.CompilerParams(vmem_limit_bytes=48 << 20),
        name="attend_grad",
    )(projected, projected, *others, projected, *others, grad, attended, logsum)


def norm_parts(rows):
    centred = rows - jnp.mean(rows, axis=-1, keepdims=True)
    variance = jnp.mean(centred * centred, axis=-1, keepdims=True)
    inverse = lax.rsqrt(variance + EPSILON)
    return centred * inverse, inverse


def norm_grad(grad, hat, inverse, scale):
    g = grad * (1.0 + scale)
    return (
        g
        - jnp.mean(g, axis=-1, keepdims=True)
        - hat * jnp.mean(g * hat, axis=-1, keepdims=True)
    ) * inverse


def gelu_tanh(inputs):
    return jax.nn.gelu(inputs, approximate=True)


MESH_ID = pl.DeviceIdType.MESH
CHUNKS = 12
KEYS, VALUES, QUERIES, OUT, FEED = 0, 1, 2, 3, 4


def guarded(low, value, high, run):
    if isinstance(value, int):
        if low <= value < high:
            run(value)
        return

    @pl.when(jnp.logical_and(value >= low, value < high))
    def _():
        run(value)


class Place:
    def __init__(self):
        self.d = lax.axis_index("dp")
        self.z = lax.axis_index("seq")
        self.c = self.d % 2
        self.x = self.d // 2 % 2
        self.y = self.d // 4
        self.p = self.d // 2

    def plane(self, flip):
        return (jnp.bitwise_xor(self.d, flip), self.z)

    def line(self, flip):
        return (self.d, jnp.bitwise_xor(self.z, flip))


def remote(src, dst, send, recv, peer):
    return pltpu.make_async_remote_copy(
        src_ref=src,
        dst_ref=dst,
        send_sem=send,
        recv_sem=recv,
        device_id=peer,
        device_id_type=MESH_ID,
    )


def greet(peers):
    barrier = pltpu.get_barrier_semaphore()
    for peer in peers:
        pl.semaphore_signal(barrier, inc=1, device_id=peer, device_id_type=MESH_ID)
    pl.semaphore_wait(barrier, len(peers))


class Gather:
    SENDS = (
        (2, 0, None),
        (4, 0, None),
        (1, 0, None),
        (1, 2, None),
        (1, 4, None),
        (4, 2, 0),
        (2, 4, 1),
        (1, 6, 0),
        (1, 6, 1),
    )

    def __init__(self, here, whole, send, recv):
        self.here, self.whole, self.send, self.recv = here, whole, send, recv
        self.depth = whole.shape[1] // 8

    def _block(self, chunk, flip, half):
        size = self.depth if half is None else self.depth // 2
        lo = 0 if half is None else half * size
        row = pl.multiple_of(jnp.bitwise_xor(self.here.d, flip) * self.depth + lo, 64)
        return self.whole.at[chunk, pl.ds(row, size), :]

    def _copy(self, chunk, slot, arriving=False):
        flip, block, half = self.SENDS[slot]
        ref = self._block(chunk, jnp.bitwise_xor(flip, block) if arriving else block, half)
        return remote(
            ref, ref, self.send.at[chunk, slot], self.recv.at[chunk, slot], self.here.plane(flip)
        )

    def begin(self, i):
        for slot in (0, 1, 2):
            self._copy(i, slot).start()

    def relay(self, i):
        self._copy(i, 0, True).wait_recv()
        self._copy(i, 5).start()
        self._copy(i, 1, True).wait_recv()
        self._copy(i, 6).start()
        self._copy(i, 3).start()
        self._copy(i, 4).start()

    def share(self, i):
        self._copy(i, 5, True).wait_recv()
        self._copy(i, 7).start()
        self._copy(i, 6, True).wait_recv()
        self._copy(i, 8).start()

    def finish(self, i):
        for slot in (2, 3, 4, 7, 8):
            self._copy(i, slot, True).wait_recv()

    def tick(self, t, prepare):
        def begin(i):
            prepare(i)
            self.begin(i)

        guarded(0, t, CHUNKS, begin)
        guarded(0, t - 2, CHUNKS, self.relay)
        guarded(0, t - 3, CHUNKS, self.share)
        guarded(0, t - 4, CHUNKS, self.finish)

    def drain(self):
        @pl.loop(0, CHUNKS)
        def _(i):
            for slot in range(len(self.SENDS)):
                self._copy(i, slot).wait_send()


class Spread:
    def __init__(self, here, source, landing, send, recv):
        self.here, self.source, self.landing = here, source, landing
        self.send, self.recv = send, recv
        self.size = source.shape[1] // 2

    def _each(self):
        here = self.here
        lats = self.source.shape[0]
        for j in range(lats):
            for core in range(2):
                z = lats * here.c + j
                own = jnp.logical_and(z == here.z, core == here.c)
                src = self.source.at[j, pl.ds(core * self.size, self.size), :]
                peer = (here.d - here.c + core, z)
                yield own, j * 2 + core, src, peer

    def _land(self, z):
        return self.landing.at[pl.ds(pl.multiple_of(z * self.size, self.size), self.size), :]

    def start(self):
        z = self.here.z
        for own, index, src, peer in self._each():

            @pl.when(own)
            def _():
                pltpu.make_async_copy(src, self._land(z), self.recv.at[z]).start()

            @pl.when(jnp.logical_not(own))
            def _():
                remote(src, self._land(z), self.send.at[index], self.recv.at[z], peer).start()

    def wait(self):
        src = self.source.at[0, pl.ds(0, self.size), :]
        for z in range(4):
            pltpu.make_async_copy(src, self._land(z), self.recv.at[z]).wait()

    def drain(self):
        z = self.here.z
        for own, index, src, peer in self._each():

            @pl.when(jnp.logical_not(own))
            def _():
                remote(src, self._land(z), self.send.at[index], self.recv.at[z], peer).wait_send()


def gelu_both(v):
    root = 0.7978845608028654
    square = v * v
    t = jnp.tanh(root * (v + 0.044715 * (v * square)))
    half = 0.5 * (1.0 + t)
    slope = half + (0.5 * root) * v * (1.0 - t * t) * (1.0 + (3 * 0.044715) * square)
    return half * v, slope


def column_sum(x):
    return jnp.sum(x, axis=0, keepdims=True)


FORWARD_OUTS = (
    "whole",
    "xs",
    "cots",
    "qkv",
    "kvo",
    "att",
    "lse",
    "mid",
    "bra",
    "nb",
    "hid",
    "gph",
    "bb",
    "gnb",
    "vec",
    "silu",
    "ups",
)


def forward_kernel(tokens, cot, qkv_w, out_w, up_w, down_w, small, ada, *refs):
    outs = dict(zip(FORWARD_OUTS, refs))
    (
        w,
        small_all,
        part,
        mod_in,
        mod,
        vec,
        silu,
        xs,
        ct,
        na,
        qkv,
        kvo,
        att,
        lse_acc,
        lse,
        mid,
        bra,
        nb,
        gbh,
        bb,
        gnb,
        hid,
        gph,
        ups,
        g_send,
        g_recv,
        own_sem,
        sp_send,
        sp_recv,
        sm_send,
        sm_recv,
        md_send,
        md_recv,
        kv_send,
        kv_recv,
        out_sem,
        ff_sem,
    ) = refs[len(FORWARD_OUTS) :]
    here = Place()
    d, z, c = here.d, here.z, here.c
    depth, width = qkv_w.shape[0], out_w.shape[1]
    rows = xs.shape[0]
    wide = up_w.shape[1]
    cut = wide // 32
    tile = 256

    mine = pl.ds(pl.multiple_of(d * depth, depth), depth)
    for i, k in ((KEYS, 1), (VALUES, 2), (QUERIES, 0)):
        pltpu.make_async_copy(
            qkv_w.at[:, pl.ds(k * width, width)], w.at[i, mine, :], own_sem.at[i]
        ).start()
    pltpu.make_async_copy(out_w, w.at[OUT, mine, :], own_sem.at[OUT]).start()
    for j in range(4):
        for k in range(8):
            pltpu.make_async_copy(
                up_w.at[:, pl.ds((4 * k + j) * cut, cut)],
                w.at[FEED + 2 * j, mine, pl.ds(k * cut, cut)],
                own_sem.at[FEED + 2 * j],
            ).start()
        pltpu.make_async_copy(
            down_w.at[pl.ds(j * depth, depth), :], w.at[FEED + 2 * j + 1, mine, :], own_sem.at[FEED + 2 * j + 1]
        ).start()

    def prepare(i):
        pltpu.make_async_copy(out_w, w.at[i, mine, :], own_sem.at[i]).wait()

    peers = [here.plane(f) for f in range(1, 8)]
    for core in range(2):
        for f in range(1, 4):
            peers.append((d - c + core, jnp.bitwise_xor(z, f)))
    greet(peers)

    gather = Gather(here, w, g_send, g_recv)
    tick = functools.partial(gather.tick, prepare=prepare)
    first = Spread(here, tokens, xs, sp_send.at[0], sp_recv.at[0])
    second = Spread(here, cot, ct, sp_send.at[1], sp_recv.at[1])

    def small_copy(f):
        dst = small_all.at[d]
        return remote(small, dst, sm_send.at[f - 1], sm_recv.at[f - 1], here.plane(f))

    for f in range(1, 8):
        small_copy(f).start()
    first.start()
    tick(0)
    tick(1)
    second.start()
    small_all[d] = small[...]
    for f in range(1, 8):
        small_copy(f).wait_recv()

    picked = [
        small_all[i // 2, pl.ds(16 + 8 * (i % 2) + d, 1), :] for i in range(16)
    ]
    cond = jnp.concatenate(picked, axis=0)
    silu[...] = (cond * jax.nn.sigmoid(cond)).astype(HALF)
    for i in range(6):
        product = nn(silu[...], ada[:, pl.ds(i * width, width)])
        for k in range(8):
            part[:, 8 * i + k, :] = product[:, k * LANES : (k + 1) * LANES]

    def mod_copy(f):
        flip = jnp.bitwise_xor(d, f)
        src = part.at[4 * (flip // 2) + z]
        return remote(src, mod_in.at[d], md_send.at[f - 1], md_recv.at[f - 1], here.plane(f))

    for f in range(1, 8):
        mod_copy(f).start()
    mod_in[d] = part[4 * here.p + z]
    tick(2)
    for f in range(1, 8):
        mod_copy(f).wait_recv()
    mod[...] = sum(mod_in[k] for k in range(1, 8)) + mod_in[0]
    for k in range(8):
        mod[pl.ds(6 * k, 6), :] = mod[pl.ds(6 * k, 6), :] + small_all[k, pl.ds(0, 6), :]
    for i in range(6):
        for k in range(8):
            vec[pl.ds(i, 1), pl.ds(k * LANES, LANES)] = mod[pl.ds(8 * i + k, 1), :]
    for k in range(8):
        lanes = pl.ds(k * LANES, LANES)
        vec[pl.ds(8, 1), lanes] = small_all[k // 2, pl.ds(6 + k % 2, 1), :]
        vec[pl.ds(9, 1), lanes] = small_all[4 + k // 2, pl.ds(6 + k % 2, 1), :]
        vec[pl.ds(10, 1), lanes] = small_all[k, pl.ds(8, 1), :]
        vec[pl.ds(11, 1), lanes] = small_all[k, pl.ds(13, 1), :]
        for j in range(4):
            vec[pl.ds(12 + j, 1), lanes] = small_all[k, pl.ds(9 + j, 1), :]

    def row(i):
        return vec[pl.ds(i, 1), :]

    exits = []

    def leave(src, name, index=None):
        dst = outs[name] if index is None else outs[name].at[index]
        copy = pltpu.make_async_copy(src, dst, out_sem.at[len(exits)])
        copy.start()
        exits.append(copy)

    leave(vec, "vec")
    leave(silu, "silu")
    tick(3)
    first.wait()
    leave(xs, "xs")

    block = 128

    @pl.loop(0, rows // block)
    def _(i):
        part_rows = pl.ds(pl.multiple_of(i * block, block), block)
        hat, _ = norm_parts(xs[part_rows, :].astype(F32))
        na[part_rows, :] = (hat * (1.0 + row(1)) + row(0)).astype(HALF)

    def project(chunk, index, bias):
        for n in range(width // tile):
            cols = pl.ds(n * tile, tile)
            value = nn(na[...], w[chunk, :, cols])
            if bias is not None:
                value = value + vec[pl.ds(bias, 1), cols]
            qkv[index, :, cols] = value.astype(HALF)

    def kv_copy(k):
        return remote(qkv.at[1 + k], kvo.at[k], kv_send.at[k], kv_recv.at[k], here.plane(1))

    tick(4)
    leave(w.at[KEYS], "whole", KEYS)
    project(KEYS, 1, None)
    kv_copy(0).start()
    tick(5)
    leave(w.at[VALUES], "whole", VALUES)
    project(VALUES, 2, 9)
    kv_copy(1).start()
    tick(6)
    leave(w.at[QUERIES], "whole", QUERIES)
    project(QUERIES, 0, 8)
    leave(qkv, "qkv")
    for k in range(2):
        kv_copy(k).wait_recv()
    leave(kvo, "kvo")

    span = 256
    low = lax.broadcasted_iota(jnp.int32, (span, LANES), 1) < HD
    lane = lax.broadcasted_iota(jnp.int32, (span, LANES), 1)

    @pl.loop(0, width // LANES)
    def _(step):
        cols = pl.ds(pl.multiple_of(step * LANES, LANES), LANES)
        keys = [qkv[1, :, cols], kvo[0, :, cols]]
        values = [qkv[2, :, cols], kvo[1, :, cols]]
        for start in range(0, rows, span):
            part_rows = pl.ds(start, span)
            q = qkv[0, part_rows, cols] * HALF(HD**-0.5)
            pieces = []
            for head in range(2):
                own = low if head == 0 else jnp.logical_not(low)
                qm = jnp.where(own, q, jnp.zeros_like(q))
                scores = [nt(qm, k) for k in keys]
                peak = functools.reduce(
                    jnp.maximum, [jnp.max(s, axis=-1, keepdims=True) for s in scores]
                )
                raised = [jnp.exp(s - peak) for s in scores]
                total = sum(jnp.sum(e, axis=-1, keepdims=True) for e in raised)
                mixed = sum(nn(e.astype(HALF), v) for e, v in zip(raised, values))
                pieces.append(mixed / total)
                logsum = jnp.broadcast_to(peak + jnp.log(total), (span, LANES))
                lse_acc[part_rows, :] = jnp.where(
                    lane == 2 * step + head, logsum, lse_acc[part_rows, :]
                )
            att[part_rows, cols] = jnp.where(low, pieces[0], pieces[1]).astype(HALF)

        @pl.when(step % 3 == 2)
        def _():
            gather.tick(7 + step // 3, prepare)

    lse[...] = lse_acc[...].T
    leave(lse, "lse")
    leave(att, "att")
    leave(w.at[OUT], "whole", OUT)
    second.wait()
    leave(ct, "cots")

    for n in range(width // tile):
        cols = pl.ds(n * tile, tile)
        branch = nn(att[...], w[OUT, :, cols]) + vec[pl.ds(10, 1), cols]
        bra[:, cols] = branch.astype(HALF)
        mid[:, cols] = xs[:, cols].astype(F32) + vec[pl.ds(2, 1), cols] * branch
    leave(mid, "mid")
    leave(bra, "bra")
    tick(9)

    @pl.loop(0, rows // block)
    def _(i):
        part_rows = pl.ds(pl.multiple_of(i * block, block), block)
        hat, _ = norm_parts(mid[part_rows, :])
        nb[part_rows, :] = (hat * (1.0 + row(4)) + row(3)).astype(HALF)
        gbh[part_rows, :] = (ct[part_rows, :].astype(F32) * row(5)).astype(HALF)
        bb[part_rows, :] = jnp.broadcast_to(row(11), (block, width))
        gnb[part_rows, :] = jnp.zeros((block, width), F32)

    leave(nb, "nb")

    def ff_copies(j, slot):
        return (
            pltpu.make_async_copy(hid.at[slot], outs["hid"].at[j], ff_sem.at[0, slot]),
            pltpu.make_async_copy(gph.at[slot], outs["gph"].at[j], ff_sem.at[1, slot]),
        )

    @pl.loop(0, 4)
    def _(j):
        slot = j % 2
        up, down = FEED + 2 * j, FEED + 2 * j + 1

        @pl.when(j >= 2)
        def _():
            for copy in ff_copies(j, slot):
                copy.wait()

        for n in range(width // tile):
            cols = pl.ds(n * tile, tile)
            pre = nn(nb[...], w[up, :, cols]) + vec[pl.ds(12 + j, 1), cols]
            grad = nt(gbh[...], w[down, cols, :])
            value, slope = gelu_both(pre)
            grad = grad * slope
            ups[pl.ds(j, 1), cols] = column_sum(grad)
            hid[slot, :, cols] = value.astype(HALF)
            gph[slot, :, cols] = grad.astype(HALF)
        for copy in ff_copies(j, slot):
            copy.start()
        gather.tick(10 + 2 * j, prepare)
        for n in range(width // tile):
            cols = pl.ds(n * tile, tile)
            bb[:, cols] = bb[:, cols] + nn(hid[slot], w[down, :, cols])
            gnb[:, cols] = gnb[:, cols] + nt(gph[slot], w[up, cols, :])
        gather.tick(11 + 2 * j, prepare)

    leave(bb, "bb")
    leave(gnb, "gnb")
    leave(ups, "ups")
    for slot in range(2):
        for copy in ff_copies(slot, slot):
            copy.wait()
    for copy in exits:
        copy.wait()
    gather.drain()
    first.drain()
    second.drain()
    for f in range(1, 8):
        small_copy(f).wait_send()
        mod_copy(f).wait_send()
    for k in range(2):
        kv_copy(k).wait_send()


def forward(tokens, cot, qkv_w, out_w, up_w, down_w, small, ada):
    depth, width = qkv_w.shape[0], out_w.shape[1]
    rows = tokens.shape[0] * tokens.shape[1]
    sds = jax.ShapeDtypeStruct
    flat, real = sds((rows, width), HALF), sds((rows, width), F32)
    shapes = dict(
        whole=sds((4, width, width), HALF),
        xs=flat,
        cots=flat,
        qkv=sds((3, rows, width), HALF),
        kvo=sds((2, rows, width), HALF),
        att=flat,
        lse=sds((LANES, rows), F32),
        mid=real,
        bra=flat,
        nb=flat,
        hid=sds((4, rows, width), HALF),
        gph=sds((4, rows, width), HALF),
        bb=real,
        gnb=real,
        vec=sds((16, width), F32),
        silu=sds((16, LANES), HALF),
        ups=sds((8, width), F32),
    )
    hbm = pl.BlockSpec(memory_space=pl.ANY)
    vmem = pl.BlockSpec(memory_space=pltpu.VMEM)
    dma = pltpu.SemaphoreType.DMA
    half = lambda *s: pltpu.VMEM(s, HALF)
    full = lambda *s: pltpu.VMEM(s, F32)
    scratch = [
        half(CHUNKS, width, width),
        full(8, 32, LANES),
        full(16, 48, LANES),
        full(8, 48, LANES),
        full(48, LANES),
        full(16, width),
        half(16, LANES),
        half(rows, width),
        half(rows, width),
        half(rows, width),
        half(3, rows, width),
        half(2, rows, width),
        half(rows, width),
        full(rows, LANES),
        full(LANES, rows),
        full(rows, width),
        half(rows, width),
        half(rows, width),
        half(rows, width),
        full(rows, width),
        full(rows, width),
        half(2, rows, width),
        half(2, rows, width),
        full(8, width),
        dma((CHUNKS, 9)),
        dma((CHUNKS, 9)),
        dma((CHUNKS,)),
        dma((2, 4)),
        dma((2, 4)),
        dma((7,)),
        dma((7,)),
        dma((7,)),
        dma((7,)),
        dma((2,)),
        dma((2,)),
        dma((24,)),
        dma((2, 2)),
    ]
    got = pl.pallas_call(
        forward_kernel,
        out_shape=tuple(shapes[name] for name in FORWARD_OUTS),
        in_specs=[hbm] * 6 + [vmem] * 2,
        out_specs=(hbm,) * len(FORWARD_OUTS),
        scratch_shapes=scratch,
        compiler_params=pltpu.CompilerParams(
            collective_id=1, has_side_effects=True, vmem_limit_bytes=67043328
        ),
        name="forward",
    )(tokens, cot, qkv_w, out_w, up_w, down_w, small, ada)
    return dict(zip(FORWARD_OUTS, got))


class Reduce:
    SLOTS = 8

    def __init__(self, bufs, sems):
        (self.own, self.rc, self.s, self.rx, self.ry, self.t, self.ry2, self.rx2, self.r, self.rz1, self.q, self.rz2, self.out) = bufs
        self.send, self.recv, self.load = sems
        self.d = lax.axis_index("dp")
        self.z = lax.axis_index("seq")
        self.c = self.d % 2
        self.x = self.d // 2 % 2
        self.y = self.d // 4
        self.h = self.z % 2
        self.depth = self.out.shape[1]
        self.cols = self.out.shape[2]
        self.pending = {}

    def _remote(self, i, slot, src, dst, peer):
        copy = pltpu.make_async_remote_copy(
            src_ref=src,
            dst_ref=dst,
            send_sem=self.send.at[i, slot],
            recv_sem=self.recv.at[i, slot],
            device_id=peer,
            device_id_type=MESH_ID,
        )
        copy.start()
        self.pending[(i, slot)] = copy

    def _plane(self, flip):
        return (jnp.bitwise_xor(self.d, flip), self.z)

    def _line(self, flip):
        return (self.d, jnp.bitwise_xor(self.z, flip))

    def sent(self, i, slot):
        self.pending.pop((i, slot)).wait_send()

    def arrived(self, i, slot):
        self.pending[(i, slot)].wait_recv()

    def begin(self, i, grads):
        self._remote(i, 0, grads.at[:, 1 - self.c], self.rc.at[i], self._plane(1))
        self.fetch = getattr(self, "fetch", {})
        copy = pltpu.make_async_copy(grads.at[:, self.c], self.own.at[i % 3], self.load.at[i % 3])
        copy.start()
        self.fetch[i] = copy

    def plane(self, i):
        slot, half = i % 3, self.cols // 2
        self.fetch.pop(i).wait()
        self.arrived(i, 0)
        if i >= 3:
            self.sent(i - 3, 1)
            self.sent(i - 3, 2)

        @pl.loop(0, 4)
        def _(k):
            self.s[slot, k] = (
                self.own[slot, k].astype(F32) + self.rc[i, k].astype(F32)
            ).astype(HALF)

        for other_y in range(2):
            pass
        self._remote(
            i, 1, self.s.at[slot].reshape(2, 2, self.depth, self.cols).at[:, 1 - self.x, :, pl.ds(0, half)],
            self.rx.at[i], self._plane(2),
        )
        self._remote(
            i, 2, self.s.at[slot].reshape(2, 2, self.depth, self.cols).at[1 - self.y, :, :, pl.ds(half, half)],
            self.ry.at[i], self._plane(4),
        )

    def cross(self, i):
        slot, half = i % 3, self.cols // 2
        self.arrived(i, 1)
        self.arrived(i, 2)
        if i >= 3:
            self.sent(i - 3, 3)
            self.sent(i - 3, 4)
        for k in range(2):
            self.t[slot, 0, k] = (
                self.s[slot, 2 * k + self.x, :, pl.ds(0, half)].astype(F32)
                + self.rx[i, k].astype(F32)
            ).astype(HALF)
            self.t[slot, 1, k] = (
                self.s[slot, 2 * self.y + k, :, pl.ds(half, half)].astype(F32)
                + self.ry[i, k].astype(F32)
            ).astype(HALF)
        self._remote(i, 3, self.t.at[slot, 0, 1 - self.y], self.ry2.at[i], self._plane(4))
        self._remote(i, 4, self.t.at[slot, 1, 1 - self.x], self.rx2.at[i], self._plane(2))

    def line(self, i):
        slot, half = i % 3, self.cols // 2
        rows = self.depth // 2
        self.arrived(i, 3)
        self.arrived(i, 4)
        if i >= 3:
            self.sent(i - 3, 5)
        self.r[slot, :, pl.ds(0, half)] = (
            self.t[slot, 0, self.y].astype(F32) + self.ry2[i].astype(F32)
        ).astype(HALF)
        self.r[slot, :, pl.ds(half, half)] = (
            self.t[slot, 1, self.x].astype(F32) + self.rx2[i].astype(F32)
        ).astype(HALF)
        away = pl.multiple_of((1 - self.h) * rows, rows)
        self._remote(i, 5, self.r.at[slot, pl.ds(away, rows), :], self.rz1.at[i], self._line(1))

    def far(self, i):
        slot, rows = i % 3, self.depth // 2
        self.arrived(i, 5)
        if i >= 3:
            self.sent(i - 3, 6)
        mine = pl.multiple_of(self.h * rows, rows)
        self.q[slot] = (
            self.r[slot, pl.ds(mine, rows), :].astype(F32) + self.rz1[i].astype(F32)
        ).astype(HALF)
        self._remote(i, 6, self.q.at[slot], self.rz2.at[i], self._line(2))

    def close(self, i):
        slot, rows = i % 3, self.depth // 2
        self.arrived(i, 6)
        mine = pl.multiple_of(self.h * rows, rows)
        self.out[i, pl.ds(mine, rows), :] = (
            self.q[slot].astype(F32) + self.rz2[i].astype(F32)
        ).astype(HALF)
        here = self.out.at[i, pl.ds(mine, rows), :]
        self._remote(i, 7, here, here, self._line(1))

    def finish(self, i):
        self.arrived(i, 7)

    def drain(self):
        for copy in self.pending.values():
            copy.wait_send()
        self.pending = {}


REDUCE_LAG = (0, 1, 2, 4, 6, 8, 10)


def reduce_steps(red, grads_of, t):
    steps = (
        lambda i: red.begin(i, grads_of(i)),
        red.plane,
        red.cross,
        red.line,
        red.far,
        red.close,
        red.finish,
    )
    for lag, step in zip(REDUCE_LAG, steps):
        if 0 <= t - lag < CHUNKS:
            step(t - lag)


def reduce_kernel(grads, out, *scratch):
    d, z = lax.axis_index("dp"), lax.axis_index("seq")
    greet(
        [(jnp.bitwise_xor(d, f), z) for f in (1, 2, 4)]
        + [(d, jnp.bitwise_xor(z, f)) for f in (1, 2)]
    )
    red = Reduce(scratch[:12] + (out,), scratch[12:])
    for t in range(CHUNKS + REDUCE_LAG[-1]):
        reduce_steps(red, lambda i: grads.at[i], t)
    red.drain()


def reduce_scratch(depth, cols):
    half, rows = cols // 2, depth // 2
    ring = 3
    return [
        pltpu.VMEM((ring, 4, depth, cols), HALF),
        pltpu.VMEM((CHUNKS, 4, depth, cols), HALF),
        pltpu.VMEM((ring, 4, depth, cols), HALF),
        pltpu.VMEM((CHUNKS, 2, depth, half), HALF),
        pltpu.VMEM((CHUNKS, 2, depth, half), HALF),
        pltpu.VMEM((ring, 2, 2, depth, half), HALF),
        pltpu.VMEM((CHUNKS, depth, half), HALF),
        pltpu.VMEM((CHUNKS, depth, half), HALF),
        pltpu.VMEM((ring, depth, cols), HALF),
        pltpu.VMEM((CHUNKS, rows, cols), HALF),
        pltpu.VMEM((ring, rows, cols), HALF),
        pltpu.VMEM((CHUNKS, rows, cols), HALF),
        pltpu.SemaphoreType.DMA((CHUNKS, Reduce.SLOTS)),
        pltpu.SemaphoreType.DMA((CHUNKS, Reduce.SLOTS)),
        pltpu.SemaphoreType.DMA((ring,)),
    ]


def reduce_all(grads):
    depth, cols = grads.shape[-2:]
    return pl.pallas_call(
        reduce_kernel,
        out_shape=jax.ShapeDtypeStruct((CHUNKS, depth, cols), HALF),
        in_specs=[pl.BlockSpec(memory_space=pl.ANY)],
        out_specs=pl.BlockSpec(memory_space=pltpu.VMEM),
        scratch_shapes=reduce_scratch(depth, cols),
        compiler_params=pltpu.CompilerParams(
            collective_id=2, has_side_effects=True, vmem_limit_bytes=58 << 20
        ),
        name="reduce_all",
    )(grads)


def body_any(
    tokens,
    condition,
    ada_weight,
    ada_bias,
    qkv_weight,
    qv_bias,
    out_weight,
    out_bias,
    up_weight,
    up_bias,
    down_weight,
    down_bias,
    cotangent,
):
    lats, part, width = tokens.shape
    dp = lax.axis_size("dp")
    seq = lax.axis_size("seq")
    me = lax.axis_index("dp")
    z = lax.axis_index("seq")
    core = me % 2
    pair = me // 2
    chip_lats = 2 * lats
    sub = seq // chip_lats
    first = core == 0

    def flip(x):
        return lax.ppermute(x, "dp", [(i, i ^ 1) for i in range(dp)])

    def shift(x, by):
        if by % sub == 0:
            return x
        return lax.ppermute(
            x, "seq", [(i, i // sub * sub + (i - by) % sub) for i in range(seq)]
        )

    def spread(x):
        halves = x.reshape(lats, 2, part // 2, width)
        keep = lax.dynamic_index_in_dim(halves, core, 1, keepdims=False)
        give = lax.dynamic_index_in_dim(halves, 1 - core, 1, keepdims=False)
        got = flip(give)
        both = jnp.concatenate(
            [jnp.where(first, keep, got), jnp.where(first, got, keep)], axis=0
        )
        both = both.reshape(seq, part // (2 * sub), width)
        return lax.all_to_all(both, "seq", 0, 0, tiled=True).reshape(-1, width)

    def collect(x):
        both = x.reshape(seq, part // (2 * sub), width)
        both = lax.all_to_all(both, "seq", 0, 0, tiled=True)
        both = both.reshape(2, lats, part // 2, width)
        mine = lax.dynamic_index_in_dim(both, core, 0, keepdims=False)
        give = lax.dynamic_index_in_dim(both, 1 - core, 0, keepdims=False)
        got = flip(give)
        return jnp.stack(
            [jnp.where(first, mine, got), jnp.where(first, got, mine)], axis=1
        ).reshape(lats, part, width)

    small = jnp.concatenate(
        [ada_bias, qv_bias, out_bias, up_bias, down_bias, condition.reshape(-1)]
    )
    small_all = lax.all_gather(small, "dp", axis=0, tiled=False)
    sizes = [a.shape[0] for a in (ada_bias, qv_bias, out_bias, up_bias, down_bias)]
    cuts = [0]
    for size in sizes:
        cuts.append(cuts[-1] + size)
    ada_bias_full, qv_full, out_bias_full, up_bias_full, down_bias_full = [
        small_all[:, a:b].reshape(-1).astype(F32) for a, b in zip(cuts[:-1], cuts[1:])
    ]
    cond_all = small_all[:, cuts[-1] :].reshape(dp * lats, width).astype(F32)
    depth = ada_weight.shape[0]
    silu_all = jax.nn.silu(cond_all).astype(HALF)
    silu_mine = lax.dynamic_slice_in_dim(silu_all, me * depth, depth, axis=1)
    partial = nn(silu_mine, ada_weight)
    row_here = z // sub
    wanted = partial.reshape(dp // 2, chip_lats, 6 * width)
    wanted = lax.dynamic_index_in_dim(wanted, row_here, 1, keepdims=True)
    wanted = jnp.broadcast_to(wanted, (dp // 2, 2, 6 * width)).reshape(dp, 6 * width)
    modulation = lax.psum_scatter(wanted, "dp", scatter_dimension=0, tiled=True)[0]
    modulation = (modulation + ada_bias_full).reshape(6, 1, width)
    shift_a, scale_a, gate_a, shift_b, scale_b, gate_b = [modulation[i] for i in range(6)]

    qkv_full = lax.all_gather(qkv_weight, "dp", axis=0, tiled=True)
    out_full = lax.all_gather(out_weight, "dp", axis=0, tiled=True)
    up_full = lax.all_gather(up_weight, "dp", axis=0, tiled=True)
    down_full = lax.all_gather(down_weight, "dp", axis=0, tiled=True)

    rows = spread(tokens).astype(F32)
    cot = spread(cotangent).astype(F32)

    hat_a, inverse_a = norm_parts(rows)
    normed_a = (hat_a * (1.0 + scale_a) + shift_a).astype(HALF)
    bias_all = jnp.concatenate([qv_full[:width], jnp.zeros((width,), F32), qv_full[width:]])
    projected = (nn(normed_a, qkv_full) + bias_all).astype(HALF)
    kv = projected[:, width:]
    ways = [(a, s) for s in range(sub) for a in range(2)]
    others = [shift(flip(kv) if a else kv, s) for a, s in ways[1:]]
    attended, logsum = attend(projected, others, width)
    branch_a = nn(attended, out_full) + out_bias_full
    middle = rows + gate_a * branch_a
    hat_b, inverse_b = norm_parts(middle)
    normed_b = (hat_b * (1.0 + scale_b) + shift_b).astype(HALF)
    hidden_pre = nn(normed_b, up_full) + up_bias_full
    hidden = gelu_tanh(hidden_pre).astype(HALF)
    branch_b = nn(hidden, down_full) + down_bias_full
    output = collect((middle + gate_b * branch_b).astype(HALF))

    grad_gate_b = jnp.sum(cot * branch_b, axis=0)
    grad_branch_b = cot * gate_b
    down_bias_grad = jnp.sum(grad_branch_b, axis=0)
    grad_branch_half = grad_branch_b.astype(HALF)
    down_weight_grad = tn(hidden, grad_branch_half).astype(HALF)
    grad_hidden = nt(grad_branch_half, down_full)
    _, gelu_back = jax.vjp(gelu_tanh, hidden_pre)
    grad_pre = gelu_back(grad_hidden)[0]
    up_bias_grad = jnp.sum(grad_pre, axis=0)
    grad_pre_half = grad_pre.astype(HALF)
    up_weight_grad = tn(normed_b, grad_pre_half).astype(HALF)
    grad_normed_b = nt(grad_pre_half, up_full)
    grad_shift_b = jnp.sum(grad_normed_b, axis=0)
    grad_scale_b = jnp.sum(grad_normed_b * hat_b, axis=0)
    grad_middle = cot + norm_grad(grad_normed_b, hat_b, inverse_b, scale_b)
    grad_gate_a = jnp.sum(grad_middle * branch_a, axis=0)
    grad_branch_a = grad_middle * gate_a
    out_bias_grad = jnp.sum(grad_branch_a, axis=0)
    grad_branch_a_half = grad_branch_a.astype(HALF)
    out_weight_grad = tn(attended, grad_branch_a_half).astype(HALF)
    grad_attended = nt(grad_branch_a_half, out_full).astype(HALF)

    results = attend_grad(projected, others, grad_attended, attended, logsum, width)
    count = len(ways)
    grad_query = results[0]
    grad_keys = results[1 : 1 + count]
    grad_values = results[1 + count :]
    grad_kv = [jnp.concatenate([k, v], axis=1) for k, v in zip(grad_keys, grad_values)]
    total_kv = grad_kv[0].astype(F32)
    for (a, s), part_kv in zip(ways[1:], grad_kv[1:]):
        back = shift(part_kv, -s)
        total_kv = total_kv + (flip(back) if a else back).astype(F32)
    grad_projected = jnp.concatenate([grad_query, total_kv.astype(HALF)], axis=1)
    qkv_weight_grad = tn(normed_a, grad_projected).astype(HALF)
    grad_proj_float = grad_projected.astype(F32)
    qv_bias_grad = jnp.concatenate(
        [
            jnp.sum(grad_proj_float[:, :width], axis=0),
            jnp.sum(grad_proj_float[:, 2 * width :], axis=0),
        ]
    )
    grad_normed_a = nt(grad_projected, qkv_full)
    grad_shift_a = jnp.sum(grad_normed_a, axis=0)
    grad_scale_a = jnp.sum(grad_normed_a * hat_a, axis=0)
    grad_tokens = grad_middle + norm_grad(grad_normed_a, hat_a, inverse_a, scale_a)
    tokens_grad = collect(grad_tokens.astype(HALF)).astype(F32)

    grad_mod = jnp.concatenate(
        [grad_shift_a, grad_scale_a, grad_gate_a, grad_shift_b, grad_scale_b, grad_gate_b]
    )
    every = lax.all_gather(grad_mod, "seq", axis=0, tiled=False)
    every = lax.all_gather(every, "dp", axis=0, tiled=False)
    every = every.reshape(dp // 2, 2, chip_lats, sub, 6 * width).sum(axis=(1, 3))
    every = every.reshape(dp * lats, 6 * width)
    every_half = every.astype(HALF)
    ada_weight_grad = tn(silu_mine, every_half)
    bias_len = ada_bias.shape[0]
    ada_bias_grad = jnp.sum(
        lax.dynamic_slice_in_dim(every, me * bias_len, bias_len, axis=1), axis=0
    )
    cond_part = nt(every_half, ada_weight).reshape(dp, lats, depth)
    cond_part = lax.all_to_all(cond_part, "dp", 0, 0, tiled=True)
    cond_part = cond_part.transpose(1, 0, 2).reshape(lats, width)
    cond_float = condition.astype(F32)
    sigmoid_cond = jax.nn.sigmoid(cond_float)
    silu_slope = sigmoid_cond * (1.0 + cond_float * (1.0 - sigmoid_cond))
    condition_grad = silu_slope * cond_part

    def reduce_weight(grad):
        share = lax.psum_scatter(grad, "dp", scatter_dimension=0, tiled=True)
        return lax.psum(share, "seq").astype(F32)

    bias_parts = jnp.concatenate(
        [
            b.reshape(dp, -1)
            for b in (qv_bias_grad, out_bias_grad, up_bias_grad, down_bias_grad)
        ],
        axis=1,
    )
    bias_parts = lax.psum_scatter(bias_parts, "dp", scatter_dimension=0, tiled=True)
    bias_parts = lax.psum(bias_parts, "seq")[0]
    cuts = [c - sizes[0] for c in cuts[1:]]
    qv_g, ob_g, ub_g, db_g = [bias_parts[a:b] for a, b in zip(cuts[:-1], cuts[1:])]
    return (
        output,
        tokens_grad,
        condition_grad,
        ada_weight_grad,
        ada_bias_grad,
        reduce_weight(qkv_weight_grad),
        qv_g,
        reduce_weight(out_weight_grad),
        ob_g,
        reduce_weight(up_weight_grad),
        ub_g,
        reduce_weight(down_weight_grad),
        db_g,
    )


def body(
    tokens,
    condition,
    ada_weight,
    ada_bias,
    qkv_weight,
    qv_bias,
    out_weight,
    out_bias,
    up_weight,
    up_bias,
    down_weight,
    down_bias,
    cotangent,
):
    lats, part, width = tokens.shape
    dp = lax.axis_size("dp")
    seq = lax.axis_size("seq")
    if (dp, seq, lats) != (8, 4, 2):
        return body_any(
            tokens,
            condition,
            ada_weight,
            ada_bias,
            qkv_weight,
            qv_bias,
            out_weight,
            out_bias,
            up_weight,
            up_bias,
            down_weight,
            down_bias,
            cotangent,
        )
    me = lax.axis_index("dp")
    z = lax.axis_index("seq")
    core = me % 2
    first = core == 0
    depth = ada_weight.shape[0]
    wide = dp * up_bias.shape[0]
    cut = wide // (4 * dp)

    def flip(x):
        return lax.ppermute(x, "dp", [(i, i ^ 1) for i in range(dp)])

    def collect(x):
        both = x.reshape(seq, part // 2, width)
        both = lax.all_to_all(both, "seq", 0, 0, tiled=True)
        both = both.reshape(2, lats, part // 2, width)
        mine = lax.dynamic_index_in_dim(both, core, 0, keepdims=False)
        give = lax.dynamic_index_in_dim(both, 1 - core, 0, keepdims=False)
        got = flip(give)
        return jnp.stack(
            [jnp.where(first, mine, got), jnp.where(first, got, mine)], axis=1
        ).reshape(lats, part, width)

    small = jnp.concatenate(
        [
            ada_bias.reshape(-1, LANES),
            qv_bias.reshape(-1, LANES),
            out_bias.reshape(-1, LANES),
            up_bias.reshape(-1, LANES),
            down_bias.reshape(-1, LANES),
            jnp.zeros((2, LANES), HALF),
            condition.reshape(-1, LANES),
        ],
        axis=0,
    ).astype(F32)
    f = forward(
        tokens, cotangent, qkv_weight, out_weight, up_weight, down_weight, small, ada_weight
    )
    whole = f["whole"]
    vec = f["vec"]
    shift_a, scale_a, gate_a, shift_b, scale_b, gate_b = [vec[i : i + 1] for i in range(6)]
    cot = f["cots"].astype(F32)
    middle = f["mid"]
    branch_b = f["bb"]
    output = collect((middle + gate_b * branch_b).astype(HALF))
    grad_gate_b = jnp.sum(cot * branch_b, axis=0)
    grad_branch_b = cot * gate_b
    down_bias_grad = jnp.sum(grad_branch_b, axis=0)
    gbh = grad_branch_b.astype(HALF)
    chunks = [None] * CHUNKS
    for j in range(4):
        chunks[FEED + 2 * j] = tn(f["nb"], f["gph"][j]).astype(HALF)
        chunks[FEED + 2 * j + 1] = tn(f["hid"][j], gbh).astype(HALF)
    up_bias_grad = f["ups"][:4].reshape(4, dp, cut).transpose(1, 0, 2).reshape(-1)
    hat_b, inverse_b = norm_parts(middle)
    gnb = f["gnb"]
    branch_a = f["bra"].astype(F32)
    grad_shift_b = jnp.sum(gnb, axis=0)
    grad_scale_b = jnp.sum(gnb * hat_b, axis=0)
    grad_middle = cot + norm_grad(gnb, hat_b, inverse_b, scale_b)
    grad_gate_a = jnp.sum(grad_middle * branch_a, axis=0)
    grad_branch_a = grad_middle * gate_a
    out_bias_grad = jnp.sum(grad_branch_a, axis=0)
    gbah = grad_branch_a.astype(HALF)
    chunks[OUT] = tn(f["att"], gbah).astype(HALF)
    grad_attended = nt(gbah, whole[OUT]).astype(HALF)
    projected = f["qkv"].transpose(1, 0, 2).reshape(-1, 3 * width)
    other = f["kvo"].transpose(1, 0, 2).reshape(-1, 2 * width)
    grad_q, dk, dko, dv, dvo = attend_grad(
        projected, [other], grad_attended, f["att"], f["lse"], width
    )
    grad_k = (dk.astype(F32) + flip(dko).astype(F32)).astype(HALF)
    grad_v = (dv.astype(F32) + flip(dvo).astype(F32)).astype(HALF)
    rows = f["xs"].astype(F32)
    hat_a, inverse_a = norm_parts(rows)
    normed_a = (hat_a * (1.0 + scale_a) + shift_a).astype(HALF)
    chunks[KEYS] = tn(normed_a, grad_k).astype(HALF)
    chunks[VALUES] = tn(normed_a, grad_v).astype(HALF)
    chunks[QUERIES] = tn(normed_a, grad_q).astype(HALF)
    qv_bias_grad = jnp.concatenate(
        [jnp.sum(grad_q.astype(F32), axis=0), jnp.sum(grad_v.astype(F32), axis=0)]
    )
    grad_normed_a = (
        nt(grad_q, whole[QUERIES]) + nt(grad_k, whole[KEYS]) + nt(grad_v, whole[VALUES])
    )
    grad_shift_a = jnp.sum(grad_normed_a, axis=0)
    grad_scale_a = jnp.sum(grad_normed_a * hat_a, axis=0)
    grad_tokens = grad_middle + norm_grad(grad_normed_a, hat_a, inverse_a, scale_a)
    tokens_grad = collect(grad_tokens.astype(HALF)).astype(F32)
    grads = jnp.stack(chunks).reshape(CHUNKS, dp // 2, 2, depth, width)
    shares = reduce_all(grads).astype(F32)
    qkv_g = jnp.concatenate([shares[QUERIES], shares[KEYS], shares[VALUES]], axis=1)
    out_g = shares[OUT]
    up_g = shares[FEED::2].reshape(4, depth, dp, cut).transpose(1, 2, 0, 3).reshape(depth, wide)
    down_g = shares[FEED + 1 :: 2].reshape(4 * cut, width)

    grad_mod = jnp.concatenate(
        [grad_shift_a, grad_scale_a, grad_gate_a, grad_shift_b, grad_scale_b, grad_gate_b]
    )
    every = lax.all_gather(grad_mod, "seq", axis=0, tiled=False)
    every = lax.all_gather(every, "dp", axis=0, tiled=False)
    every = every.reshape(dp // 2, 2, seq, 6 * width).sum(axis=1)
    every = every.reshape(dp * lats, 6 * width)
    every_half = every.astype(HALF)
    ada_weight_grad = tn(f["silu"], every_half)
    bias_len = ada_bias.shape[0]
    ada_bias_grad = jnp.sum(
        lax.dynamic_slice_in_dim(every, me * bias_len, bias_len, axis=1), axis=0
    )
    cond_part = nt(every_half, ada_weight).reshape(dp, lats, depth)
    cond_part = lax.all_to_all(cond_part, "dp", 0, 0, tiled=True)
    cond_part = cond_part.transpose(1, 0, 2).reshape(lats, width)
    cond_float = condition.astype(F32)
    sigmoid_cond = jax.nn.sigmoid(cond_float)
    silu_slope = sigmoid_cond * (1.0 + cond_float * (1.0 - sigmoid_cond))
    condition_grad = silu_slope * cond_part
    bias_parts = jnp.concatenate(
        [
            b.reshape(dp, -1)
            for b in (qv_bias_grad, out_bias_grad, up_bias_grad, down_bias_grad)
        ],
        axis=1,
    )
    bias_parts = lax.psum_scatter(bias_parts, "dp", scatter_dimension=0, tiled=True)
    bias_parts = lax.psum(bias_parts, "seq")[0]
    sizes = [a.shape[0] for a in (qv_bias, out_bias, up_bias, down_bias)]
    cuts = [0]
    for size in sizes:
        cuts.append(cuts[-1] + size)
    qv_g, ob_g, ub_g, db_g = [bias_parts[a:b] for a, b in zip(cuts[:-1], cuts[1:])]
    return (
        output,
        tokens_grad,
        condition_grad,
        ada_weight_grad,
        ada_bias_grad,
        qkv_g,
        qv_g,
        out_g,
        ob_g,
        up_g,
        ub_g,
        down_g,
        db_g,
    )


def solution(mesh):
    return jax.shard_map(
        body,
        mesh=mesh,
        in_specs=(
            P("dp", "seq", None),
            P("dp", None),
            P("dp", None),
            P("dp"),
            P("dp", None),
            P("dp"),
            P("dp", None),
            P("dp"),
            P("dp", None),
            P("dp"),
            P("dp", None),
            P("dp"),
            P("dp", "seq", None),
        ),
        out_specs=(
            P("dp", "seq", None),
            P("dp", "seq", None),
            P("dp", None),
            P("dp", None),
            P("dp"),
            P("dp", None),
            P("dp"),
            P("dp", None),
            P("dp"),
            P("dp", None),
            P("dp"),
            P("dp", None),
            P("dp"),
        ),
        check_vma=False,
    )
```

```python
import functools

import jax
import jax.numpy as jnp
from jax import lax
from jax.experimental import pallas as pl
from jax.experimental.pallas import tpu as pltpu
from jax.sharding import PartitionSpec as P

HD = 64
LANES = 128
EPSILON = 1e-06
HALF = jnp.bfloat16
F32 = jnp.float32


def nn(a, b):
    return jnp.dot(a, b, preferred_element_type=F32)


def nt(a, b):
    return lax.dot_general(a, b, (((1,), (1,)), ((), ())), preferred_element_type=F32)


def tn(a, b):
    return lax.dot_general(a, b, (((0,), (0,)), ((), ())), preferred_element_type=F32)


def attend_kernel(groups, *refs):
    q_ref = refs[0]
    k_refs = refs[1 : 1 + groups]
    v_refs = refs[1 + groups : 1 + 2 * groups]
    out_ref, lse_ref, lse_acc = refs[1 + 2 * groups :]
    step = pl.program_id(0)
    rows = q_ref.shape[0]
    block = 256
    low = lax.broadcasted_iota(jnp.int32, (block, LANES), 1) < HD
    lane = lax.broadcasted_iota(jnp.int32, (block, LANES), 1)
    for start in range(0, rows, block):
        here = pl.ds(start, block)
        q = q_ref[here, :] * HALF(HD**-0.5)
        pieces = []
        for head in range(2):
            own = low if head == 0 else jnp.logical_not(low)
            qm = jnp.where(own, q, jnp.zeros_like(q))
            scores = [nt(qm, k[...]) for k in k_refs]
            peak = functools.reduce(
                jnp.maximum, [jnp.max(s, axis=-1, keepdims=True) for s in scores]
            )
            raised = [jnp.exp(s - peak) for s in scores]
            total = sum(jnp.sum(e, axis=-1, keepdims=True) for e in raised)
            mixed = sum(nn(e.astype(HALF), v[...]) for e, v in zip(raised, v_refs))
            pieces.append(mixed / total)
            spot = lane == 2 * step + head
            logsum = jnp.broadcast_to(peak + jnp.log(total), (block, LANES))
            lse_acc[here, :] = jnp.where(spot, logsum, lse_acc[here, :])
        out_ref[here, :] = jnp.where(low, pieces[0], pieces[1]).astype(HALF)

    @pl.when(step == pl.num_programs(0) - 1)
    def _():
        lse_ref[...] = lse_acc[...].T


def attend(projected, others, width):
    rows = projected.shape[0]
    groups = 1 + len(others)
    tiles = width // LANES
    col = lambda base: pl.BlockSpec((rows, LANES), lambda i, base=base: (0, base + i))
    return pl.pallas_call(
        functools.partial(attend_kernel, groups),
        grid=(tiles,),
        out_shape=(
            jax.ShapeDtypeStruct((rows, width), HALF),
            jax.ShapeDtypeStruct((LANES, rows), F32),
        ),
        in_specs=[col(0), col(tiles)] + [col(0)] * len(others) + [col(2 * tiles)] + [col(tiles)] * len(others),
        out_specs=(col(0), pl.BlockSpec((LANES, rows), lambda i: (0, 0))),
        scratch_shapes=[pltpu.VMEM((rows, LANES), F32)],
        compiler_params=pltpu.CompilerParams(vmem_limit_bytes=48 << 20),
        name="attend",
    )(projected, projected, *others, projected, *others)


def attend_grad_kernel(groups, *refs):
    q_ref = refs[0]
    k_refs = refs[1 : 1 + groups]
    v_refs = refs[1 + groups : 1 + 2 * groups]
    do_ref, o_ref, lse_ref = refs[1 + 2 * groups : 4 + 2 * groups]
    dq_ref = refs[4 + 2 * groups]
    dk_refs = refs[5 + 2 * groups : 5 + 3 * groups]
    dv_refs = refs[5 + 3 * groups : 5 + 4 * groups]
    step = pl.program_id(0)
    rows = q_ref.shape[0]
    block = 256
    scale = HALF(HD**-0.5)
    q = q_ref[...] * scale
    grad = do_ref[...]
    product = grad.astype(F32) * o_ref[...].astype(F32)
    top = product.astype(HALF)
    rest = (product - top.astype(F32)).astype(HALF)
    pick = lax.broadcasted_iota(jnp.int32, (8, LANES), 0) == (
        lax.broadcasted_iota(jnp.int32, (8, LANES), 1) // HD
    )
    pick = jnp.where(pick, 1.0, 0.0).astype(HALF)
    inner = nt(pick, top) + nt(pick, rest)
    low = lax.broadcasted_iota(jnp.int32, (block, LANES), 1) < HD
    dq_t = [jnp.zeros((LANES, rows), F32) for _ in range(2)]
    for k_ref, v_ref, dk_ref, dv_ref in zip(k_refs, v_refs, dk_refs, dv_refs):
        for start in range(0, rows, block):
            here = pl.ds(start, block)
            k = k_ref[here, :]
            v = v_ref[here, :]
            k_t = k.T
            dks, dvs = [], []
            for head in range(2):
                own = low if head == 0 else jnp.logical_not(low)
                lse = lse_ref[pl.ds(2 * step + head, 1), :]
                scores = nt(jnp.where(own, k, jnp.zeros_like(k)), q)
                probs = jnp.exp(scores - lse)
                dvs.append(nn(probs.astype(HALF), grad))
                gp = nt(jnp.where(own, v, jnp.zeros_like(v)), grad)
                gs = (probs * (gp - inner[head : head + 1, :])).astype(HALF)
                dks.append(nn(gs, q))
                dq_t[head] = dq_t[head] + nn(k_t, gs)
            dk_ref[here, :] = jnp.where(low, dks[0], dks[1]).astype(HALF)
            dv_ref[here, :] = jnp.where(low, dvs[0], dvs[1]).astype(HALF)
    upper = lax.broadcasted_iota(jnp.int32, (LANES, rows), 0) < HD
    dq = jnp.where(upper, dq_t[0], dq_t[1]).T * HD**-0.5
    dq_ref[...] = dq.astype(HALF)


def attend_grad(projected, others, grad, attended, logsum, width):
    rows = projected.shape[0]
    groups = 1 + len(others)
    tiles = width // LANES
    col = lambda base: pl.BlockSpec((rows, LANES), lambda i, base=base: (0, base + i))
    out = jax.ShapeDtypeStruct((rows, width), HALF)
    return pl.pallas_call(
        functools.partial(attend_grad_kernel, groups),
        grid=(tiles,),
        out_shape=(out,) * (1 + 2 * groups),
        in_specs=[col(0), col(tiles)]
        + [col(0)] * len(others)
        + [col(2 * tiles)]
        + [col(tiles)] * len(others)
        + [col(0), col(0), pl.BlockSpec((LANES, rows), lambda i: (0, 0))],
        out_specs=(col(0),) * (1 + 2 * groups),
        compiler_params=pltpu.CompilerParams(vmem_limit_bytes=48 << 20),
        name="attend_grad",
    )(projected, projected, *others, projected, *others, grad, attended, logsum)


def norm_parts(rows):
    centred = rows - jnp.mean(rows, axis=-1, keepdims=True)
    variance = jnp.mean(centred * centred, axis=-1, keepdims=True)
    inverse = lax.rsqrt(variance + EPSILON)
    return centred * inverse, inverse


def norm_grad(grad, hat, inverse, scale):
    g = grad * (1.0 + scale)
    return (
        g
        - jnp.mean(g, axis=-1, keepdims=True)
        - hat * jnp.mean(g * hat, axis=-1, keepdims=True)
    ) * inverse


def gelu_tanh(inputs):
    return jax.nn.gelu(inputs, approximate=True)


MESH_ID = pl.DeviceIdType.MESH
CHUNKS = 12
KEYS, VALUES, QUERIES, OUT, FEED = 0, 1, 2, 3, 4


def guarded(low, value, high, run):
    if isinstance(value, int):
        if low <= value < high:
            run(value)
        return

    @pl.when(jnp.logical_and(value >= low, value < high))
    def _():
        run(value)


class Place:
    def __init__(self):
        self.d = lax.axis_index("dp")
        self.z = lax.axis_index("seq")
        self.c = self.d % 2
        self.x = self.d // 2 % 2
        self.y = self.d // 4
        self.p = self.d // 2

    def plane(self, flip):
        return (jnp.bitwise_xor(self.d, flip), self.z)

    def line(self, flip):
        return (self.d, jnp.bitwise_xor(self.z, flip))


def remote(src, dst, send, recv, peer):
    return pltpu.make_async_remote_copy(
        src_ref=src,
        dst_ref=dst,
        send_sem=send,
        recv_sem=recv,
        device_id=peer,
        device_id_type=MESH_ID,
    )


def greet(peers):
    barrier = pltpu.get_barrier_semaphore()
    for peer in peers:
        pl.semaphore_signal(barrier, inc=1, device_id=peer, device_id_type=MESH_ID)
    pl.semaphore_wait(barrier, len(peers))


class Gather:
    SENDS = (
        (2, 0, None),
        (4, 0, None),
        (1, 0, None),
        (1, 2, None),
        (1, 4, None),
        (4, 2, 0),
        (2, 4, 1),
        (1, 6, 0),
        (1, 6, 1),
    )

    def __init__(self, here, whole, send, recv):
        self.here, self.whole, self.send, self.recv = here, whole, send, recv
        self.depth = whole.shape[1] // 8

    def _block(self, chunk, flip, half):
        size = self.depth if half is None else self.depth // 2
        lo = 0 if half is None else half * size
        row = pl.multiple_of(jnp.bitwise_xor(self.here.d, flip) * self.depth + lo, 64)
        return self.whole.at[chunk, pl.ds(row, size), :]

    def _copy(self, chunk, slot, arriving=False):
        flip, block, half = self.SENDS[slot]
        ref = self._block(chunk, jnp.bitwise_xor(flip, block) if arriving else block, half)
        return remote(
            ref, ref, self.send.at[chunk, slot], self.recv.at[chunk, slot], self.here.plane(flip)
        )

    def begin(self, i):
        for slot in (0, 1, 2):
            self._copy(i, slot).start()

    def relay(self, i):
        self._copy(i, 0, True).wait_recv()
        self._copy(i, 5).start()
        self._copy(i, 1, True).wait_recv()
        self._copy(i, 6).start()
        self._copy(i, 3).start()
        self._copy(i, 4).start()

    def share(self, i):
        self._copy(i, 5, True).wait_recv()
        self._copy(i, 7).start()
        self._copy(i, 6, True).wait_recv()
        self._copy(i, 8).start()

    def finish(self, i):
        for slot in (2, 3, 4, 7, 8):
            self._copy(i, slot, True).wait_recv()

    def tick(self, t, prepare):
        def begin(i):
            prepare(i)
            self.begin(i)

        guarded(0, t, CHUNKS, begin)
        guarded(0, t - 2, CHUNKS, self.relay)
        guarded(0, t - 3, CHUNKS, self.share)
        guarded(0, t - 4, CHUNKS, self.finish)

    def drain(self):
        @pl.loop(0, CHUNKS)
        def _(i):
            for slot in range(len(self.SENDS)):
                self._copy(i, slot).wait_send()


class Spread:
    def __init__(self, here, source, landing, send, recv):
        self.here, self.source, self.landing = here, source, landing
        self.send, self.recv = send, recv
        self.size = source.shape[1] // 2

    def _each(self):
        here = self.here
        lats = self.source.shape[0]
        for j in range(lats):
            for core in range(2):
                z = lats * here.c + j
                own = jnp.logical_and(z == here.z, core == here.c)
                src = self.source.at[j, pl.ds(core * self.size, self.size), :]
                peer = (here.d - here.c + core, z)
                yield own, j * 2 + core, src, peer

    def _land(self, z):
        return self.landing.at[pl.ds(pl.multiple_of(z * self.size, self.size), self.size), :]

    def start(self):
        z = self.here.z
        for own, index, src, peer in self._each():

            @pl.when(own)
            def _():
                pltpu.make_async_copy(src, self._land(z), self.recv.at[z]).start()

            @pl.when(jnp.logical_not(own))
            def _():
                remote(src, self._land(z), self.send.at[index], self.recv.at[z], peer).start()

    def wait(self):
        src = self.source.at[0, pl.ds(0, self.size), :]
        for z in range(4):
            pltpu.make_async_copy(src, self._land(z), self.recv.at[z]).wait()

    def drain(self):
        z = self.here.z
        for own, index, src, peer in self._each():

            @pl.when(jnp.logical_not(own))
            def _():
                remote(src, self._land(z), self.send.at[index], self.recv.at[z], peer).wait_send()


def gelu_both(v):
    root = 0.7978845608028654
    square = v * v
    t = jnp.tanh(root * (v + 0.044715 * (v * square)))
    half = 0.5 * (1.0 + t)
    slope = half + (0.5 * root) * v * (1.0 - t * t) * (1.0 + (3 * 0.044715) * square)
    return half * v, slope


def column_sum(x):
    return jnp.sum(x, axis=0, keepdims=True)


FORWARD_OUTS = (
    "whole",
    "xs",
    "cots",
    "qkv",
    "kvo",
    "att",
    "lse",
    "mid",
    "bra",
    "nb",
    "hid",
    "gph",
    "gbh",
    "outb",
    "gnb",
    "vec",
    "silu",
    "ups",
)


def forward_kernel(tokens, cot, qkv_w, out_w, up_w, down_w, small, ada, *refs):
    outs = dict(zip(FORWARD_OUTS, refs))
    (
        w,
        small_all,
        part,
        mod_in,
        mod,
        vec,
        silu,
        xs,
        ct,
        na,
        qkv,
        kvo,
        att,
        lse_acc,
        lse,
        mid,
        bra,
        nb,
        gbh,
        bb,
        gnb,
        hid,
        gph,
        ups,
        g_send,
        g_recv,
        own_sem,
        sp_send,
        sp_recv,
        sm_send,
        sm_recv,
        md_send,
        md_recv,
        kv_send,
        kv_recv,
        out_sem,
        ff_sem,
    ) = refs[len(FORWARD_OUTS) :]
    here = Place()
    d, z, c = here.d, here.z, here.c
    depth, width = qkv_w.shape[0], out_w.shape[1]
    rows = xs.shape[0]
    wide = up_w.shape[1]
    cut = wide // 32
    tile = 256

    mine = pl.ds(pl.multiple_of(d * depth, depth), depth)
    for i, k in ((KEYS, 1), (VALUES, 2), (QUERIES, 0)):
        pltpu.make_async_copy(
            qkv_w.at[:, pl.ds(k * width, width)], w.at[i, mine, :], own_sem.at[i]
        ).start()
    pltpu.make_async_copy(out_w, w.at[OUT, mine, :], own_sem.at[OUT]).start()
    for j in range(4):
        for k in range(8):
            pltpu.make_async_copy(
                up_w.at[:, pl.ds((4 * k + j) * cut, cut)],
                w.at[FEED + 2 * j, mine, pl.ds(k * cut, cut)],
                own_sem.at[FEED + 2 * j],
            ).start()
        pltpu.make_async_copy(
            down_w.at[pl.ds(j * depth, depth), :], w.at[FEED + 2 * j + 1, mine, :], own_sem.at[FEED + 2 * j + 1]
        ).start()

    def prepare(i):
        pltpu.make_async_copy(out_w, w.at[i, mine, :], own_sem.at[i]).wait()

    peers = [here.plane(f) for f in range(1, 8)]
    for core in range(2):
        for f in range(1, 4):
            peers.append((d - c + core, jnp.bitwise_xor(z, f)))
    greet(peers)

    gather = Gather(here, w, g_send, g_recv)
    tick = functools.partial(gather.tick, prepare=prepare)
    first = Spread(here, tokens, xs, sp_send.at[0], sp_recv.at[0])
    second = Spread(here, cot, ct, sp_send.at[1], sp_recv.at[1])

    def small_copy(f):
        dst = small_all.at[d]
        return remote(small, dst, sm_send.at[f - 1], sm_recv.at[f - 1], here.plane(f))

    for f in range(1, 8):
        small_copy(f).start()
    first.start()
    tick(0)
    tick(1)
    second.start()
    small_all[d] = small[...]
    for f in range(1, 8):
        small_copy(f).wait_recv()

    picked = [
        small_all[i // 2, pl.ds(16 + 8 * (i % 2) + d, 1), :] for i in range(16)
    ]
    cond = jnp.concatenate(picked, axis=0)
    silu[...] = (cond * jax.nn.sigmoid(cond)).astype(HALF)
    for i in range(6):
        product = nn(silu[...], ada[:, pl.ds(i * width, width)])
        for k in range(8):
            part[:, 8 * i + k, :] = product[:, k * LANES : (k + 1) * LANES]

    def mod_copy(f):
        flip = jnp.bitwise_xor(d, f)
        src = part.at[4 * (flip // 2) + z]
        return remote(src, mod_in.at[d], md_send.at[f - 1], md_recv.at[f - 1], here.plane(f))

    for f in range(1, 8):
        mod_copy(f).start()
    mod_in[d] = part[4 * here.p + z]
    tick(2)
    for f in range(1, 8):
        mod_copy(f).wait_recv()
    mod[...] = sum(mod_in[k] for k in range(1, 8)) + mod_in[0]
    for k in range(8):
        mod[pl.ds(6 * k, 6), :] = mod[pl.ds(6 * k, 6), :] + small_all[k, pl.ds(0, 6), :]
    for i in range(6):
        for k in range(8):
            vec[pl.ds(i, 1), pl.ds(k * LANES, LANES)] = mod[pl.ds(8 * i + k, 1), :]
    for k in range(8):
        lanes = pl.ds(k * LANES, LANES)
        vec[pl.ds(8, 1), lanes] = small_all[k // 2, pl.ds(6 + k % 2, 1), :]
        vec[pl.ds(9, 1), lanes] = small_all[4 + k // 2, pl.ds(6 + k % 2, 1), :]
        vec[pl.ds(10, 1), lanes] = small_all[k, pl.ds(8, 1), :]
        vec[pl.ds(11, 1), lanes] = small_all[k, pl.ds(13, 1), :]
        for j in range(4):
            vec[pl.ds(12 + j, 1), lanes] = small_all[k, pl.ds(9 + j, 1), :]

    def row(i):
        return vec[pl.ds(i, 1), :]

    exits = []

    def leave(src, name, index=None):
        dst = outs[name] if index is None else outs[name].at[index]
        copy = pltpu.make_async_copy(src, dst, out_sem.at[len(exits)])
        copy.start()
        exits.append(copy)

    leave(vec, "vec")
    leave(silu, "silu")
    tick(3)
    first.wait()
    leave(xs, "xs")

    block = 128

    @pl.loop(0, rows // block)
    def _(i):
        part_rows = pl.ds(pl.multiple_of(i * block, block), block)
        hat, _ = norm_parts(xs[part_rows, :].astype(F32))
        na[part_rows, :] = (hat * (1.0 + row(1)) + row(0)).astype(HALF)

    def project(chunk, index, bias):
        for n in range(width // tile):
            cols = pl.ds(n * tile, tile)
            value = nn(na[...], w[chunk, :, cols])
            if bias is not None:
                value = value + vec[pl.ds(bias, 1), cols]
            qkv[index, :, cols] = value.astype(HALF)

    def kv_copy(k):
        return remote(qkv.at[1 + k], kvo.at[k], kv_send.at[k], kv_recv.at[k], here.plane(1))

    tick(4)
    leave(w.at[KEYS], "whole", KEYS)
    project(KEYS, 1, None)
    kv_copy(0).start()
    tick(5)
    leave(w.at[VALUES], "whole", VALUES)
    project(VALUES, 2, 9)
    kv_copy(1).start()
    tick(6)
    leave(w.at[QUERIES], "whole", QUERIES)
    project(QUERIES, 0, 8)
    leave(qkv, "qkv")
    for k in range(2):
        kv_copy(k).wait_recv()
    leave(kvo, "kvo")

    span = 256
    low = lax.broadcasted_iota(jnp.int32, (span, LANES), 1) < HD
    lane = lax.broadcasted_iota(jnp.int32, (span, LANES), 1)

    @pl.loop(0, width // LANES)
    def _(step):
        cols = pl.ds(pl.multiple_of(step * LANES, LANES), LANES)
        keys = [qkv[1, :, cols], kvo[0, :, cols]]
        values = [qkv[2, :, cols], kvo[1, :, cols]]
        for start in range(0, rows, span):
            part_rows = pl.ds(start, span)
            q = qkv[0, part_rows, cols] * HALF(HD**-0.5)
            pieces = []
            for head in range(2):
                own = low if head == 0 else jnp.logical_not(low)
                qm = jnp.where(own, q, jnp.zeros_like(q))
                scores = [nt(qm, k) for k in keys]
                peak = functools.reduce(
                    jnp.maximum, [jnp.max(s, axis=-1, keepdims=True) for s in scores]
                )
                raised = [jnp.exp(s - peak) for s in scores]
                total = sum(jnp.sum(e, axis=-1, keepdims=True) for e in raised)
                mixed = sum(nn(e.astype(HALF), v) for e, v in zip(raised, values))
                pieces.append(mixed / total)
                logsum = jnp.broadcast_to(peak + jnp.log(total), (span, LANES))
                lse_acc[part_rows, :] = jnp.where(
                    lane == 2 * step + head, logsum, lse_acc[part_rows, :]
                )
            att[part_rows, cols] = jnp.where(low, pieces[0], pieces[1]).astype(HALF)

        @pl.when(step % 3 == 2)
        def _():
            gather.tick(7 + step // 3, prepare)

    lse[...] = lse_acc[...].T
    leave(lse, "lse")
    leave(att, "att")
    leave(w.at[OUT], "whole", OUT)
    second.wait()
    leave(ct, "cots")

    for n in range(width // tile):
        cols = pl.ds(n * tile, tile)
        branch = nn(att[...], w[OUT, :, cols]) + vec[pl.ds(10, 1), cols]
        bra[:, cols] = branch.astype(HALF)
        mid[:, cols] = xs[:, cols].astype(F32) + vec[pl.ds(2, 1), cols] * branch
    leave(mid, "mid")
    leave(bra, "bra")
    tick(9)

    @pl.loop(0, rows // block)
    def _(i):
        part_rows = pl.ds(pl.multiple_of(i * block, block), block)
        hat, _ = norm_parts(mid[part_rows, :])
        nb[part_rows, :] = (hat * (1.0 + row(4)) + row(3)).astype(HALF)
        gbh[part_rows, :] = (ct[part_rows, :].astype(F32) * row(5)).astype(HALF)
        bb[part_rows, :] = jnp.broadcast_to(row(11), (block, width))
        gnb[part_rows, :] = jnp.zeros((block, width), F32)

    leave(nb, "nb")
    leave(gbh, "gbh")

    def ff_copies(j, slot):
        return (
            pltpu.make_async_copy(hid.at[slot], outs["hid"].at[j], ff_sem.at[0, slot]),
            pltpu.make_async_copy(gph.at[slot], outs["gph"].at[j], ff_sem.at[1, slot]),
        )

    @pl.loop(0, 4)
    def _(j):
        slot = j % 2
        up, down = FEED + 2 * j, FEED + 2 * j + 1

        @pl.when(j >= 2)
        def _():
            for copy in ff_copies(j, slot):
                copy.wait()

        for n in range(width // tile):
            cols = pl.ds(n * tile, tile)
            pre = nn(nb[...], w[up, :, cols]) + vec[pl.ds(12 + j, 1), cols]
            grad = nt(gbh[...], w[down, cols, :])
            value, slope = gelu_both(pre)
            grad = grad * slope
            ups[pl.ds(j, 1), cols] = column_sum(grad)
            hid[slot, :, cols] = value.astype(HALF)
            gph[slot, :, cols] = grad.astype(HALF)
        for copy in ff_copies(j, slot):
            copy.start()
        gather.tick(10 + 2 * j, prepare)
        for n in range(width // tile):
            cols = pl.ds(n * tile, tile)
            bb[:, cols] = bb[:, cols] + nn(hid[slot], w[down, :, cols])
            gnb[:, cols] = gnb[:, cols] + nt(gph[slot], w[up, cols, :])
        gather.tick(11 + 2 * j, prepare)

    leave(gnb, "gnb")
    ups[pl.ds(4, 4), :] = jnp.zeros((4, width), F32)

    @pl.loop(0, rows // block)
    def _(i):
        part_rows = pl.ds(pl.multiple_of(i * block, block), block)
        branch = bb[part_rows, :]
        grad = ct[part_rows, :].astype(F32)
        na[part_rows, :] = (mid[part_rows, :] + row(5) * branch).astype(HALF)
        ups[pl.ds(4, 1), :] = ups[pl.ds(4, 1), :] + column_sum(grad * branch)
        ups[pl.ds(5, 1), :] = ups[pl.ds(5, 1), :] + column_sum(grad)

    leave(na, "outb")
    leave(ups, "ups")
    for slot in range(2):
        for copy in ff_copies(slot, slot):
            copy.wait()
    for copy in exits:
        copy.wait()
    gather.drain()
    first.drain()
    second.drain()
    for f in range(1, 8):
        small_copy(f).wait_send()
        mod_copy(f).wait_send()
    for k in range(2):
        kv_copy(k).wait_send()


def forward(tokens, cot, qkv_w, out_w, up_w, down_w, small, ada):
    depth, width = qkv_w.shape[0], out_w.shape[1]
    rows = tokens.shape[0] * tokens.shape[1]
    sds = jax.ShapeDtypeStruct
    flat, real = sds((rows, width), HALF), sds((rows, width), F32)
    shapes = dict(
        whole=sds((4, width, width), HALF),
        xs=flat,
        cots=flat,
        qkv=sds((3, rows, width), HALF),
        kvo=sds((2, rows, width), HALF),
        att=flat,
        lse=sds((LANES, rows), F32),
        mid=real,
        bra=flat,
        nb=flat,
        hid=sds((4, rows, width), HALF),
        gph=sds((4, rows, width), HALF),
        gbh=flat,
        outb=flat,
        gnb=real,
        vec=sds((16, width), F32),
        silu=sds((16, LANES), HALF),
        ups=sds((8, width), F32),
    )
    hbm = pl.BlockSpec(memory_space=pl.ANY)
    vmem = pl.BlockSpec(memory_space=pltpu.VMEM)
    dma = pltpu.SemaphoreType.DMA
    half = lambda *s: pltpu.VMEM(s, HALF)
    full = lambda *s: pltpu.VMEM(s, F32)
    scratch = [
        half(CHUNKS, width, width),
        full(8, 32, LANES),
        full(16, 48, LANES),
        full(8, 48, LANES),
        full(48, LANES),
        full(16, width),
        half(16, LANES),
        half(rows, width),
        half(rows, width),
        half(rows, width),
        half(3, rows, width),
        half(2, rows, width),
        half(rows, width),
        full(rows, LANES),
        full(LANES, rows),
        full(rows, width),
        half(rows, width),
        half(rows, width),
        half(rows, width),
        full(rows, width),
        full(rows, width),
        half(2, rows, width),
        half(2, rows, width),
        full(8, width),
        dma((CHUNKS, 9)),
        dma((CHUNKS, 9)),
        dma((CHUNKS,)),
        dma((2, 4)),
        dma((2, 4)),
        dma((7,)),
        dma((7,)),
        dma((7,)),
        dma((7,)),
        dma((2,)),
        dma((2,)),
        dma((24,)),
        dma((2, 2)),
    ]
    got = pl.pallas_call(
        forward_kernel,
        out_shape=tuple(shapes[name] for name in FORWARD_OUTS),
        in_specs=[hbm] * 6 + [vmem] * 2,
        out_specs=(hbm,) * len(FORWARD_OUTS),
        scratch_shapes=scratch,
        compiler_params=pltpu.CompilerParams(
            collective_id=1, has_side_effects=True, vmem_limit_bytes=67043328
        ),
        name="forward",
    )(tokens, cot, qkv_w, out_w, up_w, down_w, small, ada)
    return dict(zip(FORWARD_OUTS, got))


class Reduce:
    RING = 3
    DEEP = 4

    def __init__(self, here, bufs, send, recv, credit):
        self.here = here
        (self.dw, self.rc, self.rx, self.ry, self.t, self.ry2, self.rx2, self.r, self.rz1, self.q, self.rz2, self.out) = bufs
        self.send, self.recv, self.credit = send, recv, credit
        self.depth, self.cols = self.out.shape[1:]
        self.half, self.rows = self.cols // 2, self.depth // 2
        side = here.z % 2
        self.mine = pl.ds(pl.multiple_of(side * self.rows, self.rows), self.rows)
        self.away = pl.ds(pl.multiple_of((1 - side) * self.rows, self.rows), self.rows)

    def _copy(self, i, slot, arriving=False):
        here = self.here
        s, deep = lax.rem(i, self.RING), lax.rem(i, self.DEEP)
        low, high = pl.ds(0, self.half), pl.ds(self.half, self.half)
        if slot == 0:
            src, dst, peer = self.dw.at[s, :, :, 1 - here.c], self.rc.at[deep], here.plane(1)
        elif slot == 1:
            src, dst, peer = self.dw.at[s, :, 1 - here.x, here.c, :, low], self.rx.at[deep], here.plane(2)
        elif slot == 2:
            src, dst, peer = self.dw.at[s, 1 - here.y, :, here.c, :, high], self.ry.at[deep], here.plane(4)
        elif slot == 3:
            src, dst, peer = self.t.at[s, 0, 1 - here.y], self.ry2.at[i], here.plane(4)
        elif slot == 4:
            src, dst, peer = self.t.at[s, 1, 1 - here.x], self.rx2.at[i], here.plane(2)
        elif slot == 5:
            src, dst, peer = self.r.at[s, self.away, :], self.rz1.at[i], here.line(1)
        elif slot == 6:
            src, dst, peer = self.q.at[s], self.rz2.at[i], here.line(2)
        else:
            rows = self.away if arriving else self.mine
            src = dst = self.out.at[i, rows, :]
            peer = here.line(1)
        return remote(src, dst, self.send.at[i, slot], self.recv.at[i, slot], peer)

    def _sent(self, i, *slots):
        def wait(k):
            for slot in slots:
                self._copy(k, slot).wait_send()

        guarded(0, i - self.RING, CHUNKS, wait)

    def _spend(self, i, *kinds):
        def wait(k):
            for kind in kinds:
                pl.semaphore_wait(self.credit.at[kind], 1)

        guarded(self.DEEP, i, CHUNKS, wait)

    def _grant(self, i, kind, flip):
        def signal(k):
            pl.semaphore_signal(
                self.credit.at[kind], inc=1, device_id=self.here.plane(flip), device_id_type=MESH_ID
            )

        guarded(0, i, CHUNKS - self.DEEP, signal)

    def produce(self, i, left_t, right):
        s = lax.rem(i, self.RING)
        self._sent(i, 0, 1, 2)
        tile = 256
        for n in range(self.cols // tile):
            cols = pl.ds(n * tile, tile)
            value = nn(left_t[...], right[:, cols]).astype(HALF)
            for k in range(8):
                self.dw[s, k // 4, k // 2 % 2, k % 2, :, cols] = value[
                    k * self.depth : (k + 1) * self.depth
                ]
        self._spend(i, 0)
        self._copy(i, 0).start()

    def plane(self, i):
        s, deep = lax.rem(i, self.RING), lax.rem(i, self.DEEP)
        c = self.here.c
        self._copy(i, 0, True).wait_recv()
        for y in range(2):
            for x in range(2):
                self.dw[s, y, x, c] = (
                    self.dw[s, y, x, c].astype(F32) + self.rc[deep, y, x].astype(F32)
                ).astype(HALF)
        self._grant(i, 0, 1)
        self._spend(i, 1, 2)
        self._copy(i, 1).start()
        self._copy(i, 2).start()

    def cross(self, i):
        s, deep = lax.rem(i, self.RING), lax.rem(i, self.DEEP)
        here = self.here
        low, high = pl.ds(0, self.half), pl.ds(self.half, self.half)
        self._copy(i, 1, True).wait_recv()
        self._copy(i, 2, True).wait_recv()
        self._sent(i, 3, 4)
        for k in range(2):
            self.t[s, 0, k] = (
                self.dw[s, k, here.x, here.c, :, low].astype(F32) + self.rx[deep, k].astype(F32)
            ).astype(HALF)
            self.t[s, 1, k] = (
                self.dw[s, here.y, k, here.c, :, high].astype(F32) + self.ry[deep, k].astype(F32)
            ).astype(HALF)
        self._grant(i, 1, 2)
        self._grant(i, 2, 4)
        self._copy(i, 3).start()
        self._copy(i, 4).start()

    def line(self, i):
        s = lax.rem(i, self.RING)
        here = self.here
        self._copy(i, 3, True).wait_recv()
        self._copy(i, 4, True).wait_recv()
        self._sent(i, 5)
        self.r[s, :, pl.ds(0, self.half)] = (
            self.t[s, 0, here.y].astype(F32) + self.ry2[i].astype(F32)
        ).astype(HALF)
        self.r[s, :, pl.ds(self.half, self.half)] = (
            self.t[s, 1, here.x].astype(F32) + self.rx2[i].astype(F32)
        ).astype(HALF)
        self._copy(i, 5).start()

    def far(self, i):
        s = lax.rem(i, self.RING)
        self._copy(i, 5, True).wait_recv()
        self._sent(i, 6)
        self.q[s] = (self.r[s, self.mine, :].astype(F32) + self.rz1[i].astype(F32)).astype(HALF)
        self._copy(i, 6).start()

    def close(self, i):
        s = lax.rem(i, self.RING)
        self._copy(i, 6, True).wait_recv()
        self.out[i, self.mine, :] = (self.q[s].astype(F32) + self.rz2[i].astype(F32)).astype(HALF)
        self._copy(i, 7).start()

    def finish(self, i):
        self._copy(i, 7, True).wait_recv()

    LAGS = (8, 6, 5, 4, 2, 0)

    def tick(self, t):
        steps = (self.finish, self.close, self.far, self.line, self.cross, self.plane)
        for lag, step in zip(self.LAGS, steps):
            guarded(0, t - lag, CHUNKS, step)

    def drain(self):
        for k in range(CHUNKS - self.RING, CHUNKS):
            for slot in range(7):
                self._copy(k, slot).wait_send()

        @pl.loop(0, CHUNKS)
        def _(i):
            self._copy(i, 7).wait_send()


class Collect:
    def __init__(self, here, source, target, send, recv):
        self.here, self.source, self.target = here, source, target
        self.send, self.recv = send, recv
        self.size = target.shape[1] // 2

    def _copies(self):
        here = self.here
        owner, j = here.z // 2, here.z % 2
        dst = self.target.at[j, pl.ds(pl.multiple_of(here.c * self.size, self.size), self.size), :]
        arrive = self.recv.at[2 * j + here.c]
        for z in range(4):
            own = jnp.logical_and(here.z == z, here.c == owner)
            src = self.source.at[pl.ds(z * self.size, self.size), :]
            yield own, src, dst, self.send.at[z], arrive, (here.d - here.c + owner, z)

    def start(self):
        for own, src, dst, send, recv, peer in self._copies():

            @pl.when(own)
            def _():
                pltpu.make_async_copy(src, dst, recv).start()

            @pl.when(jnp.logical_not(own))
            def _():
                remote(src, dst, send, recv, peer).start()

    def finish(self):
        for j in range(2):
            for c in range(2):
                dst = self.target.at[j, pl.ds(c * self.size, self.size), :]
                src = self.source.at[pl.ds(0, self.size), :]
                pltpu.make_async_copy(src, dst, self.recv.at[2 * j + c]).wait()
        for own, src, dst, send, recv, peer in self._copies():

            @pl.when(jnp.logical_not(own))
            def _():
                remote(src, dst, send, recv, peer).wait_send()


BACKWARD_INS = (
    "whole",
    "xs",
    "cots",
    "gbh",
    "qkv",
    "kvo",
    "att",
    "lse",
    "mid",
    "bra",
    "nb",
    "hid",
    "gph",
    "outb",
    "gnb",
    "vec",
    "ups",
    "ada",
)
BACKWARD_OUTS = ("output", "tokens", "shares", "gmod", "condp", "biases")


def backward_kernel(*refs):
    ins = dict(zip(BACKWARD_INS, refs))
    refs = refs[len(BACKWARD_INS) :]
    outs = dict(zip(BACKWARD_OUTS, refs))
    (
        w,
        xs,
        ct,
        gbh,
        qkv,
        kvo,
        kvr,
        att,
        lse,
        mid,
        bra,
        nb_t,
        tmp_t,
        hid,
        gph,
        gnb,
        ga,
        sums,
        dw,
        rc,
        rx,
        ry,
        t,
        ry2,
        rx2,
        r,
        rz1,
        q_,
        rz2,
        shares,
        gs,
        gs_in,
        gmod,
        cpart,
        condp,
        bpart,
        bin_,
        bz,
        biases,
        ld_sem,
        ff_sem,
        r_send,
        r_recv,
        credit,
        o_send,
        o_recv,
        kv_send,
        kv_recv,
        b_send,
        b_recv,
        bz_send,
        bz_recv,
        g_send,
        g_recv,
        m_send,
        m_recv,
        c_send,
        c_recv,
        out_sem,
    ) = refs[len(BACKWARD_OUTS) :]
    here = Place()
    d, z, c, p = here.d, here.z, here.c, here.p
    vec, ups, ada = ins["vec"], ins["ups"], ins["ada"]
    rows, width = xs.shape
    tile, block = 256, 128
    depth = shares.shape[1]

    loads = {}

    def load(name, src, dst):
        loads[name] = pltpu.make_async_copy(src, dst, ld_sem.at[len(loads)])
        loads[name].start()

    def need(*names):
        for name in names:
            loads[name].wait()

    def feed(which, j):
        k = 0 if which is hid else 1
        name = "hid" if which is hid else "gph"
        return pltpu.make_async_copy(ins[name].at[j], which.at[lax.rem(j, 2)], ff_sem.at[k, lax.rem(j, 2)])

    order = (
        ("nb", ins["nb"], ga),
        ("mid", ins["mid"], mid),
        ("gnb", ins["gnb"], gnb),
        ("cots", ins["cots"], ct),
        ("bra", ins["bra"], bra),
        ("att", ins["att"], att),
        ("out_w", ins["whole"].at[OUT], w.at[0]),
        ("gbh", ins["gbh"], gbh),
        ("qkv", ins["qkv"], qkv),
        ("kvo", ins["kvo"], kvo),
        ("lse", ins["lse"], lse),
        ("k_w", ins["whole"].at[KEYS], w.at[1]),
        ("v_w", ins["whole"].at[VALUES], w.at[2]),
        ("xs", ins["xs"], xs),
    )
    load(*order[0])
    feed(gph, 0).start()
    for item in order[1:8]:
        load(*item)
    feed(hid, 0).start()
    for item in order[8:]:
        load(*item)
    feed(gph, 1).start()
    feed(hid, 1).start()

    line_peers = [
        (2 * jnp.bitwise_xor(p, fp) + c, jnp.bitwise_xor(z, fz))
        for fp in range(4)
        for fz in range(4)
        if fp or fz
    ]
    greet(
        line_peers
        + [here.plane(f) for f in (1, 3, 5, 7)]
        + [(jnp.bitwise_xor(d, 1), jnp.bitwise_xor(z, f)) for f in range(1, 4)]
    )

    red = Reduce(
        here, (dw, rc, rx, ry, t, ry2, rx2, r, rz1, q_, rz2, shares), r_send, r_recv, credit
    )
    output = Collect(here, ins["outb"], outs["output"], o_send.at[0], o_recv.at[0])
    output.start()

    def row(i):
        return vec[pl.ds(i, 1), :]

    sums[...] = jnp.zeros_like(sums)

    def add(i, value):
        sums[pl.ds(i, 1), :] = sums[pl.ds(i, 1), :] + value

    need("nb")
    nb_t[...] = ga[...].T
    feed(gph, 0).wait()
    red.produce(0, nb_t, gph.at[0])
    need("mid", "gnb", "cots", "bra")

    @pl.loop(0, rows // block)
    def _(i):
        part_rows = pl.ds(pl.multiple_of(i * block, block), block)
        hat, inverse = norm_parts(mid[part_rows, :])
        grad = gnb[part_rows, :]
        add(3, column_sum(grad))
        add(4, column_sum(grad * hat))
        grad_mid = ct[part_rows, :].astype(F32) + norm_grad(grad, hat, inverse, row(4))
        add(2, column_sum(grad_mid * bra[part_rows, :].astype(F32)))
        add(6, column_sum(grad_mid))
        mid[part_rows, :] = grad_mid
        bra[part_rows, :] = (grad_mid * row(2)).astype(HALF)

    red.tick(0)
    need("att")
    tmp_t[...] = att[...].T
    red.produce(1, tmp_t, bra)
    need("out_w")
    for n in range(width // tile):
        cols = pl.ds(n * tile, tile)
        ga[:, cols] = nt(bra[...], w[0, cols, :]).astype(HALF)
    load("q_w", ins["whole"].at[QUERIES], w.at[0])
    red.tick(1)
    need("gbh", "qkv", "kvo", "lse")

    span = 256
    low = lax.broadcasted_iota(jnp.int32, (span, LANES), 1) < HD
    upper = lax.broadcasted_iota(jnp.int32, (LANES, rows), 0) < HD
    pick = lax.broadcasted_iota(jnp.int32, (8, LANES), 0) == (
        lax.broadcasted_iota(jnp.int32, (8, LANES), 1) // HD
    )
    pick = jnp.where(pick, 1.0, 0.0).astype(HALF)

    def attend_back(step):
        cols = pl.ds(pl.multiple_of(step * LANES, LANES), LANES)
        q = qkv[0, :, cols] * HALF(HD**-0.5)
        grad = ga[:, cols]
        product = grad.astype(F32) * att[:, cols].astype(F32)
        top = product.astype(HALF)
        rest = (product - top.astype(F32)).astype(HALF)
        inner = nt(pick, top) + nt(pick, rest)
        dq_t = [jnp.zeros((LANES, rows), F32) for _ in range(2)]
        for k_ref, v_ref in ((qkv.at[1], qkv.at[2]), (kvo.at[0], kvo.at[1])):
            for start in range(0, rows, span):
                part_rows = pl.ds(start, span)
                k = k_ref[part_rows, cols]
                v = v_ref[part_rows, cols]
                k_t = k.T
                dks, dvs = [], []
                for head in range(2):
                    own = low if head == 0 else jnp.logical_not(low)
                    logsum = lse[pl.ds(2 * step + head, 1), :]
                    scores = nt(jnp.where(own, k, jnp.zeros_like(k)), q)
                    probs = jnp.exp(scores - logsum)
                    dvs.append(nn(probs.astype(HALF), grad))
                    gp = nt(jnp.where(own, v, jnp.zeros_like(v)), grad)
                    score_grad = (probs * (gp - inner[head : head + 1, :])).astype(HALF)
                    dks.append(nn(score_grad, q))
                    dq_t[head] = dq_t[head] + nn(k_t, score_grad)
                k_ref[part_rows, cols] = jnp.where(low, dks[0], dks[1]).astype(HALF)
                v_ref[part_rows, cols] = jnp.where(low, dvs[0], dvs[1]).astype(HALF)
        dq = jnp.where(upper, dq_t[0], dq_t[1]).T * HD**-0.5
        qkv[0, :, cols] = dq.astype(HALF)

    @pl.loop(0, 4)
    def _(j):
        slot = lax.rem(j, 2)
        feed(hid, j).wait()
        tmp_t[...] = hid[slot].T
        red.produce(2 + 2 * j, tmp_t, gbh)

        @pl.when(j < 2)
        def _():
            feed(hid, j + 2).start()
            feed(gph, j + 2).start()

        attend_back(2 * j)
        red.tick(2 + 2 * j)

        @pl.when(j < 3)
        def _():
            feed(gph, j + 1).wait()
            red.produce(3 + 2 * j, nb_t, gph.at[1 - slot])

        attend_back(2 * j + 1)

        @pl.when(j < 3)
        def _():
            red.tick(3 + 2 * j)

    def kv_copy(k):
        return remote(kvo.at[k], kvr.at[k], kv_send.at[k], kv_recv.at[k], here.plane(1))

    kv_copy(1).start()
    kv_copy(0).start()
    need("xs")

    @pl.loop(0, rows // block)
    def _(i):
        part_rows = pl.ds(pl.multiple_of(i * block, block), block)
        hat, _ = norm_parts(xs[part_rows, :].astype(F32))
        ga[part_rows, :] = (hat * (1.0 + row(1)) + row(0)).astype(HALF)

    tmp_t[...] = ga[...].T
    red.produce(9, tmp_t, qkv.at[0])
    red.tick(9)
    for k in (1, 0):
        kv_copy(k).wait_recv()

        @pl.loop(0, rows // block)
        def _(i):
            part_rows = pl.ds(pl.multiple_of(i * block, block), block)
            qkv[1 + k, part_rows, :] = (
                qkv[1 + k, part_rows, :].astype(F32) + kvr[k, part_rows, :].astype(F32)
            ).astype(HALF)

        red.produce(11 - k, tmp_t, qkv.at[1 + k])
        red.tick(11 - k)

    sums[pl.ds(7, 1), :] = column_sum(qkv[0].astype(F32))
    sums[pl.ds(8, 1), :] = column_sum(qkv[2].astype(F32))
    sums[pl.ds(6, 1), :] = sums[pl.ds(6, 1), :] * row(2)
    sums[pl.ds(9, 1), :] = ups[pl.ds(5, 1), :] * row(5)
    for k in range(8):
        lanes = pl.ds(k * LANES, LANES)
        for s in range(2):
            source = 7 + k // 4
            bpart[k, pl.ds(s, 1), :] = sums[pl.ds(source, 1), pl.ds((2 * (k % 4) + s) * LANES, LANES)]
        bpart[k, pl.ds(2, 1), :] = sums[pl.ds(6, 1), lanes]
        for j in range(4):
            bpart[k, pl.ds(3 + j, 1), :] = ups[pl.ds(j, 1), lanes]
        bpart[k, pl.ds(7, 1), :] = sums[pl.ds(9, 1), lanes]

    def bias_copy(f):
        flip = jnp.bitwise_xor(d, f)
        return remote(bpart.at[flip], bin_.at[d], b_send.at[f - 1], b_recv.at[f - 1], here.plane(f))

    for f in range(1, 8):
        bias_copy(f).start()
    bin_[d] = bpart[d]

    need("q_w", "k_w", "v_w")
    for n in range(width // tile):
        cols = pl.ds(n * tile, tile)
        gnb[:, cols] = (
            nt(qkv[0], w[0, cols, :]) + nt(qkv[1], w[1, cols, :]) + nt(qkv[2], w[2, cols, :])
        )
    red.tick(12)

    @pl.loop(0, rows // block)
    def _(i):
        part_rows = pl.ds(pl.multiple_of(i * block, block), block)
        hat, inverse = norm_parts(xs[part_rows, :].astype(F32))
        grad = gnb[part_rows, :]
        add(0, column_sum(grad))
        add(1, column_sum(grad * hat))
        att[part_rows, :] = (
            mid[part_rows, :] + norm_grad(grad, hat, inverse, row(1))
        ).astype(HALF)

    back = Collect(here, att, outs["tokens"], o_send.at[1], o_recv.at[1])
    back.start()

    sums[pl.ds(5, 1), :] = ups[pl.ds(4, 1), :]
    for i in range(6):
        for k in range(8):
            gs[pl.ds(8 * i + k, 1), :] = sums[pl.ds(i, 1), pl.ds(k * LANES, LANES)]
    pair = remote(gs, gs_in, g_send.at[0], g_recv.at[0], here.plane(1))
    pair.start()
    for f in range(1, 8):
        bias_copy(f).wait_recv()
    total = bin_[0]
    for k in range(1, 8):
        total = total + bin_[k]
    bz[z] = total

    def line_copy(f):
        dst = bz.at[z]
        return remote(dst, dst, bz_send.at[f - 1], bz_recv.at[f - 1], here.line(f))

    for f in range(1, 4):
        line_copy(f).start()
    red.tick(13)
    pair.wait_recv()
    latent = 4 * p + z
    gmod[latent] = gs[...] + gs_in[...]

    def mod_copy(k):
        return remote(
            gmod.at[latent], gmod.at[latent], m_send.at[k], m_recv.at[k], line_peers[k]
        )

    for k in range(15):
        mod_copy(k).start()
    red.tick(14)
    for k in range(15):
        mod_copy(k).wait_recv()
    for i in range(6):
        piece = jnp.concatenate([gmod[:, 8 * i + k, :] for k in range(8)], axis=1)
        term = nt(piece.astype(HALF), ada[:, pl.ds(i * width, width)])
        share = term if i == 0 else share + term
    for k in range(8):
        cpart[k, pl.ds(0, 2), :] = share[2 * k : 2 * k + 2]

    def cond_copy(f):
        flip = jnp.bitwise_xor(d, f)
        return remote(cpart.at[flip], condp.at[d], c_send.at[f - 1], c_recv.at[f - 1], here.plane(f))

    for f in range(1, 8):
        cond_copy(f).start()
    condp[d] = cpart[d]
    red.tick(15)
    for f in range(1, 4):
        line_copy(f).wait_recv()
    biases[...] = bz[0] + bz[1] + bz[2] + bz[3]
    red.tick(16)
    red.tick(17)
    red.tick(18)
    red.tick(19)
    exits = [
        pltpu.make_async_copy(src, outs[name], out_sem.at[k])
        for k, (src, name) in enumerate(
            ((shares, "shares"), (gmod, "gmod"), (biases, "biases"))
        )
    ]
    for copy in exits:
        copy.start()
    for f in range(1, 8):
        cond_copy(f).wait_recv()
    last = pltpu.make_async_copy(condp, outs["condp"], out_sem.at[3])
    last.start()
    red.drain()
    output.finish()
    back.finish()
    pair.wait_send()
    for k in range(2):
        kv_copy(k).wait_send()
    for f in range(1, 8):
        bias_copy(f).wait_send()
        cond_copy(f).wait_send()
    for f in range(1, 4):
        line_copy(f).wait_send()
    for k in range(15):
        mod_copy(k).wait_send()
    for copy in exits:
        copy.wait()
    last.wait()


def backward(f, ada, shape):
    lats, part, width = shape
    rows = lats * part
    depth = ada.shape[0]
    half_cols, half_rows = width // 2, depth // 2
    sds = jax.ShapeDtypeStruct
    hbm = pl.BlockSpec(memory_space=pl.ANY)
    vmem = pl.BlockSpec(memory_space=pltpu.VMEM)
    dma = pltpu.SemaphoreType.DMA
    half = lambda *s: pltpu.VMEM(s, HALF)
    full = lambda *s: pltpu.VMEM(s, F32)
    ring, deep = Reduce.RING, Reduce.DEEP
    scratch = [
        half(3, width, width),
        half(rows, width),
        half(rows, width),
        half(rows, width),
        half(3, rows, width),
        half(2, rows, width),
        half(2, rows, width),
        half(rows, width),
        full(LANES, rows),
        full(rows, width),
        half(rows, width),
        half(width, rows),
        half(width, rows),
        half(2, rows, width),
        half(2, rows, width),
        full(rows, width),
        half(rows, width),
        full(16, width),
        half(ring, 2, 2, 2, depth, width),
        half(deep, 2, 2, depth, width),
        half(deep, 2, depth, half_cols),
        half(deep, 2, depth, half_cols),
        half(ring, 2, 2, depth, half_cols),
        half(CHUNKS, depth, half_cols),
        half(CHUNKS, depth, half_cols),
        half(ring, depth, width),
        half(CHUNKS, half_rows, width),
        half(ring, half_rows, width),
        half(CHUNKS, half_rows, width),
        half(CHUNKS, depth, width),
        full(48, LANES),
        full(48, LANES),
        full(16, 48, LANES),
        full(8, 8, LANES),
        full(8, 8, LANES),
        full(8, 8, LANES),
        full(8, 8, LANES),
        full(4, 8, LANES),
        full(8, LANES),
        dma((20,)),
        dma((2, 2)),
        dma((CHUNKS, 8)),
        dma((CHUNKS, 8)),
        pltpu.SemaphoreType.REGULAR((3,)),
        dma((2, 4)),
        dma((2, 4)),
        dma((2,)),
        dma((2,)),
        dma((7,)),
        dma((7,)),
        dma((3,)),
        dma((3,)),
        dma((1,)),
        dma((1,)),
        dma((15,)),
        dma((15,)),
        dma((7,)),
        dma((7,)),
        dma((4,)),
    ]
    operands = [ada if name == "ada" else f[name] for name in BACKWARD_INS]
    near = ("vec", "ups", "ada")
    got = pl.pallas_call(
        backward_kernel,
        out_shape=(
            sds((lats, part, width), HALF),
            sds((lats, part, width), HALF),
            sds((CHUNKS, depth, width), HALF),
            sds((16, 48, LANES), F32),
            sds((8, 8, LANES), F32),
            sds((8, LANES), F32),
        ),
        in_specs=[vmem if name in near else hbm for name in BACKWARD_INS],
        out_specs=(hbm,) * len(BACKWARD_OUTS),
        scratch_shapes=scratch,
        compiler_params=pltpu.CompilerParams(
            collective_id=2, has_side_effects=True, vmem_limit_bytes=67043328
        ),
        name="backward",
    )(*operands)
    return dict(zip(BACKWARD_OUTS, got))


def body_any(
    tokens,
    condition,
    ada_weight,
    ada_bias,
    qkv_weight,
    qv_bias,
    out_weight,
    out_bias,
    up_weight,
    up_bias,
    down_weight,
    down_bias,
    cotangent,
):
    lats, part, width = tokens.shape
    dp = lax.axis_size("dp")
    seq = lax.axis_size("seq")
    me = lax.axis_index("dp")
    z = lax.axis_index("seq")
    core = me % 2
    pair = me // 2
    chip_lats = 2 * lats
    sub = seq // chip_lats
    first = core == 0

    def flip(x):
        return lax.ppermute(x, "dp", [(i, i ^ 1) for i in range(dp)])

    def shift(x, by):
        if by % sub == 0:
            return x
        return lax.ppermute(
            x, "seq", [(i, i // sub * sub + (i - by) % sub) for i in range(seq)]
        )

    def spread(x):
        halves = x.reshape(lats, 2, part // 2, width)
        keep = lax.dynamic_index_in_dim(halves, core, 1, keepdims=False)
        give = lax.dynamic_index_in_dim(halves, 1 - core, 1, keepdims=False)
        got = flip(give)
        both = jnp.concatenate(
            [jnp.where(first, keep, got), jnp.where(first, got, keep)], axis=0
        )
        both = both.reshape(seq, part // (2 * sub), width)
        return lax.all_to_all(both, "seq", 0, 0, tiled=True).reshape(-1, width)

    def collect(x):
        both = x.reshape(seq, part // (2 * sub), width)
        both = lax.all_to_all(both, "seq", 0, 0, tiled=True)
        both = both.reshape(2, lats, part // 2, width)
        mine = lax.dynamic_index_in_dim(both, core, 0, keepdims=False)
        give = lax.dynamic_index_in_dim(both, 1 - core, 0, keepdims=False)
        got = flip(give)
        return jnp.stack(
            [jnp.where(first, mine, got), jnp.where(first, got, mine)], axis=1
        ).reshape(lats, part, width)

    small = jnp.concatenate(
        [ada_bias, qv_bias, out_bias, up_bias, down_bias, condition.reshape(-1)]
    )
    small_all = lax.all_gather(small, "dp", axis=0, tiled=False)
    sizes = [a.shape[0] for a in (ada_bias, qv_bias, out_bias, up_bias, down_bias)]
    cuts = [0]
    for size in sizes:
        cuts.append(cuts[-1] + size)
    ada_bias_full, qv_full, out_bias_full, up_bias_full, down_bias_full = [
        small_all[:, a:b].reshape(-1).astype(F32) for a, b in zip(cuts[:-1], cuts[1:])
    ]
    cond_all = small_all[:, cuts[-1] :].reshape(dp * lats, width).astype(F32)
    depth = ada_weight.shape[0]
    silu_all = jax.nn.silu(cond_all).astype(HALF)
    silu_mine = lax.dynamic_slice_in_dim(silu_all, me * depth, depth, axis=1)
    partial = nn(silu_mine, ada_weight)
    row_here = z // sub
    wanted = partial.reshape(dp // 2, chip_lats, 6 * width)
    wanted = lax.dynamic_index_in_dim(wanted, row_here, 1, keepdims=True)
    wanted = jnp.broadcast_to(wanted, (dp // 2, 2, 6 * width)).reshape(dp, 6 * width)
    modulation = lax.psum_scatter(wanted, "dp", scatter_dimension=0, tiled=True)[0]
    modulation = (modulation + ada_bias_full).reshape(6, 1, width)
    shift_a, scale_a, gate_a, shift_b, scale_b, gate_b = [modulation[i] for i in range(6)]

    qkv_full = lax.all_gather(qkv_weight, "dp", axis=0, tiled=True)
    out_full = lax.all_gather(out_weight, "dp", axis=0, tiled=True)
    up_full = lax.all_gather(up_weight, "dp", axis=0, tiled=True)
    down_full = lax.all_gather(down_weight, "dp", axis=0, tiled=True)

    rows = spread(tokens).astype(F32)
    cot = spread(cotangent).astype(F32)

    hat_a, inverse_a = norm_parts(rows)
    normed_a = (hat_a * (1.0 + scale_a) + shift_a).astype(HALF)
    bias_all = jnp.concatenate([qv_full[:width], jnp.zeros((width,), F32), qv_full[width:]])
    projected = (nn(normed_a, qkv_full) + bias_all).astype(HALF)
    kv = projected[:, width:]
    ways = [(a, s) for s in range(sub) for a in range(2)]
    others = [shift(flip(kv) if a else kv, s) for a, s in ways[1:]]
    attended, logsum = attend(projected, others, width)
    branch_a = nn(attended, out_full) + out_bias_full
    middle = rows + gate_a * branch_a
    hat_b, inverse_b = norm_parts(middle)
    normed_b = (hat_b * (1.0 + scale_b) + shift_b).astype(HALF)
    hidden_pre = nn(normed_b, up_full) + up_bias_full
    hidden = gelu_tanh(hidden_pre).astype(HALF)
    branch_b = nn(hidden, down_full) + down_bias_full
    output = collect((middle + gate_b * branch_b).astype(HALF))

    grad_gate_b = jnp.sum(cot * branch_b, axis=0)
    grad_branch_b = cot * gate_b
    down_bias_grad = jnp.sum(grad_branch_b, axis=0)
    grad_branch_half = grad_branch_b.astype(HALF)
    down_weight_grad = tn(hidden, grad_branch_half).astype(HALF)
    grad_hidden = nt(grad_branch_half, down_full)
    _, gelu_back = jax.vjp(gelu_tanh, hidden_pre)
    grad_pre = gelu_back(grad_hidden)[0]
    up_bias_grad = jnp.sum(grad_pre, axis=0)
    grad_pre_half = grad_pre.astype(HALF)
    up_weight_grad = tn(normed_b, grad_pre_half).astype(HALF)
    grad_normed_b = nt(grad_pre_half, up_full)
    grad_shift_b = jnp.sum(grad_normed_b, axis=0)
    grad_scale_b = jnp.sum(grad_normed_b * hat_b, axis=0)
    grad_middle = cot + norm_grad(grad_normed_b, hat_b, inverse_b, scale_b)
    grad_gate_a = jnp.sum(grad_middle * branch_a, axis=0)
    grad_branch_a = grad_middle * gate_a
    out_bias_grad = jnp.sum(grad_branch_a, axis=0)
    grad_branch_a_half = grad_branch_a.astype(HALF)
    out_weight_grad = tn(attended, grad_branch_a_half).astype(HALF)
    grad_attended = nt(grad_branch_a_half, out_full).astype(HALF)

    results = attend_grad(projected, others, grad_attended, attended, logsum, width)
    count = len(ways)
    grad_query = results[0]
    grad_keys = results[1 : 1 + count]
    grad_values = results[1 + count :]
    grad_kv = [jnp.concatenate([k, v], axis=1) for k, v in zip(grad_keys, grad_values)]
    total_kv = grad_kv[0].astype(F32)
    for (a, s), part_kv in zip(ways[1:], grad_kv[1:]):
        back = shift(part_kv, -s)
        total_kv = total_kv + (flip(back) if a else back).astype(F32)
    grad_projected = jnp.concatenate([grad_query, total_kv.astype(HALF)], axis=1)
    qkv_weight_grad = tn(normed_a, grad_projected).astype(HALF)
    grad_proj_float = grad_projected.astype(F32)
    qv_bias_grad = jnp.concatenate(
        [
            jnp.sum(grad_proj_float[:, :width], axis=0),
            jnp.sum(grad_proj_float[:, 2 * width :], axis=0),
        ]
    )
    grad_normed_a = nt(grad_projected, qkv_full)
    grad_shift_a = jnp.sum(grad_normed_a, axis=0)
    grad_scale_a = jnp.sum(grad_normed_a * hat_a, axis=0)
    grad_tokens = grad_middle + norm_grad(grad_normed_a, hat_a, inverse_a, scale_a)
    tokens_grad = collect(grad_tokens.astype(HALF)).astype(F32)

    grad_mod = jnp.concatenate(
        [grad_shift_a, grad_scale_a, grad_gate_a, grad_shift_b, grad_scale_b, grad_gate_b]
    )
    every = lax.all_gather(grad_mod, "seq", axis=0, tiled=False)
    every = lax.all_gather(every, "dp", axis=0, tiled=False)
    every = every.reshape(dp // 2, 2, chip_lats, sub, 6 * width).sum(axis=(1, 3))
    every = every.reshape(dp * lats, 6 * width)
    every_half = every.astype(HALF)
    ada_weight_grad = tn(silu_mine, every_half)
    bias_len = ada_bias.shape[0]
    ada_bias_grad = jnp.sum(
        lax.dynamic_slice_in_dim(every, me * bias_len, bias_len, axis=1), axis=0
    )
    cond_part = nt(every_half, ada_weight).reshape(dp, lats, depth)
    cond_part = lax.all_to_all(cond_part, "dp", 0, 0, tiled=True)
    cond_part = cond_part.transpose(1, 0, 2).reshape(lats, width)
    cond_float = condition.astype(F32)
    sigmoid_cond = jax.nn.sigmoid(cond_float)
    silu_slope = sigmoid_cond * (1.0 + cond_float * (1.0 - sigmoid_cond))
    condition_grad = silu_slope * cond_part

    def reduce_weight(grad):
        share = lax.psum_scatter(grad, "dp", scatter_dimension=0, tiled=True)
        return lax.psum(share, "seq").astype(F32)

    bias_parts = jnp.concatenate(
        [
            b.reshape(dp, -1)
            for b in (qv_bias_grad, out_bias_grad, up_bias_grad, down_bias_grad)
        ],
        axis=1,
    )
    bias_parts = lax.psum_scatter(bias_parts, "dp", scatter_dimension=0, tiled=True)
    bias_parts = lax.psum(bias_parts, "seq")[0]
    cuts = [c - sizes[0] for c in cuts[1:]]
    qv_g, ob_g, ub_g, db_g = [bias_parts[a:b] for a, b in zip(cuts[:-1], cuts[1:])]
    return (
        output,
        tokens_grad,
        condition_grad,
        ada_weight_grad,
        ada_bias_grad,
        reduce_weight(qkv_weight_grad),
        qv_g,
        reduce_weight(out_weight_grad),
        ob_g,
        reduce_weight(up_weight_grad),
        ub_g,
        reduce_weight(down_weight_grad),
        db_g,
    )


def body(
    tokens,
    condition,
    ada_weight,
    ada_bias,
    qkv_weight,
    qv_bias,
    out_weight,
    out_bias,
    up_weight,
    up_bias,
    down_weight,
    down_bias,
    cotangent,
):
    lats, part, width = tokens.shape
    dp = lax.axis_size("dp")
    seq = lax.axis_size("seq")
    if (dp, seq, lats) != (8, 4, 2):
        return body_any(
            tokens,
            condition,
            ada_weight,
            ada_bias,
            qkv_weight,
            qv_bias,
            out_weight,
            out_bias,
            up_weight,
            up_bias,
            down_weight,
            down_bias,
            cotangent,
        )
    me = lax.axis_index("dp")
    depth = ada_weight.shape[0]
    wide = dp * up_bias.shape[0]
    cut = wide // (4 * dp)
    small = jnp.concatenate(
        [
            ada_bias.reshape(-1, LANES),
            qv_bias.reshape(-1, LANES),
            out_bias.reshape(-1, LANES),
            up_bias.reshape(-1, LANES),
            down_bias.reshape(-1, LANES),
            jnp.zeros((2, LANES), HALF),
            condition.reshape(-1, LANES),
        ],
        axis=0,
    ).astype(F32)
    f = forward(
        tokens, cotangent, qkv_weight, out_weight, up_weight, down_weight, small, ada_weight
    )
    b = backward(f, ada_weight, tokens.shape)
    shares = b["shares"].astype(F32)
    qkv_g = jnp.concatenate([shares[9], shares[11], shares[10]], axis=1)
    up_g = jnp.stack([shares[0], shares[3], shares[5], shares[7]])
    up_g = up_g.reshape(4, depth, dp, cut).transpose(1, 2, 0, 3).reshape(depth, wide)
    down_g = shares[2:9:2].reshape(4 * cut, width)
    every = b["gmod"]
    ada_weight_grad = tn(f["silu"], every.astype(HALF).reshape(dp * lats, 6 * width))
    ada_bias_grad = lax.dynamic_slice_in_dim(
        jnp.sum(every, axis=0).reshape(-1), me * ada_bias.shape[0], ada_bias.shape[0]
    )
    cond_part = b["condp"][:, :lats].transpose(1, 0, 2).reshape(lats, width)
    cond_float = condition.astype(F32)
    sigmoid_cond = jax.nn.sigmoid(cond_float)
    silu_slope = sigmoid_cond * (1.0 + cond_float * (1.0 - sigmoid_cond))
    biases = b["biases"]
    return (
        b["output"],
        b["tokens"].astype(F32),
        silu_slope * cond_part,
        ada_weight_grad,
        ada_bias_grad,
        qkv_g,
        biases[0:2].reshape(-1),
        shares[1],
        biases[2],
        up_g,
        biases[3:7].reshape(-1),
        down_g,
        biases[7],
    )


def solution(mesh):
    return jax.shard_map(
        body,
        mesh=mesh,
        in_specs=(
            P("dp", "seq", None),
            P("dp", None),
            P("dp", None),
            P("dp"),
            P("dp", None),
            P("dp"),
            P("dp", None),
            P("dp"),
            P("dp", None),
            P("dp"),
            P("dp", None),
            P("dp"),
            P("dp", "seq", None),
        ),
        out_specs=(
            P("dp", "seq", None),
            P("dp", "seq", None),
            P("dp", None),
            P("dp", None),
            P("dp"),
            P("dp", None),
            P("dp"),
            P("dp", None),
            P("dp"),
            P("dp", None),
            P("dp"),
            P("dp", None),
            P("dp"),
        ),
        check_vma=False,
    )
```

```python
import functools

import jax
import jax.numpy as jnp
from jax import lax
from jax.experimental import pallas as pl
from jax.experimental.pallas import tpu as pltpu
from jax.sharding import PartitionSpec as P

HD = 64
LANES = 128
EPSILON = 1e-06
HALF = jnp.bfloat16
F32 = jnp.float32


def nn(a, b):
    return jnp.dot(a, b, preferred_element_type=F32)


def nt(a, b):
    return lax.dot_general(a, b, (((1,), (1,)), ((), ())), preferred_element_type=F32)


def tn(a, b):
    return lax.dot_general(a, b, (((0,), (0,)), ((), ())), preferred_element_type=F32)


def attend_kernel(groups, *refs):
    q_ref = refs[0]
    k_refs = refs[1 : 1 + groups]
    v_refs = refs[1 + groups : 1 + 2 * groups]
    out_ref, lse_ref, lse_acc = refs[1 + 2 * groups :]
    step = pl.program_id(0)
    rows = q_ref.shape[0]
    block = 256
    low = lax.broadcasted_iota(jnp.int32, (block, LANES), 1) < HD
    lane = lax.broadcasted_iota(jnp.int32, (block, LANES), 1)
    for start in range(0, rows, block):
        here = pl.ds(start, block)
        q = q_ref[here, :] * HALF(HD**-0.5)
        pieces = []
        for head in range(2):
            own = low if head == 0 else jnp.logical_not(low)
            qm = jnp.where(own, q, jnp.zeros_like(q))
            scores = [nt(qm, k[...]) for k in k_refs]
            peak = functools.reduce(
                jnp.maximum, [jnp.max(s, axis=-1, keepdims=True) for s in scores]
            )
            raised = [jnp.exp(s - peak) for s in scores]
            total = sum(jnp.sum(e, axis=-1, keepdims=True) for e in raised)
            mixed = sum(nn(e.astype(HALF), v[...]) for e, v in zip(raised, v_refs))
            pieces.append(mixed / total)
            spot = lane == 2 * step + head
            logsum = jnp.broadcast_to(peak + jnp.log(total), (block, LANES))
            lse_acc[here, :] = jnp.where(spot, logsum, lse_acc[here, :])
        out_ref[here, :] = jnp.where(low, pieces[0], pieces[1]).astype(HALF)

    @pl.when(step == pl.num_programs(0) - 1)
    def _():
        lse_ref[...] = lse_acc[...].T


def attend(projected, others, width):
    rows = projected.shape[0]
    groups = 1 + len(others)
    tiles = width // LANES
    col = lambda base: pl.BlockSpec((rows, LANES), lambda i, base=base: (0, base + i))
    return pl.pallas_call(
        functools.partial(attend_kernel, groups),
        grid=(tiles,),
        out_shape=(
            jax.ShapeDtypeStruct((rows, width), HALF),
            jax.ShapeDtypeStruct((LANES, rows), F32),
        ),
        in_specs=[col(0), col(tiles)] + [col(0)] * len(others) + [col(2 * tiles)] + [col(tiles)] * len(others),
        out_specs=(col(0), pl.BlockSpec((LANES, rows), lambda i: (0, 0))),
        scratch_shapes=[pltpu.VMEM((rows, LANES), F32)],
        compiler_params=pltpu.CompilerParams(vmem_limit_bytes=48 << 20),
        name="attend",
    )(projected, projected, *others, projected, *others)


def attend_grad_kernel(groups, *refs):
    q_ref = refs[0]
    k_refs = refs[1 : 1 + groups]
    v_refs = refs[1 + groups : 1 + 2 * groups]
    do_ref, o_ref, lse_ref = refs[1 + 2 * groups : 4 + 2 * groups]
    dq_ref = refs[4 + 2 * groups]
    dk_refs = refs[5 + 2 * groups : 5 + 3 * groups]
    dv_refs = refs[5 + 3 * groups : 5 + 4 * groups]
    step = pl.program_id(0)
    rows = q_ref.shape[0]
    block = 256
    scale = HALF(HD**-0.5)
    q = q_ref[...] * scale
    grad = do_ref[...]
    product = grad.astype(F32) * o_ref[...].astype(F32)
    top = product.astype(HALF)
    rest = (product - top.astype(F32)).astype(HALF)
    pick = lax.broadcasted_iota(jnp.int32, (8, LANES), 0) == (
        lax.broadcasted_iota(jnp.int32, (8, LANES), 1) // HD
    )
    pick = jnp.where(pick, 1.0, 0.0).astype(HALF)
    inner = nt(pick, top) + nt(pick, rest)
    low = lax.broadcasted_iota(jnp.int32, (block, LANES), 1) < HD
    dq_t = [jnp.zeros((LANES, rows), F32) for _ in range(2)]
    for k_ref, v_ref, dk_ref, dv_ref in zip(k_refs, v_refs, dk_refs, dv_refs):
        for start in range(0, rows, block):
            here = pl.ds(start, block)
            k = k_ref[here, :]
            v = v_ref[here, :]
            k_t = k.T
            dks, dvs = [], []
            for head in range(2):
                own = low if head == 0 else jnp.logical_not(low)
                lse = lse_ref[pl.ds(2 * step + head, 1), :]
                scores = nt(jnp.where(own, k, jnp.zeros_like(k)), q)
                probs = jnp.exp(scores - lse)
                dvs.append(nn(probs.astype(HALF), grad))
                gp = nt(jnp.where(own, v, jnp.zeros_like(v)), grad)
                gs = (probs * (gp - inner[head : head + 1, :])).astype(HALF)
                dks.append(nn(gs, q))
                dq_t[head] = dq_t[head] + nn(k_t, gs)
            dk_ref[here, :] = jnp.where(low, dks[0], dks[1]).astype(HALF)
            dv_ref[here, :] = jnp.where(low, dvs[0], dvs[1]).astype(HALF)
    upper = lax.broadcasted_iota(jnp.int32, (LANES, rows), 0) < HD
    dq = jnp.where(upper, dq_t[0], dq_t[1]).T * HD**-0.5
    dq_ref[...] = dq.astype(HALF)


def attend_grad(projected, others, grad, attended, logsum, width):
    rows = projected.shape[0]
    groups = 1 + len(others)
    tiles = width // LANES
    col = lambda base: pl.BlockSpec((rows, LANES), lambda i, base=base: (0, base + i))
    out = jax.ShapeDtypeStruct((rows, width), HALF)
    return pl.pallas_call(
        functools.partial(attend_grad_kernel, groups),
        grid=(tiles,),
        out_shape=(out,) * (1 + 2 * groups),
        in_specs=[col(0), col(tiles)]
        + [col(0)] * len(others)
        + [col(2 * tiles)]
        + [col(tiles)] * len(others)
        + [col(0), col(0), pl.BlockSpec((LANES, rows), lambda i: (0, 0))],
        out_specs=(col(0),) * (1 + 2 * groups),
        compiler_params=pltpu.CompilerParams(vmem_limit_bytes=48 << 20),
        name="attend_grad",
    )(projected, projected, *others, projected, *others, grad, attended, logsum)


def norm_parts(rows):
    centred = rows - jnp.mean(rows, axis=-1, keepdims=True)
    variance = jnp.mean(centred * centred, axis=-1, keepdims=True)
    inverse = lax.rsqrt(variance + EPSILON)
    return centred * inverse, inverse


def norm_grad(grad, hat, inverse, scale):
    g = grad * (1.0 + scale)
    return (
        g
        - jnp.mean(g, axis=-1, keepdims=True)
        - hat * jnp.mean(g * hat, axis=-1, keepdims=True)
    ) * inverse


def gelu_tanh(inputs):
    return jax.nn.gelu(inputs, approximate=True)


MESH_ID = pl.DeviceIdType.MESH
CHUNKS = 12
KEYS, VALUES, QUERIES, OUT, FEED = 0, 1, 2, 3, 4


def guarded(low, value, high, run):
    if isinstance(value, int):
        if low <= value < high:
            run(value)
        return

    @pl.when(jnp.logical_and(value >= low, value < high))
    def _():
        run(value)


class Place:
    def __init__(self):
        self.d = lax.axis_index("dp")
        self.z = lax.axis_index("seq")
        self.c = self.d % 2
        self.x = self.d // 2 % 2
        self.y = self.d // 4
        self.p = self.d // 2

    def plane(self, flip):
        return (jnp.bitwise_xor(self.d, flip), self.z)

    def line(self, flip):
        return (self.d, jnp.bitwise_xor(self.z, flip))


def remote(src, dst, send, recv, peer):
    return pltpu.make_async_remote_copy(
        src_ref=src,
        dst_ref=dst,
        send_sem=send,
        recv_sem=recv,
        device_id=peer,
        device_id_type=MESH_ID,
    )


def greet(peers):
    barrier = pltpu.get_barrier_semaphore()
    for peer in peers:
        pl.semaphore_signal(barrier, inc=1, device_id=peer, device_id_type=MESH_ID)
    pl.semaphore_wait(barrier, len(peers))


class Gather:
    SENDS = (
        (2, 0, "all"),
        (4, 0, "all"),
        (1, 0, "all"),
        (1, 2, "all"),
        (1, 4, "all"),
        (4, 2, "first"),
        (2, 4, "second"),
        (1, 6, "near"),
        (1, 6, "far"),
        (None, 6, "near"),
    )

    def __init__(self, here, whole, send, recv):
        self.here, self.whole, self.send, self.recv = here, whole, send, recv
        self.depth = whole.shape[1] // 8

    def _block(self, chunk, flip, part):
        n, side = self.depth, self.here.z % 2
        size, lo = {
            "all": (n, 0),
            "first": (n // 4, side * (n // 2)),
            "second": (n // 4, side * (n // 2) + n // 4),
            "near": (n // 2, side * (n // 2)),
            "far": (n // 2, (1 - side) * (n // 2)),
        }[part]
        row = pl.multiple_of(jnp.bitwise_xor(self.here.d, flip) * n + lo, 32)
        return self.whole.at[chunk, pl.ds(row, size), :]

    def _copy(self, chunk, slot, arriving=False):
        flip, block, part = self.SENDS[slot]
        if flip is None:
            peer = self.here.line(1)
            part = "far" if arriving else part
        else:
            peer = self.here.plane(flip)
            block = flip ^ block if arriving else block
        ref = self._block(chunk, block, part)
        return remote(ref, ref, self.send.at[chunk, slot], self.recv.at[chunk, slot], peer)

    def begin(self, i):
        for slot in (0, 1, 2):
            self._copy(i, slot).start()

    def relay(self, i):
        self._copy(i, 0, True).wait_recv()
        self._copy(i, 5).start()
        self._copy(i, 1, True).wait_recv()
        self._copy(i, 6).start()
        self._copy(i, 3).start()
        self._copy(i, 4).start()

    def share(self, i):
        self._copy(i, 5, True).wait_recv()
        self._copy(i, 6, True).wait_recv()
        self._copy(i, 9).start()
        self._copy(i, 7).start()

    def hand(self, i):
        self._copy(i, 9, True).wait_recv()
        self._copy(i, 8).start()

    def finish(self, i):
        for slot in (2, 3, 4, 7, 8):
            self._copy(i, slot, True).wait_recv()

    def tick(self, t, prepare):
        def begin(i):
            prepare(i)
            self.begin(i)

        guarded(0, t - 5, CHUNKS, self.finish)
        guarded(0, t - 4, CHUNKS, self.hand)
        guarded(0, t - 3, CHUNKS, self.share)
        guarded(0, t - 2, CHUNKS, self.relay)
        lead = 5
        if isinstance(t, int):
            for i in (t,) if t < lead else (t, t + 1) if t == lead else (t + 1,):
                guarded(0, i, CHUNKS, begin)
        else:
            guarded(lead, t + 1, CHUNKS, begin)

    def drain(self):
        @pl.loop(0, CHUNKS)
        def _(i):
            for slot in range(len(self.SENDS)):
                self._copy(i, slot).wait_send()


class Spread:
    def __init__(self, here, source, landing, send, recv):
        self.here, self.source, self.landing = here, source, landing
        self.send, self.recv = send, recv
        self.size = source.shape[1] // 2

    def _each(self):
        here = self.here
        lats = self.source.shape[0]
        for j in range(lats):
            for core in range(2):
                z = lats * here.c + j
                own = jnp.logical_and(z == here.z, core == here.c)
                src = self.source.at[j, pl.ds(core * self.size, self.size), :]
                peer = (here.d - here.c + core, z)
                yield own, j * 2 + core, src, peer

    def _land(self, z):
        return self.landing.at[pl.ds(pl.multiple_of(z * self.size, self.size), self.size), :]

    def start(self, pieces=range(4)):
        z = self.here.z
        for own, index, src, peer in self._each():
            if index not in pieces:
                continue

            @pl.when(own)
            def _():
                pltpu.make_async_copy(src, self._land(z), self.recv.at[z]).start()

            @pl.when(jnp.logical_not(own))
            def _():
                remote(src, self._land(z), self.send.at[index], self.recv.at[z], peer).start()

    def wait(self):
        src = self.source.at[0, pl.ds(0, self.size), :]
        for z in range(4):
            pltpu.make_async_copy(src, self._land(z), self.recv.at[z]).wait()

    def drain(self):
        z = self.here.z
        for own, index, src, peer in self._each():

            @pl.when(jnp.logical_not(own))
            def _():
                remote(src, self._land(z), self.send.at[index], self.recv.at[z], peer).wait_send()


def gelu_both(v):
    root = 0.7978845608028654
    square = v * v
    t = jnp.tanh(root * (v + 0.044715 * (v * square)))
    half = 0.5 * (1.0 + t)
    slope = half + (0.5 * root) * v * (1.0 - t * t) * (1.0 + (3 * 0.044715) * square)
    return half * v, slope


def column_sum(x):
    return jnp.sum(x, axis=0, keepdims=True)


FORWARD_OUTS = (
    "whole",
    "xs",
    "cots",
    "qkv",
    "kvo",
    "att",
    "lse",
    "mid",
    "bra",
    "nb",
    "hid",
    "gph",
    "gbh",
    "outb",
    "gnb",
    "vec",
    "silu",
    "ups",
)


def forward_kernel(tokens, cot, qkv_w, out_w, up_w, down_w, small, ada, *refs):
    outs = dict(zip(FORWARD_OUTS, refs))
    (
        w,
        small_all,
        part,
        mod_in,
        mod,
        vec,
        silu,
        xs,
        ct,
        na,
        qkv,
        kvo,
        att,
        lse_acc,
        lse,
        mid,
        bra,
        nb,
        gbh,
        bb,
        gnb,
        hid,
        gph,
        ups,
        g_send,
        g_recv,
        own_sem,
        sp_send,
        sp_recv,
        sm_send,
        sm_recv,
        md_send,
        md_recv,
        kv_send,
        kv_recv,
        out_sem,
        ff_sem,
    ) = refs[len(FORWARD_OUTS) :]
    here = Place()
    d, z, c = here.d, here.z, here.c
    depth, width = qkv_w.shape[0], out_w.shape[1]
    rows = xs.shape[0]
    wide = up_w.shape[1]
    cut = wide // 32
    tile = 256

    mine = pl.ds(pl.multiple_of(d * depth, depth), depth)
    for i, k in ((KEYS, 1), (VALUES, 2), (QUERIES, 0)):
        pltpu.make_async_copy(
            qkv_w.at[:, pl.ds(k * width, width)], w.at[i, mine, :], own_sem.at[i]
        ).start()
    pltpu.make_async_copy(out_w, w.at[OUT, mine, :], own_sem.at[OUT]).start()
    for j in range(4):
        for k in range(8):
            pltpu.make_async_copy(
                up_w.at[:, pl.ds((4 * k + j) * cut, cut)],
                w.at[FEED + 2 * j, mine, pl.ds(k * cut, cut)],
                own_sem.at[FEED + 2 * j],
            ).start()
        pltpu.make_async_copy(
            down_w.at[pl.ds(j * depth, depth), :], w.at[FEED + 2 * j + 1, mine, :], own_sem.at[FEED + 2 * j + 1]
        ).start()

    def prepare(i):
        pltpu.make_async_copy(out_w, w.at[i, mine, :], own_sem.at[i]).wait()

    peers = [here.plane(f) for f in range(1, 8)]
    for core in range(2):
        for f in range(1, 4):
            peers.append((d - c + core, jnp.bitwise_xor(z, f)))
    greet(peers)

    gather = Gather(here, w, g_send, g_recv)
    tick = functools.partial(gather.tick, prepare=prepare)
    first = Spread(here, tokens, xs, sp_send.at[0], sp_recv.at[0])
    second = Spread(here, cot, ct, sp_send.at[1], sp_recv.at[1])

    def small_copy(f):
        dst = small_all.at[d]
        return remote(small, dst, sm_send.at[f - 1], sm_recv.at[f - 1], here.plane(f))

    for f in range(1, 8):
        small_copy(f).start()
    first.start()
    tick(0)
    tick(1)
    small_all[d] = small[...]
    for f in range(1, 8):
        small_copy(f).wait_recv()

    picked = [
        small_all[i // 2, pl.ds(16 + 8 * (i % 2) + d, 1), :] for i in range(16)
    ]
    cond = jnp.concatenate(picked, axis=0)
    silu[...] = (cond * jax.nn.sigmoid(cond)).astype(HALF)
    for i in range(6):
        product = nn(silu[...], ada[:, pl.ds(i * width, width)])
        for k in range(8):
            part[:, 8 * i + k, :] = product[:, k * LANES : (k + 1) * LANES]

    def mod_copy(f):
        flip = jnp.bitwise_xor(d, f)
        src = part.at[4 * (flip // 2) + z]
        return remote(src, mod_in.at[d], md_send.at[f - 1], md_recv.at[f - 1], here.plane(f))

    for f in range(1, 8):
        mod_copy(f).start()
    mod_in[d] = part[4 * here.p + z]
    tick(2)
    for f in range(1, 8):
        mod_copy(f).wait_recv()
    mod[...] = sum(mod_in[k] for k in range(1, 8)) + mod_in[0]
    for k in range(8):
        mod[pl.ds(6 * k, 6), :] = mod[pl.ds(6 * k, 6), :] + small_all[k, pl.ds(0, 6), :]
    for i in range(6):
        for k in range(8):
            vec[pl.ds(i, 1), pl.ds(k * LANES, LANES)] = mod[pl.ds(8 * i + k, 1), :]
    for k in range(8):
        lanes = pl.ds(k * LANES, LANES)
        vec[pl.ds(8, 1), lanes] = small_all[k // 2, pl.ds(6 + k % 2, 1), :]
        vec[pl.ds(9, 1), lanes] = small_all[4 + k // 2, pl.ds(6 + k % 2, 1), :]
        vec[pl.ds(10, 1), lanes] = small_all[k, pl.ds(8, 1), :]
        vec[pl.ds(11, 1), lanes] = small_all[k, pl.ds(13, 1), :]
        for j in range(4):
            vec[pl.ds(12 + j, 1), lanes] = small_all[k, pl.ds(9 + j, 1), :]

    def row(i):
        return vec[pl.ds(i, 1), :]

    exits = []

    def leave(src, name, index=None):
        dst = outs[name] if index is None else outs[name].at[index]
        copy = pltpu.make_async_copy(src, dst, out_sem.at[len(exits)])
        copy.start()
        exits.append(copy)

    leave(vec, "vec")
    leave(silu, "silu")
    tick(3)
    tick(4)
    first.wait()
    leave(xs, "xs")

    block = 128

    @pl.loop(0, rows // block)
    def _(i):
        part_rows = pl.ds(pl.multiple_of(i * block, block), block)
        hat, _ = norm_parts(xs[part_rows, :].astype(F32))
        na[part_rows, :] = (hat * (1.0 + row(1)) + row(0)).astype(HALF)

    def project(chunk, index, bias):
        for n in range(width // tile):
            cols = pl.ds(n * tile, tile)
            value = nn(na[...], w[chunk, :, cols])
            if bias is not None:
                value = value + vec[pl.ds(bias, 1), cols]
            qkv[index, :, cols] = value.astype(HALF)

    def kv_copy(k):
        return remote(qkv.at[1 + k], kvo.at[k], kv_send.at[k], kv_recv.at[k], here.plane(1))

    tick(5)
    second.start((0,))
    leave(w.at[KEYS], "whole", KEYS)
    project(KEYS, 1, None)
    kv_copy(0).start()
    tick(6)
    second.start((1,))
    leave(w.at[VALUES], "whole", VALUES)
    project(VALUES, 2, 9)
    kv_copy(1).start()
    tick(7)
    second.start((2, 3))
    leave(w.at[QUERIES], "whole", QUERIES)
    project(QUERIES, 0, 8)
    leave(qkv, "qkv")
    for k in range(2):
        kv_copy(k).wait_recv()
    leave(kvo, "kvo")

    span = 256
    low = lax.broadcasted_iota(jnp.int32, (span, LANES), 1) < HD
    lane = lax.broadcasted_iota(jnp.int32, (span, LANES), 1)

    @pl.loop(0, width // LANES)
    def _(step):
        cols = pl.ds(pl.multiple_of(step * LANES, LANES), LANES)
        keys = [qkv[1, :, cols], kvo[0, :, cols]]
        values = [qkv[2, :, cols], kvo[1, :, cols]]
        for start in range(0, rows, span):
            part_rows = pl.ds(start, span)
            q = qkv[0, part_rows, cols] * HALF(HD**-0.5)
            pieces = []
            for head in range(2):
                own = low if head == 0 else jnp.logical_not(low)
                qm = jnp.where(own, q, jnp.zeros_like(q))
                scores = [nt(qm, k) for k in keys]
                peak = functools.reduce(
                    jnp.maximum, [jnp.max(s, axis=-1, keepdims=True) for s in scores]
                )
                raised = [jnp.exp(s - peak) for s in scores]
                total = sum(jnp.sum(e, axis=-1, keepdims=True) for e in raised)
                mixed = sum(nn(e.astype(HALF), v) for e, v in zip(raised, values))
                pieces.append(mixed / total)
                logsum = jnp.broadcast_to(peak + jnp.log(total), (span, LANES))
                lse_acc[part_rows, :] = jnp.where(
                    lane == 2 * step + head, logsum, lse_acc[part_rows, :]
                )
            att[part_rows, cols] = jnp.where(low, pieces[0], pieces[1]).astype(HALF)

        @pl.when(step % 3 == 2)
        def _():
            gather.tick(8 + step // 3, prepare)

    lse[...] = lse_acc[...].T
    leave(lse, "lse")
    leave(att, "att")
    leave(w.at[OUT], "whole", OUT)
    second.wait()
    leave(ct, "cots")

    for n in range(width // tile):
        cols = pl.ds(n * tile, tile)
        branch = nn(att[...], w[OUT, :, cols]) + vec[pl.ds(10, 1), cols]
        bra[:, cols] = branch.astype(HALF)
        mid[:, cols] = xs[:, cols].astype(F32) + vec[pl.ds(2, 1), cols] * branch
    leave(mid, "mid")
    leave(bra, "bra")
    tick(10)

    @pl.loop(0, rows // block)
    def _(i):
        part_rows = pl.ds(pl.multiple_of(i * block, block), block)
        hat, _ = norm_parts(mid[part_rows, :])
        nb[part_rows, :] = (hat * (1.0 + row(4)) + row(3)).astype(HALF)
        gbh[part_rows, :] = (ct[part_rows, :].astype(F32) * row(5)).astype(HALF)
        bb[part_rows, :] = jnp.broadcast_to(row(11), (block, width))
        gnb[part_rows, :] = jnp.zeros((block, width), F32)

    leave(nb, "nb")
    leave(gbh, "gbh")

    def ff_copies(j, slot):
        return (
            pltpu.make_async_copy(hid.at[slot], outs["hid"].at[j], ff_sem.at[0, slot]),
            pltpu.make_async_copy(gph.at[slot], outs["gph"].at[j], ff_sem.at[1, slot]),
        )

    @pl.loop(0, 4)
    def _(j):
        slot = j % 2
        up, down = FEED + 2 * j, FEED + 2 * j + 1

        @pl.when(j >= 2)
        def _():
            for copy in ff_copies(j, slot):
                copy.wait()

        for n in range(width // tile):
            cols = pl.ds(n * tile, tile)
            pre = nn(nb[...], w[up, :, cols]) + vec[pl.ds(12 + j, 1), cols]
            grad = nt(gbh[...], w[down, cols, :])
            value, slope = gelu_both(pre)
            grad = grad * slope
            ups[pl.ds(j, 1), cols] = column_sum(grad)
            hid[slot, :, cols] = value.astype(HALF)
            gph[slot, :, cols] = grad.astype(HALF)
        for copy in ff_copies(j, slot):
            copy.start()
        gather.tick(11 + 2 * j, prepare)
        for n in range(width // tile):
            cols = pl.ds(n * tile, tile)
            bb[:, cols] = bb[:, cols] + nn(hid[slot], w[down, :, cols])
            gnb[:, cols] = gnb[:, cols] + nt(gph[slot], w[up, cols, :])
        gather.tick(12 + 2 * j, prepare)

    leave(gnb, "gnb")
    ups[pl.ds(4, 4), :] = jnp.zeros((4, width), F32)

    @pl.loop(0, rows // block)
    def _(i):
        part_rows = pl.ds(pl.multiple_of(i * block, block), block)
        branch = bb[part_rows, :]
        grad = ct[part_rows, :].astype(F32)
        na[part_rows, :] = (mid[part_rows, :] + row(5) * branch).astype(HALF)
        ups[pl.ds(4, 1), :] = ups[pl.ds(4, 1), :] + column_sum(grad * branch)
        ups[pl.ds(5, 1), :] = ups[pl.ds(5, 1), :] + column_sum(grad)

    leave(na, "outb")
    leave(ups, "ups")
    for slot in range(2):
        for copy in ff_copies(slot, slot):
            copy.wait()
    for copy in exits:
        copy.wait()
    gather.drain()
    first.drain()
    second.drain()
    for f in range(1, 8):
        small_copy(f).wait_send()
        mod_copy(f).wait_send()
    for k in range(2):
        kv_copy(k).wait_send()


def forward(tokens, cot, qkv_w, out_w, up_w, down_w, small, ada):
    depth, width = qkv_w.shape[0], out_w.shape[1]
    rows = tokens.shape[0] * tokens.shape[1]
    sds = jax.ShapeDtypeStruct
    flat, real = sds((rows, width), HALF), sds((rows, width), F32)
    shapes = dict(
        whole=sds((4, width, width), HALF),
        xs=flat,
        cots=flat,
        qkv=sds((3, rows, width), HALF),
        kvo=sds((2, rows, width), HALF),
        att=flat,
        lse=sds((LANES, rows), F32),
        mid=real,
        bra=flat,
        nb=flat,
        hid=sds((4, rows, width), HALF),
        gph=sds((4, rows, width), HALF),
        gbh=flat,
        outb=flat,
        gnb=real,
        vec=sds((16, width), F32),
        silu=sds((16, LANES), HALF),
        ups=sds((8, width), F32),
    )
    hbm = pl.BlockSpec(memory_space=pl.ANY)
    vmem = pl.BlockSpec(memory_space=pltpu.VMEM)
    dma = pltpu.SemaphoreType.DMA
    half = lambda *s: pltpu.VMEM(s, HALF)
    full = lambda *s: pltpu.VMEM(s, F32)
    scratch = [
        half(CHUNKS, width, width),
        full(8, 32, LANES),
        full(16, 48, LANES),
        full(8, 48, LANES),
        full(48, LANES),
        full(16, width),
        half(16, LANES),
        half(rows, width),
        half(rows, width),
        half(rows, width),
        half(3, rows, width),
        half(2, rows, width),
        half(rows, width),
        full(rows, LANES),
        full(LANES, rows),
        full(rows, width),
        half(rows, width),
        half(rows, width),
        half(rows, width),
        full(rows, width),
        full(rows, width),
        half(2, rows, width),
        half(2, rows, width),
        full(8, width),
        dma((CHUNKS, 10)),
        dma((CHUNKS, 10)),
        dma((CHUNKS,)),
        dma((2, 4)),
        dma((2, 4)),
        dma((7,)),
        dma((7,)),
        dma((7,)),
        dma((7,)),
        dma((2,)),
        dma((2,)),
        dma((24,)),
        dma((2, 2)),
    ]
    got = pl.pallas_call(
        forward_kernel,
        out_shape=tuple(shapes[name] for name in FORWARD_OUTS),
        in_specs=[hbm] * 6 + [vmem] * 2,
        out_specs=(hbm,) * len(FORWARD_OUTS),
        scratch_shapes=scratch,
        compiler_params=pltpu.CompilerParams(
            collective_id=1, has_side_effects=True, vmem_limit_bytes=67043328
        ),
        name="forward",
    )(tokens, cot, qkv_w, out_w, up_w, down_w, small, ada)
    return dict(zip(FORWARD_OUTS, got))


class Reduce:
    COUNT = 2 * CHUNKS
    RING = 6
    DEEP = 8

    def __init__(self, here, bufs, send, recv, credit):
        self.here = here
        (self.dw, self.rc, self.rx, self.ry, self.t, self.ry2, self.rx2, self.r, self.rz1, self.q, self.rz2, self.out) = bufs
        self.send, self.recv, self.credit = send, recv, credit
        self.depth, self.cols = self.out.shape[1], self.out.shape[2] // 2
        self.half = self.cols // 2
        self.inner = jnp.logical_or(here.z == 1, here.z == 2)
        self.outer = jnp.logical_not(self.inner)

    def _copy(self, i, slot, arriving=False):
        here = self.here
        s, deep = lax.rem(i, self.RING), lax.rem(i, self.DEEP)
        low, high = pl.ds(0, self.half), pl.ds(self.half, self.half)
        if slot == 0:
            src, dst, peer = self.dw.at[s, :, :, 1 - here.c], self.rc.at[deep], here.plane(1)
        elif slot == 1:
            src, dst, peer = self.dw.at[s, :, 1 - here.x, here.c, :, low], self.rx.at[deep], here.plane(2)
        elif slot == 2:
            src, dst, peer = self.dw.at[s, 1 - here.y, :, here.c, :, high], self.ry.at[deep], here.plane(4)
        elif slot == 3:
            src, dst, peer = self.t.at[s, 0, 1 - here.y], self.ry2.at[i], here.plane(4)
        elif slot == 4:
            src, dst, peer = self.t.at[s, 1, 1 - here.x], self.rx2.at[i], here.plane(2)
        elif slot == 5:
            src, dst, peer = self.r.at[s], self.rz1.at[i], here.line(1)
        elif slot == 6:
            src, dst, peer = self.q.at[s], self.rz2.at[i], here.line(3)
        else:
            src = dst = self._share(i)
            peer = here.line(1)
        return remote(src, dst, self.send.at[i, slot], self.recv.at[i, slot], peer)

    def _share(self, i):
        cols = pl.ds(pl.multiple_of(lax.rem(i, 2) * self.cols, self.cols), self.cols)
        return self.out.at[lax.div(i, 2), :, cols]

    def _sent(self, i, *slots):
        def wait(k):
            for slot in slots:
                self._copy(k, slot).wait_send()

        guarded(0, i - self.RING, self.COUNT, wait)

    def _spend(self, i, *kinds):
        def wait(k):
            for kind in kinds:
                pl.semaphore_wait(self.credit.at[kind], 1)

        guarded(self.DEEP, i, self.COUNT, wait)

    def _grant(self, i, kind, flip):
        def signal(k):
            pl.semaphore_signal(
                self.credit.at[kind], inc=1, device_id=self.here.plane(flip), device_id_type=MESH_ID
            )

        guarded(0, i, self.COUNT - self.DEEP, signal)

    def produce(self, i, side, left_t, right):
        s = lax.rem(i, self.RING)
        self._sent(i, 0, 1, 2)
        tile = 256
        for n in range(self.cols // tile):
            value = nn(left_t[...], right[:, pl.ds(side * self.cols + n * tile, tile)]).astype(HALF)
            for k in range(8):
                self.dw[s, k // 4, k // 2 % 2, k % 2, :, pl.ds(n * tile, tile)] = value[
                    k * self.depth : (k + 1) * self.depth
                ]
        self._spend(i, 0)
        self._copy(i, 0).start()

    def plane(self, i):
        s, deep = lax.rem(i, self.RING), lax.rem(i, self.DEEP)
        c = self.here.c
        self._copy(i, 0, True).wait_recv()
        for y in range(2):
            for x in range(2):
                self.dw[s, y, x, c] = (
                    self.dw[s, y, x, c].astype(F32) + self.rc[deep, y, x].astype(F32)
                ).astype(HALF)
        self._grant(i, 0, 1)
        self._spend(i, 1, 2)
        self._copy(i, 1).start()
        self._copy(i, 2).start()

    def cross(self, i):
        s, deep = lax.rem(i, self.RING), lax.rem(i, self.DEEP)
        here = self.here
        low, high = pl.ds(0, self.half), pl.ds(self.half, self.half)
        self._copy(i, 1, True).wait_recv()
        self._copy(i, 2, True).wait_recv()
        self._sent(i, 3, 4)
        for k in range(2):
            self.t[s, 0, k] = (
                self.dw[s, k, here.x, here.c, :, low].astype(F32) + self.rx[deep, k].astype(F32)
            ).astype(HALF)
            self.t[s, 1, k] = (
                self.dw[s, here.y, k, here.c, :, high].astype(F32) + self.ry[deep, k].astype(F32)
            ).astype(HALF)
        self._grant(i, 1, 2)
        self._grant(i, 2, 4)
        self._copy(i, 3).start()
        self._copy(i, 4).start()

    def line(self, i):
        s = lax.rem(i, self.RING)
        here = self.here
        self._copy(i, 3, True).wait_recv()
        self._copy(i, 4, True).wait_recv()

        @pl.when(self.outer)
        def _():
            self._sent(i, 5)

        self.r[s, :, pl.ds(0, self.half)] = (
            self.t[s, 0, here.y].astype(F32) + self.ry2[i].astype(F32)
        ).astype(HALF)
        self.r[s, :, pl.ds(self.half, self.half)] = (
            self.t[s, 1, here.x].astype(F32) + self.rx2[i].astype(F32)
        ).astype(HALF)

        @pl.when(self.outer)
        def _():
            self._copy(i, 5).start()

    def far(self, i):
        s = lax.rem(i, self.RING)

        @pl.when(self.inner)
        def _():
            self._copy(i, 5, True).wait_recv()
            self._sent(i, 6)
            self.q[s] = (self.r[s].astype(F32) + self.rz1[i].astype(F32)).astype(HALF)
            self._copy(i, 6).start()

    def close(self, i):
        s = lax.rem(i, self.RING)

        @pl.when(self.inner)
        def _():
            self._copy(i, 6, True).wait_recv()
            self._share(i)[...] = (self.q[s].astype(F32) + self.rz2[i].astype(F32)).astype(HALF)
            self._copy(i, 7).start()

    def finish(self, i):
        @pl.when(self.outer)
        def _():
            self._copy(i, 7, True).wait_recv()

    LAGS = (11, 9, 7, 5, 3, 0)

    def tick(self, t):
        steps = (self.finish, self.close, self.far, self.line, self.cross, self.plane)
        for lag, step in zip(self.LAGS, steps):
            guarded(0, t - lag, self.COUNT, step)

    def drain(self):
        for k in range(self.COUNT - self.RING, self.COUNT):
            for slot in range(5):
                self._copy(k, slot).wait_send()

        @pl.when(self.outer)
        def _():
            for k in range(self.COUNT - self.RING, self.COUNT):
                self._copy(k, 5).wait_send()

        @pl.when(self.inner)
        def _():
            for k in range(self.COUNT - self.RING, self.COUNT):
                self._copy(k, 6).wait_send()

            @pl.loop(0, self.COUNT)
            def _(i):
                self._copy(i, 7).wait_send()


class Collect:
    def __init__(self, here, source, target, send, recv):
        self.here, self.source, self.target = here, source, target
        self.send, self.recv = send, recv
        self.size = target.shape[1] // 2

    def _copy(self, z):
        here = self.here
        owner, j = here.z // 2, here.z % 2
        dst = self.target.at[j, pl.ds(pl.multiple_of(here.c * self.size, self.size), self.size), :]
        arrive = self.recv.at[2 * j + here.c]
        own = jnp.logical_and(here.z == z, here.c == owner)
        src = self.source.at[pl.ds(pl.multiple_of(z * self.size, self.size), self.size), :]
        return own, src, dst, self.send.at[z], arrive, (here.d - here.c + owner, z)

    def piece(self, z):
        own, src, dst, send, recv, peer = self._copy(z)

        @pl.when(own)
        def _():
            pltpu.make_async_copy(src, dst, recv).start()

        @pl.when(jnp.logical_not(own))
        def _():
            remote(src, dst, send, recv, peer).start()

    def start(self):
        for z in range(4):
            self.piece(z)

    def finish(self):
        for j in range(2):
            for c in range(2):
                dst = self.target.at[j, pl.ds(c * self.size, self.size), :]
                src = self.source.at[pl.ds(0, self.size), :]
                pltpu.make_async_copy(src, dst, self.recv.at[2 * j + c]).wait()
        for z in range(4):
            own, src, dst, send, recv, peer = self._copy(z)

            @pl.when(jnp.logical_not(own))
            def _():
                remote(src, dst, send, recv, peer).wait_send()


BACKWARD_INS = (
    "whole",
    "xs",
    "cots",
    "gbh",
    "qkv",
    "kvo",
    "att",
    "lse",
    "mid",
    "bra",
    "nb",
    "hid",
    "gph",
    "outb",
    "gnb",
    "vec",
    "ups",
    "ada",
)
BACKWARD_OUTS = ("output", "tokens", "shares", "gmod", "condp", "biases")


def backward_kernel(*refs):
    ins = dict(zip(BACKWARD_INS, refs))
    refs = refs[len(BACKWARD_INS) :]
    outs = dict(zip(BACKWARD_OUTS, refs))
    (
        w,
        xs,
        ct,
        gbh,
        qkv,
        kvo,
        kvr,
        att,
        lse,
        mid,
        bra,
        nb_t,
        tmp_t,
        hid,
        gph,
        gnb,
        ga,
        sums,
        dw,
        rc,
        rx,
        ry,
        t,
        ry2,
        rx2,
        r,
        rz1,
        q_,
        rz2,
        shares,
        gs,
        gs_in,
        gmod,
        cpart,
        condp,
        bpart,
        bin_,
        bz,
        biases,
        ld_sem,
        ff_sem,
        r_send,
        r_recv,
        credit,
        o_send,
        o_recv,
        kv_send,
        kv_recv,
        b_send,
        b_recv,
        bz_send,
        bz_recv,
        g_send,
        g_recv,
        m_send,
        m_recv,
        c_send,
        c_recv,
        out_sem,
    ) = refs[len(BACKWARD_OUTS) :]
    here = Place()
    d, z, c, p = here.d, here.z, here.c, here.p
    vec, ups, ada = ins["vec"], ins["ups"], ins["ada"]
    rows, width = xs.shape
    tile, block = 256, 128
    depth = shares.shape[1]

    loads = {}

    def load(name, src, dst):
        loads[name] = pltpu.make_async_copy(src, dst, ld_sem.at[len(loads)])
        loads[name].start()

    def need(*names):
        for name in names:
            loads[name].wait()

    def feed(which, j):
        k = 0 if which is hid else 1
        name = "hid" if which is hid else "gph"
        return pltpu.make_async_copy(ins[name].at[j], which.at[lax.rem(j, 2)], ff_sem.at[k, lax.rem(j, 2)])

    order = (
        ("nb", ins["nb"], ga),
        ("mid", ins["mid"], mid),
        ("gnb", ins["gnb"], gnb),
        ("cots", ins["cots"], ct),
        ("bra", ins["bra"], bra),
        ("att", ins["att"], att),
        ("out_w", ins["whole"].at[OUT], w.at[0]),
        ("gbh", ins["gbh"], gbh),
        ("qkv", ins["qkv"], qkv),
        ("kvo", ins["kvo"], kvo),
        ("lse", ins["lse"], lse),
        ("k_w", ins["whole"].at[KEYS], w.at[1]),
        ("v_w", ins["whole"].at[VALUES], w.at[2]),
        ("xs", ins["xs"], xs),
    )
    load(*order[0])
    feed(gph, 0).start()
    for item in order[1:8]:
        load(*item)
    feed(hid, 0).start()
    for item in order[8:]:
        load(*item)
    feed(gph, 1).start()
    feed(hid, 1).start()

    line_peers = [
        (2 * jnp.bitwise_xor(p, fp) + c, jnp.bitwise_xor(z, fz))
        for fp in range(4)
        for fz in range(4)
        if fp or fz
    ]
    greet(
        line_peers
        + [here.plane(f) for f in (1, 3, 5, 7)]
        + [(jnp.bitwise_xor(d, 1), jnp.bitwise_xor(z, f)) for f in range(1, 4)]
    )

    red = Reduce(
        here, (dw, rc, rx, ry, t, ry2, rx2, r, rz1, q_, rz2, shares), r_send, r_recv, credit
    )
    output = Collect(here, ins["outb"], outs["output"], o_send.at[0], o_recv.at[0])
    output.start()

    def row(i):
        return vec[pl.ds(i, 1), :]

    sums[...] = jnp.zeros_like(sums)

    def add(i, value):
        sums[pl.ds(i, 1), :] = sums[pl.ds(i, 1), :] + value

    need("nb")
    nb_t[...] = ga[...].T
    feed(gph, 0).wait()
    red.produce(0, 0, nb_t, gph.at[0])
    red.produce(1, 1, nb_t, gph.at[0])
    need("mid", "gnb", "cots", "bra")

    @pl.loop(0, rows // block)
    def _(i):
        part_rows = pl.ds(pl.multiple_of(i * block, block), block)
        hat, inverse = norm_parts(mid[part_rows, :])
        grad = gnb[part_rows, :]
        add(3, column_sum(grad))
        add(4, column_sum(grad * hat))
        grad_mid = ct[part_rows, :].astype(F32) + norm_grad(grad, hat, inverse, row(4))
        add(2, column_sum(grad_mid * bra[part_rows, :].astype(F32)))
        add(6, column_sum(grad_mid))
        mid[part_rows, :] = grad_mid
        bra[part_rows, :] = (grad_mid * row(2)).astype(HALF)

    red.tick(0)
    red.tick(1)
    need("att")
    tmp_t[...] = att[...].T
    red.produce(2, 0, tmp_t, bra)
    red.produce(3, 1, tmp_t, bra)
    need("out_w")
    for n in range(width // tile):
        cols = pl.ds(n * tile, tile)
        ga[:, cols] = nt(bra[...], w[0, cols, :]).astype(HALF)
    load("q_w", ins["whole"].at[QUERIES], w.at[0])
    red.tick(2)
    red.tick(3)
    need("gbh", "qkv", "kvo", "lse")

    span = 256
    low = lax.broadcasted_iota(jnp.int32, (span, LANES), 1) < HD
    upper = lax.broadcasted_iota(jnp.int32, (LANES, rows), 0) < HD
    pick = lax.broadcasted_iota(jnp.int32, (8, LANES), 0) == (
        lax.broadcasted_iota(jnp.int32, (8, LANES), 1) // HD
    )
    pick = jnp.where(pick, 1.0, 0.0).astype(HALF)

    def attend_back(step, between):
        cols = pl.ds(pl.multiple_of(step * LANES, LANES), LANES)
        q = qkv[0, :, cols] * HALF(HD**-0.5)
        grad = ga[:, cols]
        product = grad.astype(F32) * att[:, cols].astype(F32)
        top = product.astype(HALF)
        rest = (product - top.astype(F32)).astype(HALF)
        inner = nt(pick, top) + nt(pick, rest)
        dq_t = [jnp.zeros((LANES, rows), F32) for _ in range(2)]
        for group, (k_ref, v_ref) in enumerate(((qkv.at[1], qkv.at[2]), (kvo.at[0], kvo.at[1]))):
            if group:
                between()
            for start in range(0, rows, span):
                part_rows = pl.ds(start, span)
                k = k_ref[part_rows, cols]
                v = v_ref[part_rows, cols]
                k_t = k.T
                dks, dvs = [], []
                for head in range(2):
                    own = low if head == 0 else jnp.logical_not(low)
                    logsum = lse[pl.ds(2 * step + head, 1), :]
                    scores = nt(jnp.where(own, k, jnp.zeros_like(k)), q)
                    probs = jnp.exp(scores - logsum)
                    dvs.append(nn(probs.astype(HALF), grad))
                    gp = nt(jnp.where(own, v, jnp.zeros_like(v)), grad)
                    score_grad = (probs * (gp - inner[head : head + 1, :])).astype(HALF)
                    dks.append(nn(score_grad, q))
                    dq_t[head] = dq_t[head] + nn(k_t, score_grad)
                k_ref[part_rows, cols] = jnp.where(low, dks[0], dks[1]).astype(HALF)
                v_ref[part_rows, cols] = jnp.where(low, dvs[0], dvs[1]).astype(HALF)
        dq = jnp.where(upper, dq_t[0], dq_t[1]).T * HD**-0.5
        qkv[0, :, cols] = dq.astype(HALF)

    @pl.loop(0, 4)
    def _(j):
        slot, base = lax.rem(j, 2), 4 + 2 * j
        feed(hid, j).wait()
        tmp_t[...] = hid[slot].T
        red.produce(base, 0, tmp_t, gbh)

        @pl.when(j < 2)
        def _():
            feed(hid, j + 2).start()

        def even():
            red.tick(base)
            red.produce(base + 1, 1, tmp_t, gbh)

        attend_back(2 * j, even)
        attend_back(2 * j + 1, lambda: red.tick(base + 1))

    def kv_copy(k):
        return remote(kvo.at[k], kvr.at[k], kv_send.at[k], kv_recv.at[k], here.plane(1))

    kv_copy(1).start()
    kv_copy(0).start()
    feed(gph, 2).start()
    feed(gph, 1).wait()
    for side in range(2):
        red.produce(12 + side, side, nb_t, gph.at[1])
    feed(gph, 3).start()
    red.tick(12)
    need("xs", "q_w", "k_w", "v_w")
    for k in (1, 0):
        kv_copy(k).wait_recv()

        @pl.loop(0, rows // block)
        def _(i):
            part_rows = pl.ds(pl.multiple_of(i * block, block), block)
            qkv[1 + k, part_rows, :] = (
                qkv[1 + k, part_rows, :].astype(F32) + kvr[k, part_rows, :].astype(F32)
            ).astype(HALF)

    def project_back(lo, hi):
        @pl.loop(lo, hi)
        def _(n):
            cols = pl.ds(pl.multiple_of(n * tile, tile), tile)
            gnb[:, cols] = (
                nt(qkv[0], w[0, cols, :]) + nt(qkv[1], w[1, cols, :]) + nt(qkv[2], w[2, cols, :])
            )

    project_back(0, 2)
    red.tick(13)
    project_back(2, 4)
    feed(gph, 2).wait()
    for side in range(2):
        red.produce(14 + side, side, nb_t, gph.at[0])
    red.tick(14)

    back = Collect(here, att, outs["tokens"], o_send.at[1], o_recv.at[1])

    @pl.loop(0, rows // block)
    def _(i):
        part_rows = pl.ds(pl.multiple_of(i * block, block), block)
        hat, inverse = norm_parts(xs[part_rows, :].astype(F32))
        ga[part_rows, :] = (hat * (1.0 + row(1)) + row(0)).astype(HALF)
        grad = gnb[part_rows, :]
        add(0, column_sum(grad))
        add(1, column_sum(grad * hat))
        att[part_rows, :] = (
            mid[part_rows, :] + norm_grad(grad, hat, inverse, row(1))
        ).astype(HALF)
        back.piece(i)

        @pl.when(i == 1)
        def _():
            red.tick(15)

    sums[pl.ds(5, 1), :] = ups[pl.ds(4, 1), :]
    for i in range(6):
        for k in range(8):
            gs[pl.ds(8 * i + k, 1), :] = sums[pl.ds(i, 1), pl.ds(k * LANES, LANES)]
    pair = remote(gs, gs_in, g_send.at[0], g_recv.at[0], here.plane(1))
    pair.start()
    sums[pl.ds(7, 1), :] = column_sum(qkv[0].astype(F32))
    sums[pl.ds(8, 1), :] = column_sum(qkv[2].astype(F32))
    sums[pl.ds(6, 1), :] = sums[pl.ds(6, 1), :] * row(2)
    sums[pl.ds(9, 1), :] = ups[pl.ds(5, 1), :] * row(5)
    for k in range(8):
        lanes = pl.ds(k * LANES, LANES)
        for s in range(2):
            source = 7 + k // 4
            bpart[k, pl.ds(s, 1), :] = sums[pl.ds(source, 1), pl.ds((2 * (k % 4) + s) * LANES, LANES)]
        bpart[k, pl.ds(2, 1), :] = sums[pl.ds(6, 1), lanes]
        for j in range(4):
            bpart[k, pl.ds(3 + j, 1), :] = ups[pl.ds(j, 1), lanes]
        bpart[k, pl.ds(7, 1), :] = sums[pl.ds(9, 1), lanes]

    def bias_copy(f):
        flip = jnp.bitwise_xor(d, f)
        return remote(bpart.at[flip], bin_.at[d], b_send.at[f - 1], b_recv.at[f - 1], here.plane(f))

    for f in range(1, 8):
        bias_copy(f).start()
    bin_[d] = bpart[d]
    feed(gph, 3).wait()
    for side in range(2):
        red.produce(16 + side, side, nb_t, gph.at[1])
    red.tick(16)
    pair.wait_recv()
    latent = 4 * p + z
    gmod[latent] = gs[...] + gs_in[...]

    def mod_copy(k):
        return remote(
            gmod.at[latent], gmod.at[latent], m_send.at[k], m_recv.at[k], line_peers[k]
        )

    for k in range(15):
        mod_copy(k).start()
    red.tick(17)
    tmp_t[...] = ga[...].T
    for side in range(2):
        red.produce(18 + side, side, tmp_t, qkv.at[0])
    red.tick(18)
    red.tick(19)
    for side in range(2):
        red.produce(20 + side, side, tmp_t, qkv.at[2])
    red.tick(20)
    red.tick(21)
    for side in range(2):
        red.produce(22 + side, side, tmp_t, qkv.at[1])
    red.tick(22)
    red.tick(23)
    for f in range(1, 8):
        bias_copy(f).wait_recv()
    total = bin_[0]
    for k in range(1, 8):
        total = total + bin_[k]
    bz[z] = total

    def line_copy(f):
        dst = bz.at[z]
        return remote(dst, dst, bz_send.at[f - 1], bz_recv.at[f - 1], here.line(f))

    for f in range(1, 4):
        line_copy(f).start()
    for k in range(24, 28):
        red.tick(k)
    for k in range(15):
        mod_copy(k).wait_recv()
    for i in range(6):
        piece = jnp.concatenate([gmod[:, 8 * i + k, :] for k in range(8)], axis=1)
        term = nt(piece.astype(HALF), ada[:, pl.ds(i * width, width)])
        share = term if i == 0 else share + term
    for k in range(8):
        cpart[k, pl.ds(0, 2), :] = share[2 * k : 2 * k + 2]

    def cond_copy(f):
        flip = jnp.bitwise_xor(d, f)
        return remote(cpart.at[flip], condp.at[d], c_send.at[f - 1], c_recv.at[f - 1], here.plane(f))

    for f in range(1, 8):
        cond_copy(f).start()
    condp[d] = cpart[d]
    for f in range(1, 4):
        line_copy(f).wait_recv()
    biases[...] = bz[0] + bz[1] + bz[2] + bz[3]

    @pl.loop(28, Reduce.COUNT + Reduce.LAGS[0])
    def _(k):
        red.tick(k)

    exits = [
        pltpu.make_async_copy(src, outs[name], out_sem.at[k])
        for k, (src, name) in enumerate(
            ((shares, "shares"), (gmod, "gmod"), (biases, "biases"))
        )
    ]
    for copy in exits:
        copy.start()
    for f in range(1, 8):
        cond_copy(f).wait_recv()
    last = pltpu.make_async_copy(condp, outs["condp"], out_sem.at[3])
    last.start()
    red.drain()
    output.finish()
    back.finish()
    pair.wait_send()
    for k in range(2):
        kv_copy(k).wait_send()
    for f in range(1, 8):
        bias_copy(f).wait_send()
        cond_copy(f).wait_send()
    for f in range(1, 4):
        line_copy(f).wait_send()
    for k in range(15):
        mod_copy(k).wait_send()
    for copy in exits:
        copy.wait()
    last.wait()


def backward(f, ada, shape):
    lats, part, width = shape
    rows = lats * part
    depth = ada.shape[0]
    half_cols, part_cols = width // 2, width // 4
    sds = jax.ShapeDtypeStruct
    hbm = pl.BlockSpec(memory_space=pl.ANY)
    vmem = pl.BlockSpec(memory_space=pltpu.VMEM)
    dma = pltpu.SemaphoreType.DMA
    half = lambda *s: pltpu.VMEM(s, HALF)
    full = lambda *s: pltpu.VMEM(s, F32)
    ring, deep, count = Reduce.RING, Reduce.DEEP, Reduce.COUNT
    scratch = [
        half(3, width, width),
        half(rows, width),
        half(rows, width),
        half(rows, width),
        half(3, rows, width),
        half(2, rows, width),
        half(2, rows, width),
        half(rows, width),
        full(LANES, rows),
        full(rows, width),
        half(rows, width),
        half(width, rows),
        half(width, rows),
        half(2, rows, width),
        half(2, rows, width),
        full(rows, width),
        half(rows, width),
        full(16, width),
        half(ring, 2, 2, 2, depth, half_cols),
        half(deep, 2, 2, depth, half_cols),
        half(deep, 2, depth, part_cols),
        half(deep, 2, depth, part_cols),
        half(ring, 2, 2, depth, part_cols),
        half(count, depth, part_cols),
        half(count, depth, part_cols),
        half(ring, depth, half_cols),
        half(count, depth, half_cols),
        half(ring, depth, half_cols),
        half(count, depth, half_cols),
        half(CHUNKS, depth, width),
        full(48, LANES),
        full(48, LANES),
        full(16, 48, LANES),
        full(8, 8, LANES),
        full(8, 8, LANES),
        full(8, 8, LANES),
        full(8, 8, LANES),
        full(4, 8, LANES),
        full(8, LANES),
        dma((20,)),
        dma((2, 2)),
        dma((count, 8)),
        dma((count, 8)),
        pltpu.SemaphoreType.REGULAR((3,)),
        dma((2, 4)),
        dma((2, 4)),
        dma((2,)),
        dma((2,)),
        dma((7,)),
        dma((7,)),
        dma((3,)),
        dma((3,)),
        dma((1,)),
        dma((1,)),
        dma((15,)),
        dma((15,)),
        dma((7,)),
        dma((7,)),
        dma((4,)),
    ]
    operands = [ada if name == "ada" else f[name] for name in BACKWARD_INS]
    near = ("vec", "ups", "ada")
    got = pl.pallas_call(
        backward_kernel,
        out_shape=(
            sds((lats, part, width), HALF),
            sds((lats, part, width), HALF),
            sds((CHUNKS, depth, width), HALF),
            sds((16, 48, LANES), F32),
            sds((8, 8, LANES), F32),
            sds((8, LANES), F32),
        ),
        in_specs=[vmem if name in near else hbm for name in BACKWARD_INS],
        out_specs=(hbm,) * len(BACKWARD_OUTS),
        scratch_shapes=scratch,
        compiler_params=pltpu.CompilerParams(
            collective_id=2, has_side_effects=True, vmem_limit_bytes=67043328
        ),
        name="backward",
    )(*operands)
    return dict(zip(BACKWARD_OUTS, got))


def body_any(
    tokens,
    condition,
    ada_weight,
    ada_bias,
    qkv_weight,
    qv_bias,
    out_weight,
    out_bias,
    up_weight,
    up_bias,
    down_weight,
    down_bias,
    cotangent,
):
    lats, part, width = tokens.shape
    dp = lax.axis_size("dp")
    seq = lax.axis_size("seq")
    me = lax.axis_index("dp")
    z = lax.axis_index("seq")
    core = me % 2
    pair = me // 2
    chip_lats = 2 * lats
    sub = seq // chip_lats
    first = core == 0

    def flip(x):
        return lax.ppermute(x, "dp", [(i, i ^ 1) for i in range(dp)])

    def shift(x, by):
        if by % sub == 0:
            return x
        return lax.ppermute(
            x, "seq", [(i, i // sub * sub + (i - by) % sub) for i in range(seq)]
        )

    def spread(x):
        halves = x.reshape(lats, 2, part // 2, width)
        keep = lax.dynamic_index_in_dim(halves, core, 1, keepdims=False)
        give = lax.dynamic_index_in_dim(halves, 1 - core, 1, keepdims=False)
        got = flip(give)
        both = jnp.concatenate(
            [jnp.where(first, keep, got), jnp.where(first, got, keep)], axis=0
        )
        both = both.reshape(seq, part // (2 * sub), width)
        return lax.all_to_all(both, "seq", 0, 0, tiled=True).reshape(-1, width)

    def collect(x):
        both = x.reshape(seq, part // (2 * sub), width)
        both = lax.all_to_all(both, "seq", 0, 0, tiled=True)
        both = both.reshape(2, lats, part // 2, width)
        mine = lax.dynamic_index_in_dim(both, core, 0, keepdims=False)
        give = lax.dynamic_index_in_dim(both, 1 - core, 0, keepdims=False)
        got = flip(give)
        return jnp.stack(
            [jnp.where(first, mine, got), jnp.where(first, got, mine)], axis=1
        ).reshape(lats, part, width)

    small = jnp.concatenate(
        [ada_bias, qv_bias, out_bias, up_bias, down_bias, condition.reshape(-1)]
    )
    small_all = lax.all_gather(small, "dp", axis=0, tiled=False)
    sizes = [a.shape[0] for a in (ada_bias, qv_bias, out_bias, up_bias, down_bias)]
    cuts = [0]
    for size in sizes:
        cuts.append(cuts[-1] + size)
    ada_bias_full, qv_full, out_bias_full, up_bias_full, down_bias_full = [
        small_all[:, a:b].reshape(-1).astype(F32) for a, b in zip(cuts[:-1], cuts[1:])
    ]
    cond_all = small_all[:, cuts[-1] :].reshape(dp * lats, width).astype(F32)
    depth = ada_weight.shape[0]
    silu_all = jax.nn.silu(cond_all).astype(HALF)
    silu_mine = lax.dynamic_slice_in_dim(silu_all, me * depth, depth, axis=1)
    partial = nn(silu_mine, ada_weight)
    row_here = z // sub
    wanted = partial.reshape(dp // 2, chip_lats, 6 * width)
    wanted = lax.dynamic_index_in_dim(wanted, row_here, 1, keepdims=True)
    wanted = jnp.broadcast_to(wanted, (dp // 2, 2, 6 * width)).reshape(dp, 6 * width)
    modulation = lax.psum_scatter(wanted, "dp", scatter_dimension=0, tiled=True)[0]
    modulation = (modulation + ada_bias_full).reshape(6, 1, width)
    shift_a, scale_a, gate_a, shift_b, scale_b, gate_b = [modulation[i] for i in range(6)]

    qkv_full = lax.all_gather(qkv_weight, "dp", axis=0, tiled=True)
    out_full = lax.all_gather(out_weight, "dp", axis=0, tiled=True)
    up_full = lax.all_gather(up_weight, "dp", axis=0, tiled=True)
    down_full = lax.all_gather(down_weight, "dp", axis=0, tiled=True)

    rows = spread(tokens).astype(F32)
    cot = spread(cotangent).astype(F32)

    hat_a, inverse_a = norm_parts(rows)
    normed_a = (hat_a * (1.0 + scale_a) + shift_a).astype(HALF)
    bias_all = jnp.concatenate([qv_full[:width], jnp.zeros((width,), F32), qv_full[width:]])
    projected = (nn(normed_a, qkv_full) + bias_all).astype(HALF)
    kv = projected[:, width:]
    ways = [(a, s) for s in range(sub) for a in range(2)]
    others = [shift(flip(kv) if a else kv, s) for a, s in ways[1:]]
    attended, logsum = attend(projected, others, width)
    branch_a = nn(attended, out_full) + out_bias_full
    middle = rows + gate_a * branch_a
    hat_b, inverse_b = norm_parts(middle)
    normed_b = (hat_b * (1.0 + scale_b) + shift_b).astype(HALF)
    hidden_pre = nn(normed_b, up_full) + up_bias_full
    hidden = gelu_tanh(hidden_pre).astype(HALF)
    branch_b = nn(hidden, down_full) + down_bias_full
    output = collect((middle + gate_b * branch_b).astype(HALF))

    grad_gate_b = jnp.sum(cot * branch_b, axis=0)
    grad_branch_b = cot * gate_b
    down_bias_grad = jnp.sum(grad_branch_b, axis=0)
    grad_branch_half = grad_branch_b.astype(HALF)
    down_weight_grad = tn(hidden, grad_branch_half).astype(HALF)
    grad_hidden = nt(grad_branch_half, down_full)
    _, gelu_back = jax.vjp(gelu_tanh, hidden_pre)
    grad_pre = gelu_back(grad_hidden)[0]
    up_bias_grad = jnp.sum(grad_pre, axis=0)
    grad_pre_half = grad_pre.astype(HALF)
    up_weight_grad = tn(normed_b, grad_pre_half).astype(HALF)
    grad_normed_b = nt(grad_pre_half, up_full)
    grad_shift_b = jnp.sum(grad_normed_b, axis=0)
    grad_scale_b = jnp.sum(grad_normed_b * hat_b, axis=0)
    grad_middle = cot + norm_grad(grad_normed_b, hat_b, inverse_b, scale_b)
    grad_gate_a = jnp.sum(grad_middle * branch_a, axis=0)
    grad_branch_a = grad_middle * gate_a
    out_bias_grad = jnp.sum(grad_branch_a, axis=0)
    grad_branch_a_half = grad_branch_a.astype(HALF)
    out_weight_grad = tn(attended, grad_branch_a_half).astype(HALF)
    grad_attended = nt(grad_branch_a_half, out_full).astype(HALF)

    results = attend_grad(projected, others, grad_attended, attended, logsum, width)
    count = len(ways)
    grad_query = results[0]
    grad_keys = results[1 : 1 + count]
    grad_values = results[1 + count :]
    grad_kv = [jnp.concatenate([k, v], axis=1) for k, v in zip(grad_keys, grad_values)]
    total_kv = grad_kv[0].astype(F32)
    for (a, s), part_kv in zip(ways[1:], grad_kv[1:]):
        back = shift(part_kv, -s)
        total_kv = total_kv + (flip(back) if a else back).astype(F32)
    grad_projected = jnp.concatenate([grad_query, total_kv.astype(HALF)], axis=1)
    qkv_weight_grad = tn(normed_a, grad_projected).astype(HALF)
    grad_proj_float = grad_projected.astype(F32)
    qv_bias_grad = jnp.concatenate(
        [
            jnp.sum(grad_proj_float[:, :width], axis=0),
            jnp.sum(grad_proj_float[:, 2 * width :], axis=0),
        ]
    )
    grad_normed_a = nt(grad_projected, qkv_full)
    grad_shift_a = jnp.sum(grad_normed_a, axis=0)
    grad_scale_a = jnp.sum(grad_normed_a * hat_a, axis=0)
    grad_tokens = grad_middle + norm_grad(grad_normed_a, hat_a, inverse_a, scale_a)
    tokens_grad = collect(grad_tokens.astype(HALF)).astype(F32)

    grad_mod = jnp.concatenate(
        [grad_shift_a, grad_scale_a, grad_gate_a, grad_shift_b, grad_scale_b, grad_gate_b]
    )
    every = lax.all_gather(grad_mod, "seq", axis=0, tiled=False)
    every = lax.all_gather(every, "dp", axis=0, tiled=False)
    every = every.reshape(dp // 2, 2, chip_lats, sub, 6 * width).sum(axis=(1, 3))
    every = every.reshape(dp * lats, 6 * width)
    every_half = every.astype(HALF)
    ada_weight_grad = tn(silu_mine, every_half)
    bias_len = ada_bias.shape[0]
    ada_bias_grad = jnp.sum(
        lax.dynamic_slice_in_dim(every, me * bias_len, bias_len, axis=1), axis=0
    )
    cond_part = nt(every_half, ada_weight).reshape(dp, lats, depth)
    cond_part = lax.all_to_all(cond_part, "dp", 0, 0, tiled=True)
    cond_part = cond_part.transpose(1, 0, 2).reshape(lats, width)
    cond_float = condition.astype(F32)
    sigmoid_cond = jax.nn.sigmoid(cond_float)
    silu_slope = sigmoid_cond * (1.0 + cond_float * (1.0 - sigmoid_cond))
    condition_grad = silu_slope * cond_part

    def reduce_weight(grad):
        share = lax.psum_scatter(grad, "dp", scatter_dimension=0, tiled=True)
        return lax.psum(share, "seq").astype(F32)

    bias_parts = jnp.concatenate(
        [
            b.reshape(dp, -1)
            for b in (qv_bias_grad, out_bias_grad, up_bias_grad, down_bias_grad)
        ],
        axis=1,
    )
    bias_parts = lax.psum_scatter(bias_parts, "dp", scatter_dimension=0, tiled=True)
    bias_parts = lax.psum(bias_parts, "seq")[0]
    cuts = [c - sizes[0] for c in cuts[1:]]
    qv_g, ob_g, ub_g, db_g = [bias_parts[a:b] for a, b in zip(cuts[:-1], cuts[1:])]
    return (
        output,
        tokens_grad,
        condition_grad,
        ada_weight_grad,
        ada_bias_grad,
        reduce_weight(qkv_weight_grad),
        qv_g,
        reduce_weight(out_weight_grad),
        ob_g,
        reduce_weight(up_weight_grad),
        ub_g,
        reduce_weight(down_weight_grad),
        db_g,
    )


def body(
    tokens,
    condition,
    ada_weight,
    ada_bias,
    qkv_weight,
    qv_bias,
    out_weight,
    out_bias,
    up_weight,
    up_bias,
    down_weight,
    down_bias,
    cotangent,
):
    lats, part, width = tokens.shape
    dp = lax.axis_size("dp")
    seq = lax.axis_size("seq")
    if (dp, seq, lats) != (8, 4, 2):
        return body_any(
            tokens,
            condition,
            ada_weight,
            ada_bias,
            qkv_weight,
            qv_bias,
            out_weight,
            out_bias,
            up_weight,
            up_bias,
            down_weight,
            down_bias,
            cotangent,
        )
    me = lax.axis_index("dp")
    depth = ada_weight.shape[0]
    wide = dp * up_bias.shape[0]
    cut = wide // (4 * dp)
    small = jnp.concatenate(
        [
            ada_bias.reshape(-1, LANES),
            qv_bias.reshape(-1, LANES),
            out_bias.reshape(-1, LANES),
            up_bias.reshape(-1, LANES),
            down_bias.reshape(-1, LANES),
            jnp.zeros((2, LANES), HALF),
            condition.reshape(-1, LANES),
        ],
        axis=0,
    ).astype(F32)
    f = forward(
        tokens, cotangent, qkv_weight, out_weight, up_weight, down_weight, small, ada_weight
    )
    b = backward(f, ada_weight, tokens.shape)
    shares = b["shares"].astype(F32)
    qkv_g = jnp.concatenate([shares[9], shares[11], shares[10]], axis=1)
    up_g = jnp.stack([shares[0], shares[6], shares[7], shares[8]])
    up_g = up_g.reshape(4, depth, dp, cut).transpose(1, 2, 0, 3).reshape(depth, wide)
    down_g = shares[2:6].reshape(4 * cut, width)
    every = b["gmod"]
    ada_weight_grad = tn(f["silu"], every.astype(HALF).reshape(dp * lats, 6 * width))
    ada_bias_grad = lax.dynamic_slice_in_dim(
        jnp.sum(every, axis=0).reshape(-1), me * ada_bias.shape[0], ada_bias.shape[0]
    )
    cond_part = b["condp"][:, :lats].transpose(1, 0, 2).reshape(lats, width)
    cond_float = condition.astype(F32)
    sigmoid_cond = jax.nn.sigmoid(cond_float)
    silu_slope = sigmoid_cond * (1.0 + cond_float * (1.0 - sigmoid_cond))
    biases = b["biases"]
    return (
        b["output"],
        b["tokens"].astype(F32),
        silu_slope * cond_part,
        ada_weight_grad,
        ada_bias_grad,
        qkv_g,
        biases[0:2].reshape(-1),
        shares[1],
        biases[2],
        up_g,
        biases[3:7].reshape(-1),
        down_g,
        biases[7],
    )


def solution(mesh):
    return jax.shard_map(
        body,
        mesh=mesh,
        in_specs=(
            P("dp", "seq", None),
            P("dp", None),
            P("dp", None),
            P("dp"),
            P("dp", None),
            P("dp"),
            P("dp", None),
            P("dp"),
            P("dp", None),
            P("dp"),
            P("dp", None),
            P("dp"),
            P("dp", "seq", None),
        ),
        out_specs=(
            P("dp", "seq", None),
            P("dp", "seq", None),
            P("dp", None),
            P("dp", None),
            P("dp"),
            P("dp", None),
            P("dp"),
            P("dp", None),
            P("dp"),
            P("dp", None),
            P("dp"),
            P("dp", None),
            P("dp"),
        ),
        check_vma=False,
    )
```

```python
import functools

import jax
import jax.numpy as jnp
from jax import lax
from jax.experimental import pallas as pl
from jax.experimental.pallas import tpu as pltpu
from jax.sharding import PartitionSpec as P

HD = 64
LANES = 128
EPSILON = 1e-06
HALF = jnp.bfloat16
F32 = jnp.float32


def nn(a, b):
    return jnp.dot(a, b, preferred_element_type=F32)


def nt(a, b):
    return lax.dot_general(a, b, (((1,), (1,)), ((), ())), preferred_element_type=F32)


def tn(a, b):
    return lax.dot_general(a, b, (((0,), (0,)), ((), ())), preferred_element_type=F32)


def attend_kernel(groups, *refs):
    q_ref = refs[0]
    k_refs = refs[1 : 1 + groups]
    v_refs = refs[1 + groups : 1 + 2 * groups]
    out_ref, lse_ref, lse_acc = refs[1 + 2 * groups :]
    step = pl.program_id(0)
    rows = q_ref.shape[0]
    block = 256
    low = lax.broadcasted_iota(jnp.int32, (block, LANES), 1) < HD
    lane = lax.broadcasted_iota(jnp.int32, (block, LANES), 1)
    for start in range(0, rows, block):
        here = pl.ds(start, block)
        q = q_ref[here, :] * HALF(HD**-0.5)
        pieces = []
        for head in range(2):
            own = low if head == 0 else jnp.logical_not(low)
            qm = jnp.where(own, q, jnp.zeros_like(q))
            scores = [nt(qm, k[...]) for k in k_refs]
            peak = functools.reduce(
                jnp.maximum, [jnp.max(s, axis=-1, keepdims=True) for s in scores]
            )
            raised = [jnp.exp(s - peak) for s in scores]
            total = sum(jnp.sum(e, axis=-1, keepdims=True) for e in raised)
            mixed = sum(nn(e.astype(HALF), v[...]) for e, v in zip(raised, v_refs))
            pieces.append(mixed / total)
            spot = lane == 2 * step + head
            logsum = jnp.broadcast_to(peak + jnp.log(total), (block, LANES))
            lse_acc[here, :] = jnp.where(spot, logsum, lse_acc[here, :])
        out_ref[here, :] = jnp.where(low, pieces[0], pieces[1]).astype(HALF)

    @pl.when(step == pl.num_programs(0) - 1)
    def _():
        lse_ref[...] = lse_acc[...].T


def attend(projected, others, width):
    rows = projected.shape[0]
    groups = 1 + len(others)
    tiles = width // LANES
    col = lambda base: pl.BlockSpec((rows, LANES), lambda i, base=base: (0, base + i))
    return pl.pallas_call(
        functools.partial(attend_kernel, groups),
        grid=(tiles,),
        out_shape=(
            jax.ShapeDtypeStruct((rows, width), HALF),
            jax.ShapeDtypeStruct((LANES, rows), F32),
        ),
        in_specs=[col(0), col(tiles)] + [col(0)] * len(others) + [col(2 * tiles)] + [col(tiles)] * len(others),
        out_specs=(col(0), pl.BlockSpec((LANES, rows), lambda i: (0, 0))),
        scratch_shapes=[pltpu.VMEM((rows, LANES), F32)],
        compiler_params=pltpu.CompilerParams(vmem_limit_bytes=48 << 20),
        name="attend",
    )(projected, projected, *others, projected, *others)


def attend_grad_kernel(groups, *refs):
    q_ref = refs[0]
    k_refs = refs[1 : 1 + groups]
    v_refs = refs[1 + groups : 1 + 2 * groups]
    do_ref, o_ref, lse_ref = refs[1 + 2 * groups : 4 + 2 * groups]
    dq_ref = refs[4 + 2 * groups]
    dk_refs = refs[5 + 2 * groups : 5 + 3 * groups]
    dv_refs = refs[5 + 3 * groups : 5 + 4 * groups]
    step = pl.program_id(0)
    rows = q_ref.shape[0]
    block = 256
    scale = HALF(HD**-0.5)
    q = q_ref[...] * scale
    grad = do_ref[...]
    product = grad.astype(F32) * o_ref[...].astype(F32)
    top = product.astype(HALF)
    rest = (product - top.astype(F32)).astype(HALF)
    pick = lax.broadcasted_iota(jnp.int32, (8, LANES), 0) == (
        lax.broadcasted_iota(jnp.int32, (8, LANES), 1) // HD
    )
    pick = jnp.where(pick, 1.0, 0.0).astype(HALF)
    inner = nt(pick, top) + nt(pick, rest)
    low = lax.broadcasted_iota(jnp.int32, (block, LANES), 1) < HD
    dq_t = [jnp.zeros((LANES, rows), F32) for _ in range(2)]
    for k_ref, v_ref, dk_ref, dv_ref in zip(k_refs, v_refs, dk_refs, dv_refs):
        for start in range(0, rows, block):
            here = pl.ds(start, block)
            k = k_ref[here, :]
            v = v_ref[here, :]
            k_t = k.T
            dks, dvs = [], []
            for head in range(2):
                own = low if head == 0 else jnp.logical_not(low)
                lse = lse_ref[pl.ds(2 * step + head, 1), :]
                scores = nt(jnp.where(own, k, jnp.zeros_like(k)), q)
                probs = jnp.exp(scores - lse)
                dvs.append(nn(probs.astype(HALF), grad))
                gp = nt(jnp.where(own, v, jnp.zeros_like(v)), grad)
                gs = (probs * (gp - inner[head : head + 1, :])).astype(HALF)
                dks.append(nn(gs, q))
                dq_t[head] = dq_t[head] + nn(k_t, gs)
            dk_ref[here, :] = jnp.where(low, dks[0], dks[1]).astype(HALF)
            dv_ref[here, :] = jnp.where(low, dvs[0], dvs[1]).astype(HALF)
    upper = lax.broadcasted_iota(jnp.int32, (LANES, rows), 0) < HD
    dq = jnp.where(upper, dq_t[0], dq_t[1]).T * HD**-0.5
    dq_ref[...] = dq.astype(HALF)


def attend_grad(projected, others, grad, attended, logsum, width):
    rows = projected.shape[0]
    groups = 1 + len(others)
    tiles = width // LANES
    col = lambda base: pl.BlockSpec((rows, LANES), lambda i, base=base: (0, base + i))
    out = jax.ShapeDtypeStruct((rows, width), HALF)
    return pl.pallas_call(
        functools.partial(attend_grad_kernel, groups),
        grid=(tiles,),
        out_shape=(out,) * (1 + 2 * groups),
        in_specs=[col(0), col(tiles)]
        + [col(0)] * len(others)
        + [col(2 * tiles)]
        + [col(tiles)] * len(others)
        + [col(0), col(0), pl.BlockSpec((LANES, rows), lambda i: (0, 0))],
        out_specs=(col(0),) * (1 + 2 * groups),
        compiler_params=pltpu.CompilerParams(vmem_limit_bytes=48 << 20),
        name="attend_grad",
    )(projected, projected, *others, projected, *others, grad, attended, logsum)


def norm_parts(rows):
    centred = rows - jnp.mean(rows, axis=-1, keepdims=True)
    variance = jnp.mean(centred * centred, axis=-1, keepdims=True)
    inverse = lax.rsqrt(variance + EPSILON)
    return centred * inverse, inverse


def norm_grad(grad, hat, inverse, scale):
    g = grad * (1.0 + scale)
    return (
        g
        - jnp.mean(g, axis=-1, keepdims=True)
        - hat * jnp.mean(g * hat, axis=-1, keepdims=True)
    ) * inverse


def gelu_tanh(inputs):
    return jax.nn.gelu(inputs, approximate=True)


MESH_ID = pl.DeviceIdType.MESH
CHUNKS = 12
KEYS, VALUES, QUERIES, OUT, FEED = 0, 1, 2, 3, 4


def guarded(low, value, high, run):
    if isinstance(value, int):
        if low <= value < high:
            run(value)
        return

    @pl.when(jnp.logical_and(value >= low, value < high))
    def _():
        run(value)


class Place:
    def __init__(self):
        self.d = lax.axis_index("dp")
        self.z = lax.axis_index("seq")
        self.c = self.d % 2
        self.x = self.d // 2 % 2
        self.y = self.d // 4
        self.p = self.d // 2

    def plane(self, flip):
        return (jnp.bitwise_xor(self.d, flip), self.z)

    def line(self, flip):
        return (self.d, jnp.bitwise_xor(self.z, flip))


def remote(src, dst, send, recv, peer):
    return pltpu.make_async_remote_copy(
        src_ref=src,
        dst_ref=dst,
        send_sem=send,
        recv_sem=recv,
        device_id=peer,
        device_id_type=MESH_ID,
    )


def greet(peers):
    barrier = pltpu.get_barrier_semaphore()
    for peer in peers:
        pl.semaphore_signal(barrier, inc=1, device_id=peer, device_id_type=MESH_ID)
    pl.semaphore_wait(barrier, len(peers))


class Gather:
    SENDS = (
        (2, 0, "all"),
        (4, 0, "all"),
        (1, 0, "all"),
        (1, 2, "all"),
        (1, 4, "all"),
        (4, 2, "first"),
        (2, 4, "second"),
        (1, 6, "near"),
        (1, 6, "far"),
        (None, 6, "near"),
    )

    def __init__(self, here, whole, send, recv):
        self.here, self.whole, self.send, self.recv = here, whole, send, recv
        self.depth = whole.shape[1] // 8

    def _block(self, chunk, flip, part):
        n, side = self.depth, self.here.z % 2
        size, lo = {
            "all": (n, 0),
            "first": (n // 4, side * (n // 2)),
            "second": (n // 4, side * (n // 2) + n // 4),
            "near": (n // 2, side * (n // 2)),
            "far": (n // 2, (1 - side) * (n // 2)),
        }[part]
        row = pl.multiple_of(jnp.bitwise_xor(self.here.d, flip) * n + lo, 32)
        return self.whole.at[chunk, pl.ds(row, size), :]

    def _copy(self, chunk, slot, arriving=False):
        flip, block, part = self.SENDS[slot]
        if flip is None:
            peer = self.here.line(1)
            part = "far" if arriving else part
        else:
            peer = self.here.plane(flip)
            block = flip ^ block if arriving else block
        ref = self._block(chunk, block, part)
        return remote(ref, ref, self.send.at[chunk, slot], self.recv.at[chunk, slot], peer)

    def begin(self, i):
        for slot in (0, 1, 2):
            self._copy(i, slot).start()

    def relay(self, i):
        self._copy(i, 0, True).wait_recv()
        self._copy(i, 5).start()
        self._copy(i, 1, True).wait_recv()
        self._copy(i, 6).start()
        self._copy(i, 3).start()
        self._copy(i, 4).start()

    def share(self, i):
        self._copy(i, 5, True).wait_recv()
        self._copy(i, 6, True).wait_recv()
        self._copy(i, 9).start()
        self._copy(i, 7).start()

    def hand(self, i):
        self._copy(i, 9, True).wait_recv()
        self._copy(i, 8).start()

    def finish(self, i):
        for slot in (2, 3, 4, 7, 8):
            self._copy(i, slot, True).wait_recv()

    def tick(self, t, prepare):
        def begin(i):
            prepare(i)
            self.begin(i)

        guarded(0, t - 5, CHUNKS, self.finish)
        guarded(0, t - 4, CHUNKS, self.hand)
        guarded(0, t - 3, CHUNKS, self.share)
        guarded(0, t - 2, CHUNKS, self.relay)
        lead = 5
        if isinstance(t, int):
            for i in (t,) if t < lead else (t, t + 1) if t == lead else (t + 1,):
                guarded(0, i, CHUNKS, begin)
        else:
            guarded(lead, t + 1, CHUNKS, begin)

    def drain(self):
        @pl.loop(0, CHUNKS)
        def _(i):
            for slot in range(len(self.SENDS)):
                self._copy(i, slot).wait_send()


class Spread:
    def __init__(self, here, source, landing, send, recv):
        self.here, self.source, self.landing = here, source, landing
        self.send, self.recv = send, recv
        self.size = source.shape[1] // 2

    def _each(self):
        here = self.here
        lats = self.source.shape[0]
        for j in range(lats):
            for core in range(2):
                z = lats * here.c + j
                own = jnp.logical_and(z == here.z, core == here.c)
                src = self.source.at[j, pl.ds(core * self.size, self.size), :]
                peer = (here.d - here.c + core, z)
                yield own, j * 2 + core, src, peer

    def _land(self, z):
        return self.landing.at[pl.ds(pl.multiple_of(z * self.size, self.size), self.size), :]

    def start(self, pieces=range(4)):
        z = self.here.z
        for own, index, src, peer in self._each():
            if index not in pieces:
                continue

            @pl.when(own)
            def _():
                pltpu.make_async_copy(src, self._land(z), self.recv.at[z]).start()

            @pl.when(jnp.logical_not(own))
            def _():
                remote(src, self._land(z), self.send.at[index], self.recv.at[z], peer).start()

    def wait(self):
        src = self.source.at[0, pl.ds(0, self.size), :]
        for z in range(4):
            pltpu.make_async_copy(src, self._land(z), self.recv.at[z]).wait()

    def drain(self):
        z = self.here.z
        for own, index, src, peer in self._each():

            @pl.when(jnp.logical_not(own))
            def _():
                remote(src, self._land(z), self.send.at[index], self.recv.at[z], peer).wait_send()


def gelu_both(v):
    root = 0.7978845608028654
    square = v * v
    t = jnp.tanh(root * (v + 0.044715 * (v * square)))
    half = 0.5 * (1.0 + t)
    slope = half + (0.5 * root) * v * (1.0 - t * t) * (1.0 + (3 * 0.044715) * square)
    return half * v, slope


def column_sum(x):
    return jnp.sum(x, axis=0, keepdims=True)


FORWARD_OUTS = (
    "whole",
    "xs",
    "cots",
    "qkv",
    "kvo",
    "att",
    "lse",
    "mid",
    "bra",
    "nb",
    "hid",
    "gph",
    "gbh",
    "outb",
    "gnb",
    "vec",
    "silu",
    "ups",
)


def forward_kernel(tokens, cot, qkv_w, out_w, up_w, down_w, small, ada, *refs):
    outs = dict(zip(FORWARD_OUTS, refs))
    (
        w,
        small_all,
        part,
        mod_in,
        mod,
        vec,
        silu,
        xs,
        ct,
        na,
        qkv,
        kvo,
        att,
        lse_acc,
        lse,
        mid,
        bra,
        nb,
        gbh,
        bb,
        gnb,
        hid,
        gph,
        ups,
        g_send,
        g_recv,
        own_sem,
        sp_send,
        sp_recv,
        sm_send,
        sm_recv,
        md_send,
        md_recv,
        kv_send,
        kv_recv,
        out_sem,
        ff_sem,
    ) = refs[len(FORWARD_OUTS) :]
    here = Place()
    d, z, c = here.d, here.z, here.c
    depth, width = qkv_w.shape[0], out_w.shape[1]
    rows = xs.shape[0]
    wide = up_w.shape[1]
    cut = wide // 32
    tile = 256

    mine = pl.ds(pl.multiple_of(d * depth, depth), depth)
    for i, k in ((KEYS, 1), (VALUES, 2), (QUERIES, 0)):
        pltpu.make_async_copy(
            qkv_w.at[:, pl.ds(k * width, width)], w.at[i, mine, :], own_sem.at[i]
        ).start()
    pltpu.make_async_copy(out_w, w.at[OUT, mine, :], own_sem.at[OUT]).start()
    for j in range(4):
        for k in range(8):
            pltpu.make_async_copy(
                up_w.at[:, pl.ds((4 * k + j) * cut, cut)],
                w.at[FEED + 2 * j, mine, pl.ds(k * cut, cut)],
                own_sem.at[FEED + 2 * j],
            ).start()
        pltpu.make_async_copy(
            down_w.at[pl.ds(j * depth, depth), :], w.at[FEED + 2 * j + 1, mine, :], own_sem.at[FEED + 2 * j + 1]
        ).start()

    def prepare(i):
        pltpu.make_async_copy(out_w, w.at[i, mine, :], own_sem.at[i]).wait()

    peers = [here.plane(f) for f in range(1, 8)]
    for core in range(2):
        for f in range(1, 4):
            peers.append((d - c + core, jnp.bitwise_xor(z, f)))
    greet(peers)

    gather = Gather(here, w, g_send, g_recv)
    tick = functools.partial(gather.tick, prepare=prepare)
    first = Spread(here, tokens, xs, sp_send.at[0], sp_recv.at[0])
    second = Spread(here, cot, ct, sp_send.at[1], sp_recv.at[1])

    def small_copy(f):
        dst = small_all.at[d]
        return remote(small, dst, sm_send.at[f - 1], sm_recv.at[f - 1], here.plane(f))

    for f in range(1, 8):
        small_copy(f).start()
    first.start()
    tick(0)
    tick(1)
    small_all[d] = small[...]
    for f in range(1, 8):
        small_copy(f).wait_recv()

    picked = [
        small_all[i // 2, pl.ds(16 + 8 * (i % 2) + d, 1), :] for i in range(16)
    ]
    cond = jnp.concatenate(picked, axis=0)
    silu[...] = (cond * jax.nn.sigmoid(cond)).astype(HALF)
    for i in range(6):
        product = nn(silu[...], ada[:, pl.ds(i * width, width)])
        for k in range(8):
            part[:, 8 * i + k, :] = product[:, k * LANES : (k + 1) * LANES]

    def mod_copy(f):
        flip = jnp.bitwise_xor(d, f)
        src = part.at[4 * (flip // 2) + z]
        return remote(src, mod_in.at[d], md_send.at[f - 1], md_recv.at[f - 1], here.plane(f))

    for f in range(1, 8):
        mod_copy(f).start()
    mod_in[d] = part[4 * here.p + z]
    tick(2)
    for f in range(1, 8):
        mod_copy(f).wait_recv()
    mod[...] = sum(mod_in[k] for k in range(1, 8)) + mod_in[0]
    for k in range(8):
        mod[pl.ds(6 * k, 6), :] = mod[pl.ds(6 * k, 6), :] + small_all[k, pl.ds(0, 6), :]
    for i in range(6):
        for k in range(8):
            vec[pl.ds(i, 1), pl.ds(k * LANES, LANES)] = mod[pl.ds(8 * i + k, 1), :]
    for k in range(8):
        lanes = pl.ds(k * LANES, LANES)
        vec[pl.ds(8, 1), lanes] = small_all[k // 2, pl.ds(6 + k % 2, 1), :]
        vec[pl.ds(9, 1), lanes] = small_all[4 + k // 2, pl.ds(6 + k % 2, 1), :]
        vec[pl.ds(10, 1), lanes] = small_all[k, pl.ds(8, 1), :]
        vec[pl.ds(11, 1), lanes] = small_all[k, pl.ds(13, 1), :]
        for j in range(4):
            vec[pl.ds(12 + j, 1), lanes] = small_all[k, pl.ds(9 + j, 1), :]

    def row(i):
        return vec[pl.ds(i, 1), :]

    exits = []

    def leave(src, name, index=None):
        dst = outs[name] if index is None else outs[name].at[index]
        copy = pltpu.make_async_copy(src, dst, out_sem.at[len(exits)])
        copy.start()
        exits.append(copy)

    leave(vec, "vec")
    leave(silu, "silu")
    tick(3)
    tick(4)
    first.wait()
    leave(xs, "xs")

    block = 128

    @pl.loop(0, rows // block)
    def _(i):
        part_rows = pl.ds(pl.multiple_of(i * block, block), block)
        hat, _ = norm_parts(xs[part_rows, :].astype(F32))
        na[part_rows, :] = (hat * (1.0 + row(1)) + row(0)).astype(HALF)

    def project(chunk, index, bias):
        for n in range(width // tile):
            cols = pl.ds(n * tile, tile)
            value = nn(na[...], w[chunk, :, cols])
            if bias is not None:
                value = value + vec[pl.ds(bias, 1), cols]
            qkv[index, :, cols] = value.astype(HALF)

    def kv_copy(k):
        return remote(qkv.at[1 + k], kvo.at[k], kv_send.at[k], kv_recv.at[k], here.plane(1))

    tick(5)
    second.start((0,))
    leave(w.at[KEYS], "whole", KEYS)
    project(KEYS, 1, None)
    kv_copy(0).start()
    tick(6)
    second.start((1,))
    leave(w.at[VALUES], "whole", VALUES)
    project(VALUES, 2, 9)
    kv_copy(1).start()
    tick(7)
    second.start((2, 3))
    leave(w.at[QUERIES], "whole", QUERIES)
    project(QUERIES, 0, 8)
    leave(qkv, "qkv")
    for k in range(2):
        kv_copy(k).wait_recv()
    leave(kvo, "kvo")

    span = 256
    low = lax.broadcasted_iota(jnp.int32, (span, LANES), 1) < HD
    lane = lax.broadcasted_iota(jnp.int32, (span, LANES), 1)

    @pl.loop(0, width // LANES)
    def _(step):
        cols = pl.ds(pl.multiple_of(step * LANES, LANES), LANES)
        keys = [qkv[1, :, cols], kvo[0, :, cols]]
        values = [qkv[2, :, cols], kvo[1, :, cols]]
        for start in range(0, rows, span):
            part_rows = pl.ds(start, span)
            q = qkv[0, part_rows, cols] * HALF(HD**-0.5)
            pieces = []
            for head in range(2):
                own = low if head == 0 else jnp.logical_not(low)
                qm = jnp.where(own, q, jnp.zeros_like(q))
                scores = [nt(qm, k) for k in keys]
                peak = functools.reduce(
                    jnp.maximum, [jnp.max(s, axis=-1, keepdims=True) for s in scores]
                )
                raised = [jnp.exp(s - peak) for s in scores]
                total = sum(jnp.sum(e, axis=-1, keepdims=True) for e in raised)
                mixed = sum(nn(e.astype(HALF), v) for e, v in zip(raised, values))
                pieces.append(mixed / total)
                logsum = jnp.broadcast_to(peak + jnp.log(total), (span, LANES))
                lse_acc[part_rows, :] = jnp.where(
                    lane == 2 * step + head, logsum, lse_acc[part_rows, :]
                )
            att[part_rows, cols] = jnp.where(low, pieces[0], pieces[1]).astype(HALF)

        @pl.when(step % 3 == 2)
        def _():
            gather.tick(8 + step // 3, prepare)

    lse[...] = lse_acc[...].T
    leave(lse, "lse")
    leave(att, "att")
    leave(w.at[OUT], "whole", OUT)
    second.wait()
    leave(ct, "cots")

    for n in range(width // tile):
        cols = pl.ds(n * tile, tile)
        branch = nn(att[...], w[OUT, :, cols]) + vec[pl.ds(10, 1), cols]
        bra[:, cols] = branch.astype(HALF)
        mid[:, cols] = xs[:, cols].astype(F32) + vec[pl.ds(2, 1), cols] * branch
    leave(mid, "mid")
    leave(bra, "bra")
    tick(10)

    @pl.loop(0, rows // block)
    def _(i):
        part_rows = pl.ds(pl.multiple_of(i * block, block), block)
        hat, _ = norm_parts(mid[part_rows, :])
        nb[part_rows, :] = (hat * (1.0 + row(4)) + row(3)).astype(HALF)
        gbh[part_rows, :] = (ct[part_rows, :].astype(F32) * row(5)).astype(HALF)
        bb[part_rows, :] = jnp.broadcast_to(row(11), (block, width))
        gnb[part_rows, :] = jnp.zeros((block, width), F32)

    leave(nb, "nb")
    leave(gbh, "gbh")

    def ff_copies(j, slot):
        return (
            pltpu.make_async_copy(hid.at[slot], outs["hid"].at[j], ff_sem.at[0, slot]),
            pltpu.make_async_copy(gph.at[slot], outs["gph"].at[j], ff_sem.at[1, slot]),
        )

    @pl.loop(0, 4)
    def _(j):
        slot = j % 2
        up, down = FEED + 2 * j, FEED + 2 * j + 1

        @pl.when(j >= 2)
        def _():
            for copy in ff_copies(j, slot):
                copy.wait()

        for n in range(width // tile):
            cols = pl.ds(n * tile, tile)
            pre = nn(nb[...], w[up, :, cols]) + vec[pl.ds(12 + j, 1), cols]
            grad = nt(gbh[...], w[down, cols, :])
            value, slope = gelu_both(pre)
            grad = grad * slope
            ups[pl.ds(j, 1), cols] = column_sum(grad)
            hid[slot, :, cols] = value.astype(HALF)
            gph[slot, :, cols] = grad.astype(HALF)
        for copy in ff_copies(j, slot):
            copy.start()
        gather.tick(11 + 2 * j, prepare)
        for n in range(width // tile):
            cols = pl.ds(n * tile, tile)
            bb[:, cols] = bb[:, cols] + nn(hid[slot], w[down, :, cols])
            gnb[:, cols] = gnb[:, cols] + nt(gph[slot], w[up, cols, :])
        gather.tick(12 + 2 * j, prepare)

    leave(gnb, "gnb")
    ups[pl.ds(4, 4), :] = jnp.zeros((4, width), F32)

    @pl.loop(0, rows // block)
    def _(i):
        part_rows = pl.ds(pl.multiple_of(i * block, block), block)
        branch = bb[part_rows, :]
        grad = ct[part_rows, :].astype(F32)
        na[part_rows, :] = (mid[part_rows, :] + row(5) * branch).astype(HALF)
        ups[pl.ds(4, 1), :] = ups[pl.ds(4, 1), :] + column_sum(grad * branch)
        ups[pl.ds(5, 1), :] = ups[pl.ds(5, 1), :] + column_sum(grad)

    leave(na, "outb")
    leave(ups, "ups")
    for slot in range(2):
        for copy in ff_copies(slot, slot):
            copy.wait()
    for copy in exits:
        copy.wait()
    gather.drain()
    first.drain()
    second.drain()
    for f in range(1, 8):
        small_copy(f).wait_send()
        mod_copy(f).wait_send()
    for k in range(2):
        kv_copy(k).wait_send()


def forward(tokens, cot, qkv_w, out_w, up_w, down_w, small, ada):
    depth, width = qkv_w.shape[0], out_w.shape[1]
    rows = tokens.shape[0] * tokens.shape[1]
    sds = jax.ShapeDtypeStruct
    flat, real = sds((rows, width), HALF), sds((rows, width), F32)
    shapes = dict(
        whole=sds((4, width, width), HALF),
        xs=flat,
        cots=flat,
        qkv=sds((3, rows, width), HALF),
        kvo=sds((2, rows, width), HALF),
        att=flat,
        lse=sds((LANES, rows), F32),
        mid=real,
        bra=flat,
        nb=flat,
        hid=sds((4, rows, width), HALF),
        gph=sds((4, rows, width), HALF),
        gbh=flat,
        outb=flat,
        gnb=real,
        vec=sds((16, width), F32),
        silu=sds((16, LANES), HALF),
        ups=sds((8, width), F32),
    )
    hbm = pl.BlockSpec(memory_space=pl.ANY)
    vmem = pl.BlockSpec(memory_space=pltpu.VMEM)
    dma = pltpu.SemaphoreType.DMA
    half = lambda *s: pltpu.VMEM(s, HALF)
    full = lambda *s: pltpu.VMEM(s, F32)
    scratch = [
        half(CHUNKS, width, width),
        full(8, 32, LANES),
        full(16, 48, LANES),
        full(8, 48, LANES),
        full(48, LANES),
        full(16, width),
        half(16, LANES),
        half(rows, width),
        half(rows, width),
        half(rows, width),
        half(3, rows, width),
        half(2, rows, width),
        half(rows, width),
        full(rows, LANES),
        full(LANES, rows),
        full(rows, width),
        half(rows, width),
        half(rows, width),
        half(rows, width),
        full(rows, width),
        full(rows, width),
        half(2, rows, width),
        half(2, rows, width),
        full(8, width),
        dma((CHUNKS, 10)),
        dma((CHUNKS, 10)),
        dma((CHUNKS,)),
        dma((2, 4)),
        dma((2, 4)),
        dma((7,)),
        dma((7,)),
        dma((7,)),
        dma((7,)),
        dma((2,)),
        dma((2,)),
        dma((24,)),
        dma((2, 2)),
    ]
    got = pl.pallas_call(
        forward_kernel,
        out_shape=tuple(shapes[name] for name in FORWARD_OUTS),
        in_specs=[hbm] * 6 + [vmem] * 2,
        out_specs=(hbm,) * len(FORWARD_OUTS),
        scratch_shapes=scratch,
        compiler_params=pltpu.CompilerParams(
            collective_id=1, has_side_effects=True, vmem_limit_bytes=67043328
        ),
        name="forward",
    )(tokens, cot, qkv_w, out_w, up_w, down_w, small, ada)
    return dict(zip(FORWARD_OUTS, got))


class Reduce:
    COUNT = 2 * CHUNKS
    RING = 6
    DEEP = 8

    def __init__(self, here, bufs, send, recv, credit):
        self.here = here
        (self.dw, self.rc, self.rx, self.ry, self.t, self.ry2, self.rx2, self.r, self.rz1, self.q, self.rz2, self.out) = bufs
        self.send, self.recv, self.credit = send, recv, credit
        self.depth, self.cols = self.out.shape[1], self.out.shape[2] // 2
        self.half = self.cols // 2
        self.inner = jnp.logical_or(here.z == 1, here.z == 2)
        self.outer = jnp.logical_not(self.inner)

    def _copy(self, i, slot, arriving=False):
        here = self.here
        s, deep = lax.rem(i, self.RING), lax.rem(i, self.DEEP)
        low, high = pl.ds(0, self.half), pl.ds(self.half, self.half)
        if slot == 0:
            src, dst, peer = self.dw.at[s, :, :, 1 - here.c], self.rc.at[deep], here.plane(1)
        elif slot == 1:
            src, dst, peer = self.dw.at[s, :, 1 - here.x, here.c, :, low], self.rx.at[deep], here.plane(2)
        elif slot == 2:
            src, dst, peer = self.dw.at[s, 1 - here.y, :, here.c, :, high], self.ry.at[deep], here.plane(4)
        elif slot == 3:
            src, dst, peer = self.t.at[s, 0, 1 - here.y], self.ry2.at[i], here.plane(4)
        elif slot == 4:
            src, dst, peer = self.t.at[s, 1, 1 - here.x], self.rx2.at[i], here.plane(2)
        elif slot == 5:
            src, dst, peer = self.r.at[s], self.rz1.at[i], here.line(1)
        elif slot == 6:
            src, dst, peer = self.q.at[s], self.rz2.at[i], here.line(3)
        else:
            src = dst = self._share(i)
            peer = here.line(1)
        return remote(src, dst, self.send.at[i, slot], self.recv.at[i, slot], peer)

    def _share(self, i):
        cols = pl.ds(pl.multiple_of(lax.rem(i, 2) * self.cols, self.cols), self.cols)
        return self.out.at[lax.div(i, 2), :, cols]

    def _sent(self, i, *slots):
        def wait(k):
            for slot in slots:
                self._copy(k, slot).wait_send()

        guarded(0, i - self.RING, self.COUNT, wait)

    def _spend(self, i, *kinds):
        def wait(k):
            for kind in kinds:
                pl.semaphore_wait(self.credit.at[kind], 1)

        guarded(self.DEEP, i, self.COUNT, wait)

    def _grant(self, i, kind, flip):
        def signal(k):
            pl.semaphore_signal(
                self.credit.at[kind], inc=1, device_id=self.here.plane(flip), device_id_type=MESH_ID
            )

        guarded(0, i, self.COUNT - self.DEEP, signal)

    def produce(self, i, side, left_t, right):
        s = lax.rem(i, self.RING)
        self._sent(i, 0, 1, 2)
        tile = 256
        for n in range(self.cols // tile):
            value = nn(left_t[...], right[:, pl.ds(side * self.cols + n * tile, tile)]).astype(HALF)
            for k in range(8):
                self.dw[s, k // 4, k // 2 % 2, k % 2, :, pl.ds(n * tile, tile)] = value[
                    k * self.depth : (k + 1) * self.depth
                ]
        self._spend(i, 0)
        self._copy(i, 0).start()

    def plane(self, i):
        s, deep = lax.rem(i, self.RING), lax.rem(i, self.DEEP)
        c = self.here.c
        self._copy(i, 0, True).wait_recv()
        for y in range(2):
            for x in range(2):
                self.dw[s, y, x, c] = (
                    self.dw[s, y, x, c].astype(F32) + self.rc[deep, y, x].astype(F32)
                ).astype(HALF)
        self._grant(i, 0, 1)
        self._spend(i, 1, 2)
        self._copy(i, 1).start()
        self._copy(i, 2).start()

    def cross(self, i):
        s, deep = lax.rem(i, self.RING), lax.rem(i, self.DEEP)
        here = self.here
        low, high = pl.ds(0, self.half), pl.ds(self.half, self.half)
        self._copy(i, 1, True).wait_recv()
        self._copy(i, 2, True).wait_recv()
        self._sent(i, 3, 4)
        for k in range(2):
            self.t[s, 0, k] = (
                self.dw[s, k, here.x, here.c, :, low].astype(F32) + self.rx[deep, k].astype(F32)
            ).astype(HALF)
            self.t[s, 1, k] = (
                self.dw[s, here.y, k, here.c, :, high].astype(F32) + self.ry[deep, k].astype(F32)
            ).astype(HALF)
        self._grant(i, 1, 2)
        self._grant(i, 2, 4)
        self._copy(i, 3).start()
        self._copy(i, 4).start()

    def line(self, i):
        s = lax.rem(i, self.RING)
        here = self.here
        self._copy(i, 3, True).wait_recv()
        self._copy(i, 4, True).wait_recv()

        @pl.when(self.outer)
        def _():
            self._sent(i, 5)

        self.r[s, :, pl.ds(0, self.half)] = (
            self.t[s, 0, here.y].astype(F32) + self.ry2[i].astype(F32)
        ).astype(HALF)
        self.r[s, :, pl.ds(self.half, self.half)] = (
            self.t[s, 1, here.x].astype(F32) + self.rx2[i].astype(F32)
        ).astype(HALF)

        @pl.when(self.outer)
        def _():
            self._copy(i, 5).start()

    def far(self, i):
        s = lax.rem(i, self.RING)

        @pl.when(self.inner)
        def _():
            self._copy(i, 5, True).wait_recv()
            self._sent(i, 6)
            self.q[s] = (self.r[s].astype(F32) + self.rz1[i].astype(F32)).astype(HALF)
            self._copy(i, 6).start()

    def close(self, i):
        s = lax.rem(i, self.RING)

        @pl.when(self.inner)
        def _():
            self._copy(i, 6, True).wait_recv()
            self._share(i)[...] = (self.q[s].astype(F32) + self.rz2[i].astype(F32)).astype(HALF)
            self._copy(i, 7).start()

    def finish(self, i):
        @pl.when(self.outer)
        def _():
            self._copy(i, 7, True).wait_recv()

    LAGS = (11, 9, 7, 5, 3, 0)

    def tick(self, t):
        steps = (self.finish, self.close, self.far, self.line, self.cross, self.plane)
        for lag, step in zip(self.LAGS, steps):
            guarded(0, t - lag, self.COUNT, step)

    def drain(self):
        for k in range(self.COUNT - self.RING, self.COUNT):
            for slot in range(5):
                self._copy(k, slot).wait_send()

        @pl.when(self.outer)
        def _():
            for k in range(self.COUNT - self.RING, self.COUNT):
                self._copy(k, 5).wait_send()

        @pl.when(self.inner)
        def _():
            for k in range(self.COUNT - self.RING, self.COUNT):
                self._copy(k, 6).wait_send()

            @pl.loop(0, self.COUNT)
            def _(i):
                self._copy(i, 7).wait_send()


class Collect:
    def __init__(self, here, source, target, send, recv):
        self.here, self.source, self.target = here, source, target
        self.send, self.recv = send, recv
        self.size = target.shape[1] // 2

    def _copy(self, z):
        here = self.here
        owner, j = here.z // 2, here.z % 2
        dst = self.target.at[j, pl.ds(pl.multiple_of(here.c * self.size, self.size), self.size), :]
        arrive = self.recv.at[2 * j + here.c]
        own = jnp.logical_and(here.z == z, here.c == owner)
        src = self.source.at[pl.ds(pl.multiple_of(z * self.size, self.size), self.size), :]
        return own, src, dst, self.send.at[z], arrive, (here.d - here.c + owner, z)

    def piece(self, z):
        own, src, dst, send, recv, peer = self._copy(z)

        @pl.when(own)
        def _():
            pltpu.make_async_copy(src, dst, recv).start()

        @pl.when(jnp.logical_not(own))
        def _():
            remote(src, dst, send, recv, peer).start()

    def start(self):
        for z in range(4):
            self.piece(z)

    def finish(self):
        for j in range(2):
            for c in range(2):
                dst = self.target.at[j, pl.ds(c * self.size, self.size), :]
                src = self.source.at[pl.ds(0, self.size), :]
                pltpu.make_async_copy(src, dst, self.recv.at[2 * j + c]).wait()
        for z in range(4):
            own, src, dst, send, recv, peer = self._copy(z)

            @pl.when(jnp.logical_not(own))
            def _():
                remote(src, dst, send, recv, peer).wait_send()


BACKWARD_INS = (
    "whole",
    "xs",
    "cots",
    "gbh",
    "qkv",
    "kvo",
    "att",
    "lse",
    "mid",
    "bra",
    "nb",
    "hid",
    "gph",
    "outb",
    "gnb",
    "vec",
    "ups",
    "ada",
)
BACKWARD_OUTS = ("output", "tokens", "qkv_g", "out_g", "up_g", "down_g", "gmod", "condp", "biases")


def backward_kernel(*refs):
    ins = dict(zip(BACKWARD_INS, refs))
    refs = refs[len(BACKWARD_INS) :]
    outs = dict(zip(BACKWARD_OUTS, refs))
    (
        w,
        xs,
        ct,
        gbh,
        qkv,
        kvo,
        kvr,
        att,
        lse,
        mid,
        bra,
        nb_t,
        tmp_t,
        hid,
        gph,
        gnb,
        ga,
        sums,
        dw,
        rc,
        rx,
        ry,
        t,
        ry2,
        rx2,
        r,
        rz1,
        q_,
        rz2,
        shares,
        gs,
        gs_in,
        gmod,
        cpart,
        condp,
        bpart,
        bin_,
        bz,
        biases,
        ld_sem,
        ff_sem,
        r_send,
        r_recv,
        credit,
        o_send,
        o_recv,
        kv_send,
        kv_recv,
        b_send,
        b_recv,
        bz_send,
        bz_recv,
        g_send,
        g_recv,
        m_send,
        m_recv,
        c_send,
        c_recv,
        out_sem,
    ) = refs[len(BACKWARD_OUTS) :]
    here = Place()
    d, z, c, p = here.d, here.z, here.c, here.p
    vec, ups, ada = ins["vec"], ins["ups"], ins["ada"]
    rows, width = xs.shape
    tile, block = 256, 128
    depth = shares.shape[1]

    loads = {}

    def load(name, src, dst):
        loads[name] = pltpu.make_async_copy(src, dst, ld_sem.at[len(loads)])
        loads[name].start()

    def need(*names):
        for name in names:
            loads[name].wait()

    def feed(which, j):
        k = 0 if which is hid else 1
        name = "hid" if which is hid else "gph"
        return pltpu.make_async_copy(ins[name].at[j], which.at[lax.rem(j, 2)], ff_sem.at[k, lax.rem(j, 2)])

    order = (
        ("nb", ins["nb"], ga),
        ("mid", ins["mid"], mid),
        ("gnb", ins["gnb"], gnb),
        ("cots", ins["cots"], ct),
        ("bra", ins["bra"], bra),
        ("att", ins["att"], att),
        ("out_w", ins["whole"].at[OUT], w.at[0]),
        ("gbh", ins["gbh"], gbh),
        ("qkv", ins["qkv"], qkv),
        ("kvo", ins["kvo"], kvo),
        ("lse", ins["lse"], lse),
        ("k_w", ins["whole"].at[KEYS], w.at[1]),
        ("v_w", ins["whole"].at[VALUES], w.at[2]),
        ("xs", ins["xs"], xs),
    )
    load(*order[0])
    feed(gph, 0).start()
    for item in order[1:8]:
        load(*item)
    feed(hid, 0).start()
    for item in order[8:]:
        load(*item)
    feed(gph, 1).start()
    feed(hid, 1).start()

    line_peers = [
        (2 * jnp.bitwise_xor(p, fp) + c, jnp.bitwise_xor(z, fz))
        for fp in range(4)
        for fz in range(4)
        if fp or fz
    ]
    greet(
        line_peers
        + [here.plane(f) for f in (1, 3, 5, 7)]
        + [(jnp.bitwise_xor(d, 1), jnp.bitwise_xor(z, f)) for f in range(1, 4)]
    )

    red = Reduce(
        here, (dw, rc, rx, ry, t, ry2, rx2, r, rz1, q_, rz2, shares), r_send, r_recv, credit
    )
    output = Collect(here, ins["outb"], outs["output"], o_send.at[0], o_recv.at[0])
    output.start()

    def row(i):
        return vec[pl.ds(i, 1), :]

    sums[...] = jnp.zeros_like(sums)

    def add(i, value):
        sums[pl.ds(i, 1), :] = sums[pl.ds(i, 1), :] + value

    need("nb")
    nb_t[...] = ga[...].T
    feed(gph, 0).wait()
    red.produce(0, 0, nb_t, gph.at[0])
    red.produce(1, 1, nb_t, gph.at[0])
    need("mid", "gnb", "cots", "bra")

    @pl.loop(0, rows // block)
    def _(i):
        part_rows = pl.ds(pl.multiple_of(i * block, block), block)
        hat, inverse = norm_parts(mid[part_rows, :])
        grad = gnb[part_rows, :]
        add(3, column_sum(grad))
        add(4, column_sum(grad * hat))
        grad_mid = ct[part_rows, :].astype(F32) + norm_grad(grad, hat, inverse, row(4))
        add(2, column_sum(grad_mid * bra[part_rows, :].astype(F32)))
        add(6, column_sum(grad_mid))
        mid[part_rows, :] = grad_mid
        bra[part_rows, :] = (grad_mid * row(2)).astype(HALF)

    red.tick(0)
    red.tick(1)
    need("att")
    tmp_t[...] = att[...].T
    red.produce(2, 0, tmp_t, bra)
    red.produce(3, 1, tmp_t, bra)
    need("out_w")
    for n in range(width // tile):
        cols = pl.ds(n * tile, tile)
        ga[:, cols] = nt(bra[...], w[0, cols, :]).astype(HALF)
    load("q_w", ins["whole"].at[QUERIES], w.at[0])
    red.tick(2)
    red.tick(3)
    need("gbh", "qkv", "kvo", "lse")

    span = 256
    low = lax.broadcasted_iota(jnp.int32, (span, LANES), 1) < HD
    upper = lax.broadcasted_iota(jnp.int32, (LANES, rows), 0) < HD
    pick = lax.broadcasted_iota(jnp.int32, (8, LANES), 0) == (
        lax.broadcasted_iota(jnp.int32, (8, LANES), 1) // HD
    )
    pick = jnp.where(pick, 1.0, 0.0).astype(HALF)

    def attend_back(step, between):
        cols = pl.ds(pl.multiple_of(step * LANES, LANES), LANES)
        q = qkv[0, :, cols] * HALF(HD**-0.5)
        grad = ga[:, cols]
        product = grad.astype(F32) * att[:, cols].astype(F32)
        top = product.astype(HALF)
        rest = (product - top.astype(F32)).astype(HALF)
        inner = nt(pick, top) + nt(pick, rest)
        dq_t = [jnp.zeros((LANES, rows), F32) for _ in range(2)]
        for group, (k_ref, v_ref) in enumerate(((qkv.at[1], qkv.at[2]), (kvo.at[0], kvo.at[1]))):
            if group:
                between()
            for start in range(0, rows, span):
                part_rows = pl.ds(start, span)
                k = k_ref[part_rows, cols]
                v = v_ref[part_rows, cols]
                k_t = k.T
                dks, dvs = [], []
                for head in range(2):
                    own = low if head == 0 else jnp.logical_not(low)
                    logsum = lse[pl.ds(2 * step + head, 1), :]
                    scores = nt(jnp.where(own, k, jnp.zeros_like(k)), q)
                    probs = jnp.exp(scores - logsum)
                    dvs.append(nn(probs.astype(HALF), grad))
                    gp = nt(jnp.where(own, v, jnp.zeros_like(v)), grad)
                    score_grad = (probs * (gp - inner[head : head + 1, :])).astype(HALF)
                    dks.append(nn(score_grad, q))
                    dq_t[head] = dq_t[head] + nn(k_t, score_grad)
                k_ref[part_rows, cols] = jnp.where(low, dks[0], dks[1]).astype(HALF)
                v_ref[part_rows, cols] = jnp.where(low, dvs[0], dvs[1]).astype(HALF)
        dq = jnp.where(upper, dq_t[0], dq_t[1]).T * HD**-0.5
        qkv[0, :, cols] = dq.astype(HALF)

    @pl.loop(0, 4)
    def _(j):
        slot, base = lax.rem(j, 2), 4 + 2 * j
        feed(hid, j).wait()
        tmp_t[...] = hid[slot].T
        red.produce(base, 0, tmp_t, gbh)

        @pl.when(j < 2)
        def _():
            feed(hid, j + 2).start()

        def even():
            red.tick(base)
            red.produce(base + 1, 1, tmp_t, gbh)

        attend_back(2 * j, even)
        attend_back(2 * j + 1, lambda: red.tick(base + 1))

    def kv_copy(k):
        return remote(kvo.at[k], kvr.at[k], kv_send.at[k], kv_recv.at[k], here.plane(1))

    kv_copy(1).start()
    kv_copy(0).start()
    feed(gph, 2).start()
    feed(gph, 1).wait()
    for side in range(2):
        red.produce(12 + side, side, nb_t, gph.at[1])
    feed(gph, 3).start()
    red.tick(12)
    need("xs", "q_w", "k_w", "v_w")
    for k in (1, 0):
        kv_copy(k).wait_recv()

        @pl.loop(0, rows // block)
        def _(i):
            part_rows = pl.ds(pl.multiple_of(i * block, block), block)
            qkv[1 + k, part_rows, :] = (
                qkv[1 + k, part_rows, :].astype(F32) + kvr[k, part_rows, :].astype(F32)
            ).astype(HALF)

    def project_back(lo, hi):
        @pl.loop(lo, hi)
        def _(n):
            cols = pl.ds(pl.multiple_of(n * tile, tile), tile)
            gnb[:, cols] = (
                nt(qkv[0], w[0, cols, :]) + nt(qkv[1], w[1, cols, :]) + nt(qkv[2], w[2, cols, :])
            )

    project_back(0, 2)
    red.tick(13)
    project_back(2, 4)
    feed(gph, 2).wait()
    for side in range(2):
        red.produce(14 + side, side, nb_t, gph.at[0])
    red.tick(14)

    back = Collect(here, att, outs["tokens"], o_send.at[1], o_recv.at[1])

    @pl.loop(0, rows // block)
    def _(i):
        part_rows = pl.ds(pl.multiple_of(i * block, block), block)
        hat, inverse = norm_parts(xs[part_rows, :].astype(F32))
        ga[part_rows, :] = (hat * (1.0 + row(1)) + row(0)).astype(HALF)
        grad = gnb[part_rows, :]
        add(0, column_sum(grad))
        add(1, column_sum(grad * hat))
        att[part_rows, :] = (
            mid[part_rows, :] + norm_grad(grad, hat, inverse, row(1))
        ).astype(HALF)
        back.piece(i)

        @pl.when(i == 1)
        def _():
            red.tick(15)

    sums[pl.ds(5, 1), :] = ups[pl.ds(4, 1), :]
    for i in range(6):
        for k in range(8):
            gs[pl.ds(8 * i + k, 1), :] = sums[pl.ds(i, 1), pl.ds(k * LANES, LANES)]
    pair = remote(gs, gs_in, g_send.at[0], g_recv.at[0], here.plane(1))
    pair.start()
    sums[pl.ds(7, 1), :] = column_sum(qkv[0].astype(F32))
    sums[pl.ds(8, 1), :] = column_sum(qkv[2].astype(F32))
    sums[pl.ds(6, 1), :] = sums[pl.ds(6, 1), :] * row(2)
    sums[pl.ds(9, 1), :] = ups[pl.ds(5, 1), :] * row(5)
    for k in range(8):
        lanes = pl.ds(k * LANES, LANES)
        for s in range(2):
            source = 7 + k // 4
            bpart[k, pl.ds(s, 1), :] = sums[pl.ds(source, 1), pl.ds((2 * (k % 4) + s) * LANES, LANES)]
        bpart[k, pl.ds(2, 1), :] = sums[pl.ds(6, 1), lanes]
        for j in range(4):
            bpart[k, pl.ds(3 + j, 1), :] = ups[pl.ds(j, 1), lanes]
        bpart[k, pl.ds(7, 1), :] = sums[pl.ds(9, 1), lanes]

    def bias_copy(f):
        flip = jnp.bitwise_xor(d, f)
        return remote(bpart.at[flip], bin_.at[d], b_send.at[f - 1], b_recv.at[f - 1], here.plane(f))

    for f in range(1, 8):
        bias_copy(f).start()
    bin_[d] = bpart[d]
    feed(gph, 3).wait()
    for side in range(2):
        red.produce(16 + side, side, nb_t, gph.at[1])
    red.tick(16)
    pair.wait_recv()
    latent = 4 * p + z
    gmod[latent] = gs[...] + gs_in[...]

    def mod_copy(k):
        return remote(
            gmod.at[latent], gmod.at[latent], m_send.at[k], m_recv.at[k], line_peers[k]
        )

    for k in range(15):
        mod_copy(k).start()
    red.tick(17)
    tmp_t[...] = ga[...].T
    for side in range(2):
        red.produce(18 + side, side, tmp_t, qkv.at[0])
    red.tick(18)
    red.tick(19)
    for side in range(2):
        red.produce(20 + side, side, tmp_t, qkv.at[2])
    red.tick(20)
    red.tick(21)
    for side in range(2):
        red.produce(22 + side, side, tmp_t, qkv.at[1])
    red.tick(22)
    red.tick(23)
    for f in range(1, 8):
        bias_copy(f).wait_recv()
    total = bin_[0]
    for k in range(1, 8):
        total = total + bin_[k]
    bz[z] = total

    def line_copy(f):
        dst = bz.at[z]
        return remote(dst, dst, bz_send.at[f - 1], bz_recv.at[f - 1], here.line(f))

    for f in range(1, 4):
        line_copy(f).start()
    for k in range(24, 28):
        red.tick(k)
    for k in range(15):
        mod_copy(k).wait_recv()
    for i in range(6):
        piece = jnp.concatenate([gmod[:, 8 * i + k, :] for k in range(8)], axis=1)
        term = nt(piece.astype(HALF), ada[:, pl.ds(i * width, width)])
        share = term if i == 0 else share + term
    for k in range(8):
        cpart[k, pl.ds(0, 2), :] = share[2 * k : 2 * k + 2]

    def cond_copy(f):
        flip = jnp.bitwise_xor(d, f)
        return remote(cpart.at[flip], condp.at[d], c_send.at[f - 1], c_recv.at[f - 1], here.plane(f))

    for f in range(1, 8):
        cond_copy(f).start()
    condp[d] = cpart[d]
    for f in range(1, 4):
        line_copy(f).wait_recv()
    biases[...] = bz[0] + bz[1] + bz[2] + bz[3]

    @pl.loop(28, Reduce.COUNT + Reduce.LAGS[0])
    def _(k):
        red.tick(k)

    cut = width // 8
    exits = [
        pltpu.make_async_copy(gmod, outs["gmod"], out_sem.at[1]),
        pltpu.make_async_copy(biases, outs["biases"], out_sem.at[2]),
        pltpu.make_async_copy(shares.at[1], outs["out_g"], out_sem.at[4]),
    ]
    for k, i in enumerate((9, 11, 10)):
        dst = outs["qkv_g"].at[:, pl.ds(k * width, width)]
        exits.append(pltpu.make_async_copy(shares.at[i], dst, out_sem.at[5 + k]))
    for j in range(4):
        dst = outs["down_g"].at[pl.ds(j * depth, depth), :]
        exits.append(pltpu.make_async_copy(shares.at[2 + j], dst, out_sem.at[8 + j]))
    for j, i in enumerate((0, 6, 7, 8)):
        for k in range(8):
            pltpu.make_async_copy(
                shares.at[i, :, pl.ds(k * cut, cut)],
                outs["up_g"].at[:, pl.ds((4 * k + j) * cut, cut)],
                out_sem.at[12 + j],
            ).start()
    for copy in exits:
        copy.start()
    for f in range(1, 8):
        cond_copy(f).wait_recv()
    last = pltpu.make_async_copy(condp, outs["condp"], out_sem.at[3])
    last.start()
    red.drain()
    output.finish()
    back.finish()
    pair.wait_send()
    for k in range(2):
        kv_copy(k).wait_send()
    for f in range(1, 8):
        bias_copy(f).wait_send()
        cond_copy(f).wait_send()
    for f in range(1, 4):
        line_copy(f).wait_send()
    for k in range(15):
        mod_copy(k).wait_send()
    for copy in exits:
        copy.wait()
    for j in range(4):
        dst = outs["up_g"].at[:, pl.ds(0, width)]
        pltpu.make_async_copy(shares.at[0], dst, out_sem.at[12 + j]).wait()
    last.wait()


def backward(f, ada, shape):
    lats, part, width = shape
    rows = lats * part
    depth = ada.shape[0]
    half_cols, part_cols = width // 2, width // 4
    sds = jax.ShapeDtypeStruct
    hbm = pl.BlockSpec(memory_space=pl.ANY)
    vmem = pl.BlockSpec(memory_space=pltpu.VMEM)
    dma = pltpu.SemaphoreType.DMA
    half = lambda *s: pltpu.VMEM(s, HALF)
    full = lambda *s: pltpu.VMEM(s, F32)
    ring, deep, count = Reduce.RING, Reduce.DEEP, Reduce.COUNT
    scratch = [
        half(3, width, width),
        half(rows, width),
        half(rows, width),
        half(rows, width),
        half(3, rows, width),
        half(2, rows, width),
        half(2, rows, width),
        half(rows, width),
        full(LANES, rows),
        full(rows, width),
        half(rows, width),
        half(width, rows),
        half(width, rows),
        half(2, rows, width),
        half(2, rows, width),
        full(rows, width),
        half(rows, width),
        full(16, width),
        half(ring, 2, 2, 2, depth, half_cols),
        half(deep, 2, 2, depth, half_cols),
        half(deep, 2, depth, part_cols),
        half(deep, 2, depth, part_cols),
        half(ring, 2, 2, depth, part_cols),
        half(count, depth, part_cols),
        half(count, depth, part_cols),
        half(ring, depth, half_cols),
        half(count, depth, half_cols),
        half(ring, depth, half_cols),
        half(count, depth, half_cols),
        half(CHUNKS, depth, width),
        full(48, LANES),
        full(48, LANES),
        full(16, 48, LANES),
        full(8, 8, LANES),
        full(8, 8, LANES),
        full(8, 8, LANES),
        full(8, 8, LANES),
        full(4, 8, LANES),
        full(8, LANES),
        dma((20,)),
        dma((2, 2)),
        dma((count, 8)),
        dma((count, 8)),
        pltpu.SemaphoreType.REGULAR((3,)),
        dma((2, 4)),
        dma((2, 4)),
        dma((2,)),
        dma((2,)),
        dma((7,)),
        dma((7,)),
        dma((3,)),
        dma((3,)),
        dma((1,)),
        dma((1,)),
        dma((15,)),
        dma((15,)),
        dma((7,)),
        dma((7,)),
        dma((16,)),
    ]
    operands = [ada if name == "ada" else f[name] for name in BACKWARD_INS]
    near = ("vec", "ups", "ada")
    got = pl.pallas_call(
        backward_kernel,
        out_shape=(
            sds((lats, part, width), HALF),
            sds((lats, part, width), HALF),
            sds((depth, 3 * width), HALF),
            sds((depth, width), HALF),
            sds((depth, 4 * width), HALF),
            sds((4 * depth, width), HALF),
            sds((16, 48, LANES), F32),
            sds((8, 8, LANES), F32),
            sds((8, LANES), F32),
        ),
        in_specs=[vmem if name in near else hbm for name in BACKWARD_INS],
        out_specs=(hbm,) * len(BACKWARD_OUTS),
        scratch_shapes=scratch,
        compiler_params=pltpu.CompilerParams(
            collective_id=2, has_side_effects=True, vmem_limit_bytes=67043328
        ),
        name="backward",
    )(*operands)
    return dict(zip(BACKWARD_OUTS, got))


def body_any(
    tokens,
    condition,
    ada_weight,
    ada_bias,
    qkv_weight,
    qv_bias,
    out_weight,
    out_bias,
    up_weight,
    up_bias,
    down_weight,
    down_bias,
    cotangent,
):
    lats, part, width = tokens.shape
    dp = lax.axis_size("dp")
    seq = lax.axis_size("seq")
    me = lax.axis_index("dp")
    z = lax.axis_index("seq")
    core = me % 2
    pair = me // 2
    chip_lats = 2 * lats
    sub = seq // chip_lats
    first = core == 0

    def flip(x):
        return lax.ppermute(x, "dp", [(i, i ^ 1) for i in range(dp)])

    def shift(x, by):
        if by % sub == 0:
            return x
        return lax.ppermute(
            x, "seq", [(i, i // sub * sub + (i - by) % sub) for i in range(seq)]
        )

    def spread(x):
        halves = x.reshape(lats, 2, part // 2, width)
        keep = lax.dynamic_index_in_dim(halves, core, 1, keepdims=False)
        give = lax.dynamic_index_in_dim(halves, 1 - core, 1, keepdims=False)
        got = flip(give)
        both = jnp.concatenate(
            [jnp.where(first, keep, got), jnp.where(first, got, keep)], axis=0
        )
        both = both.reshape(seq, part // (2 * sub), width)
        return lax.all_to_all(both, "seq", 0, 0, tiled=True).reshape(-1, width)

    def collect(x):
        both = x.reshape(seq, part // (2 * sub), width)
        both = lax.all_to_all(both, "seq", 0, 0, tiled=True)
        both = both.reshape(2, lats, part // 2, width)
        mine = lax.dynamic_index_in_dim(both, core, 0, keepdims=False)
        give = lax.dynamic_index_in_dim(both, 1 - core, 0, keepdims=False)
        got = flip(give)
        return jnp.stack(
            [jnp.where(first, mine, got), jnp.where(first, got, mine)], axis=1
        ).reshape(lats, part, width)

    small = jnp.concatenate(
        [ada_bias, qv_bias, out_bias, up_bias, down_bias, condition.reshape(-1)]
    )
    small_all = lax.all_gather(small, "dp", axis=0, tiled=False)
    sizes = [a.shape[0] for a in (ada_bias, qv_bias, out_bias, up_bias, down_bias)]
    cuts = [0]
    for size in sizes:
        cuts.append(cuts[-1] + size)
    ada_bias_full, qv_full, out_bias_full, up_bias_full, down_bias_full = [
        small_all[:, a:b].reshape(-1).astype(F32) for a, b in zip(cuts[:-1], cuts[1:])
    ]
    cond_all = small_all[:, cuts[-1] :].reshape(dp * lats, width).astype(F32)
    depth = ada_weight.shape[0]
    silu_all = jax.nn.silu(cond_all).astype(HALF)
    silu_mine = lax.dynamic_slice_in_dim(silu_all, me * depth, depth, axis=1)
    partial = nn(silu_mine, ada_weight)
    row_here = z // sub
    wanted = partial.reshape(dp // 2, chip_lats, 6 * width)
    wanted = lax.dynamic_index_in_dim(wanted, row_here, 1, keepdims=True)
    wanted = jnp.broadcast_to(wanted, (dp // 2, 2, 6 * width)).reshape(dp, 6 * width)
    modulation = lax.psum_scatter(wanted, "dp", scatter_dimension=0, tiled=True)[0]
    modulation = (modulation + ada_bias_full).reshape(6, 1, width)
    shift_a, scale_a, gate_a, shift_b, scale_b, gate_b = [modulation[i] for i in range(6)]

    qkv_full = lax.all_gather(qkv_weight, "dp", axis=0, tiled=True)
    out_full = lax.all_gather(out_weight, "dp", axis=0, tiled=True)
    up_full = lax.all_gather(up_weight, "dp", axis=0, tiled=True)
    down_full = lax.all_gather(down_weight, "dp", axis=0, tiled=True)

    rows = spread(tokens).astype(F32)
    cot = spread(cotangent).astype(F32)

    hat_a, inverse_a = norm_parts(rows)
    normed_a = (hat_a * (1.0 + scale_a) + shift_a).astype(HALF)
    bias_all = jnp.concatenate([qv_full[:width], jnp.zeros((width,), F32), qv_full[width:]])
    projected = (nn(normed_a, qkv_full) + bias_all).astype(HALF)
    kv = projected[:, width:]
    ways = [(a, s) for s in range(sub) for a in range(2)]
    others = [shift(flip(kv) if a else kv, s) for a, s in ways[1:]]
    attended, logsum = attend(projected, others, width)
    branch_a = nn(attended, out_full) + out_bias_full
    middle = rows + gate_a * branch_a
    hat_b, inverse_b = norm_parts(middle)
    normed_b = (hat_b * (1.0 + scale_b) + shift_b).astype(HALF)
    hidden_pre = nn(normed_b, up_full) + up_bias_full
    hidden = gelu_tanh(hidden_pre).astype(HALF)
    branch_b = nn(hidden, down_full) + down_bias_full
    output = collect((middle + gate_b * branch_b).astype(HALF))

    grad_gate_b = jnp.sum(cot * branch_b, axis=0)
    grad_branch_b = cot * gate_b
    down_bias_grad = jnp.sum(grad_branch_b, axis=0)
    grad_branch_half = grad_branch_b.astype(HALF)
    down_weight_grad = tn(hidden, grad_branch_half).astype(HALF)
    grad_hidden = nt(grad_branch_half, down_full)
    _, gelu_back = jax.vjp(gelu_tanh, hidden_pre)
    grad_pre = gelu_back(grad_hidden)[0]
    up_bias_grad = jnp.sum(grad_pre, axis=0)
    grad_pre_half = grad_pre.astype(HALF)
    up_weight_grad = tn(normed_b, grad_pre_half).astype(HALF)
    grad_normed_b = nt(grad_pre_half, up_full)
    grad_shift_b = jnp.sum(grad_normed_b, axis=0)
    grad_scale_b = jnp.sum(grad_normed_b * hat_b, axis=0)
    grad_middle = cot + norm_grad(grad_normed_b, hat_b, inverse_b, scale_b)
    grad_gate_a = jnp.sum(grad_middle * branch_a, axis=0)
    grad_branch_a = grad_middle * gate_a
    out_bias_grad = jnp.sum(grad_branch_a, axis=0)
    grad_branch_a_half = grad_branch_a.astype(HALF)
    out_weight_grad = tn(attended, grad_branch_a_half).astype(HALF)
    grad_attended = nt(grad_branch_a_half, out_full).astype(HALF)

    results = attend_grad(projected, others, grad_attended, attended, logsum, width)
    count = len(ways)
    grad_query = results[0]
    grad_keys = results[1 : 1 + count]
    grad_values = results[1 + count :]
    grad_kv = [jnp.concatenate([k, v], axis=1) for k, v in zip(grad_keys, grad_values)]
    total_kv = grad_kv[0].astype(F32)
    for (a, s), part_kv in zip(ways[1:], grad_kv[1:]):
        back = shift(part_kv, -s)
        total_kv = total_kv + (flip(back) if a else back).astype(F32)
    grad_projected = jnp.concatenate([grad_query, total_kv.astype(HALF)], axis=1)
    qkv_weight_grad = tn(normed_a, grad_projected).astype(HALF)
    grad_proj_float = grad_projected.astype(F32)
    qv_bias_grad = jnp.concatenate(
        [
            jnp.sum(grad_proj_float[:, :width], axis=0),
            jnp.sum(grad_proj_float[:, 2 * width :], axis=0),
        ]
    )
    grad_normed_a = nt(grad_projected, qkv_full)
    grad_shift_a = jnp.sum(grad_normed_a, axis=0)
    grad_scale_a = jnp.sum(grad_normed_a * hat_a, axis=0)
    grad_tokens = grad_middle + norm_grad(grad_normed_a, hat_a, inverse_a, scale_a)
    tokens_grad = collect(grad_tokens.astype(HALF)).astype(F32)

    grad_mod = jnp.concatenate(
        [grad_shift_a, grad_scale_a, grad_gate_a, grad_shift_b, grad_scale_b, grad_gate_b]
    )
    every = lax.all_gather(grad_mod, "seq", axis=0, tiled=False)
    every = lax.all_gather(every, "dp", axis=0, tiled=False)
    every = every.reshape(dp // 2, 2, chip_lats, sub, 6 * width).sum(axis=(1, 3))
    every = every.reshape(dp * lats, 6 * width)
    every_half = every.astype(HALF)
    ada_weight_grad = tn(silu_mine, every_half)
    bias_len = ada_bias.shape[0]
    ada_bias_grad = jnp.sum(
        lax.dynamic_slice_in_dim(every, me * bias_len, bias_len, axis=1), axis=0
    )
    cond_part = nt(every_half, ada_weight).reshape(dp, lats, depth)
    cond_part = lax.all_to_all(cond_part, "dp", 0, 0, tiled=True)
    cond_part = cond_part.transpose(1, 0, 2).reshape(lats, width)
    cond_float = condition.astype(F32)
    sigmoid_cond = jax.nn.sigmoid(cond_float)
    silu_slope = sigmoid_cond * (1.0 + cond_float * (1.0 - sigmoid_cond))
    condition_grad = silu_slope * cond_part

    def reduce_weight(grad):
        share = lax.psum_scatter(grad, "dp", scatter_dimension=0, tiled=True)
        return lax.psum(share, "seq").astype(F32)

    bias_parts = jnp.concatenate(
        [
            b.reshape(dp, -1)
            for b in (qv_bias_grad, out_bias_grad, up_bias_grad, down_bias_grad)
        ],
        axis=1,
    )
    bias_parts = lax.psum_scatter(bias_parts, "dp", scatter_dimension=0, tiled=True)
    bias_parts = lax.psum(bias_parts, "seq")[0]
    cuts = [c - sizes[0] for c in cuts[1:]]
    qv_g, ob_g, ub_g, db_g = [bias_parts[a:b] for a, b in zip(cuts[:-1], cuts[1:])]
    return (
        output,
        tokens_grad,
        condition_grad,
        ada_weight_grad,
        ada_bias_grad,
        reduce_weight(qkv_weight_grad),
        qv_g,
        reduce_weight(out_weight_grad),
        ob_g,
        reduce_weight(up_weight_grad),
        ub_g,
        reduce_weight(down_weight_grad),
        db_g,
    )


def body(
    tokens,
    condition,
    ada_weight,
    ada_bias,
    qkv_weight,
    qv_bias,
    out_weight,
    out_bias,
    up_weight,
    up_bias,
    down_weight,
    down_bias,
    cotangent,
):
    lats, part, width = tokens.shape
    dp = lax.axis_size("dp")
    seq = lax.axis_size("seq")
    if (dp, seq, lats) != (8, 4, 2):
        return body_any(
            tokens,
            condition,
            ada_weight,
            ada_bias,
            qkv_weight,
            qv_bias,
            out_weight,
            out_bias,
            up_weight,
            up_bias,
            down_weight,
            down_bias,
            cotangent,
        )
    me = lax.axis_index("dp")
    depth = ada_weight.shape[0]
    wide = dp * up_bias.shape[0]
    cut = wide // (4 * dp)
    small = jnp.concatenate(
        [
            ada_bias.reshape(-1, LANES),
            qv_bias.reshape(-1, LANES),
            out_bias.reshape(-1, LANES),
            up_bias.reshape(-1, LANES),
            down_bias.reshape(-1, LANES),
            jnp.zeros((2, LANES), HALF),
            condition.reshape(-1, LANES),
        ],
        axis=0,
    ).astype(F32)
    f = forward(
        tokens, cotangent, qkv_weight, out_weight, up_weight, down_weight, small, ada_weight
    )
    b = backward(f, ada_weight, tokens.shape)
    every = b["gmod"]
    ada_weight_grad = tn(f["silu"], every.astype(HALF).reshape(dp * lats, 6 * width))
    ada_bias_grad = lax.dynamic_slice_in_dim(
        jnp.sum(every, axis=0).reshape(-1), me * ada_bias.shape[0], ada_bias.shape[0]
    )
    cond_part = b["condp"][:, :lats].transpose(1, 0, 2).reshape(lats, width)
    cond_float = condition.astype(F32)
    sigmoid_cond = jax.nn.sigmoid(cond_float)
    silu_slope = sigmoid_cond * (1.0 + cond_float * (1.0 - sigmoid_cond))
    biases = b["biases"]
    return (
        b["output"],
        b["tokens"].astype(F32),
        silu_slope * cond_part,
        ada_weight_grad,
        ada_bias_grad,
        b["qkv_g"].astype(F32),
        biases[0:2].reshape(-1),
        b["out_g"].astype(F32),
        biases[2],
        b["up_g"].astype(F32),
        biases[3:7].reshape(-1),
        b["down_g"].astype(F32),
        biases[7],
    )


def solution(mesh):
    return jax.shard_map(
        body,
        mesh=mesh,
        in_specs=(
            P("dp", "seq", None),
            P("dp", None),
            P("dp", None),
            P("dp"),
            P("dp", None),
            P("dp"),
            P("dp", None),
            P("dp"),
            P("dp", None),
            P("dp"),
            P("dp", None),
            P("dp"),
            P("dp", "seq", None),
        ),
        out_specs=(
            P("dp", "seq", None),
            P("dp", "seq", None),
            P("dp", None),
            P("dp", None),
            P("dp"),
            P("dp", None),
            P("dp"),
            P("dp", None),
            P("dp"),
            P("dp", None),
            P("dp"),
            P("dp", None),
            P("dp"),
        ),
        check_vma=False,
    )
```
